256 devices in a mesh: batch: 64 (over z, x, y_hi), chan: 4 (over y_lo, core).
Axes of the slice: x: 4, y: 4 (y_hi: 2, y_lo: 2; y = y_hi * 2 + y_lo), z: 8, core: 2. Of those that a mesh axis runs over, the one named last changes fastest.
Arguments:
- signal: float32 [1024, 32768], P('chan', 'batch'), may hold values from -6 to 6
- cotangent: float32 [1024, 32768], P('chan', 'batch'), may hold values from -6 to 6
- first_layer: float32 [33, 64], replicated, may hold values from -5 to 5
- second_layer: float32 [64, 1024], P(None, 'chan'), may hold values from -0.75 to 0.75
- decay_rate: float32 [1024], P('chan'), may hold values from 0.3 to 600
- skip_gain: float32 [1024], P('chan'), may hold values from -4 to 4
Outputs:
- input_grad: float32 [1024, 32768], P('chan', 'batch')
- first_grad: float32 [33, 64], replicated
- second_grad: float32 [64, 1024], P(None, 'chan')
- decay_grad: float32 [1024], P('chan')
- skip_grad: float32 [1024], P('chan')
The draws below stay inside these ranges and needn't reach their ends.
All inputs are finite; a program needn't handle non-finite values.
Results may differ from the reference program's by a relative error of at most 0.0003.
Values sent between devices are 32-bit elements; how exact they have to be, the bound alone decides.
No kernel may reach another device: no remote copies, remote signals or barrier semaphores. Data moves between devices by JAX's collectives and lax.ppermute only.
A program may use at most 128 MiB of HBM per device.

```python
import math
import jax
import jax.numpy as jnp
from jax import lax

WIDTH = 1024
LENGTH = 32768
ORDER = 64
BANDS = 16
EMBED = 33


def block_levels(key, shape, pieces, smallest, top_value):
    gain, own = 1.0, jax.random.fold_in(key, 6)
    for position, parts in pieces:
        heights = jnp.exp(jax.random.uniform(jax.random.fold_in(own, position), (parts,), jnp.float32, smallest / len(pieces), top_value / len(pieces)))
        gain = gain * jnp.repeat(heights, shape[position] // parts).reshape([-1 if axis == position else 1 for axis in range(len(shape))])
    return gain


def scatter_about(own_key, extent, deviation, reach, split=(), kind=jnp.bfloat16):
    result = deviation * jax.random.normal(own_key, extent, jnp.float32)
    if split:
        result = result * block_levels(own_key, extent, split, -0.22, 0.18)
    return jnp.clip(result, -reach, reach).astype(kind)


def setup_inputs(seed: int = 0) -> dict:
    key_of = jax.random.split(jax.random.key(seed), 7)
    return {
        "signal": scatter_about(key_of[0], (WIDTH, LENGTH), 1.0, 6.0, ((0, 4), (1, 64)), jnp.float32),
        "cotangent": scatter_about(key_of[1], (WIDTH, LENGTH), 1.0, 6.0, ((0, 4), (1, 64)), jnp.float32),
        "first_layer": scatter_about(key_of[2], (EMBED, ORDER), 1.0, 5.0, (), jnp.float32),
        "second_layer": scatter_about(key_of[3], (ORDER, WIDTH), ORDER ** -0.5, 0.75, ((1, 4),), jnp.float32),
        "decay_rate": jnp.clip(jnp.exp(math.log(600.0) - 7.6009024 * jax.random.uniform(key_of[4], (WIDTH,), jnp.float32) ** block_levels(key_of[4], (WIDTH,), ((0, 4),), -0.2, 0.2)), 0.3, 600.0),
        "skip_gain": scatter_about(key_of[5], (WIDTH,), 1.0, 4.0, ((0, 4),), jnp.float32),
    }


precise = lax.Precision.HIGHEST
epsilon = 1e-06

def features(positions, length, band_count):
    band_index = jnp.arange(1, band_count + 1, dtype=jnp.int32)
    phase = (band_index[:, None] * positions[None, :] % length).astype(jnp.float32) * (2.0 * math.pi / length)
    linear = positions.astype(jnp.float32)[None, :] / length
    return jnp.concatenate([linear, jnp.cos(phase), jnp.sin(phase)], axis=0)

def reference(signal, cotangent, first_layer, second_layer, decay_rate, skip_gain):
    positions = jnp.arange(LENGTH, dtype=jnp.int32)
    embed = features(positions, LENGTH, BANDS)
    before = jnp.dot(first_layer.T, embed, precision=precise)
    basis = jnp.sin(before)
    fraction = positions.astype(jnp.float32) / LENGTH
    factor = 1.0 / math.sqrt(LENGTH)
    padded = 2 * LENGTH
    stride = 64
    blocks_count = WIDTH // stride

    def step(carry, index):
        start = (index * stride).astype(jnp.int32)
        values = lax.dynamic_slice_in_dim(signal, start, stride, 0)
        cotan = lax.dynamic_slice_in_dim(cotangent, start, stride, 0)
        columns = lax.dynamic_slice_in_dim(second_layer, start, stride, 1)
        rates = lax.dynamic_slice_in_dim(decay_rate, start, stride, 0)
        gains = lax.dynamic_slice_in_dim(skip_gain, start, stride, 0)
        window = jnp.exp(-rates[:, None] * fraction[None, :])
        shaped = window * jnp.dot(columns.T, basis, precision=precise)
        norms = jnp.sqrt(lax.optimization_barrier(jnp.sum(shaped * shaped, axis=1, keepdims=True)) + epsilon)
        filt = shaped / norms
        spec_val = jnp.fft.rfft(values, n=padded)
        spec_cot = jnp.fft.rfft(cotan, n=padded)
        spec_filt = jnp.fft.rfft(filt, n=padded)
        in_grad = jnp.fft.irfft(jnp.conj(spec_filt) * spec_cot, n=padded)[:, :LENGTH] + gains[:, None] * cotan
        dfilt = factor * jnp.fft.irfft(jnp.conj(spec_val) * spec_cot, n=padded)[:, :LENGTH]
        skip_part = factor * lax.optimization_barrier(jnp.sum(cotan * values, axis=1))
        project = lax.optimization_barrier(jnp.sum(filt * dfilt, axis=1, keepdims=True))
        draw = (dfilt - filt * project) / norms
        decay_part = -lax.optimization_barrier(jnp.sum(draw * shaped * fraction[None, :], axis=1))
        dmix = draw * window
        second_part = jnp.dot(basis, dmix.T, precision=precise)
        carry = carry + jnp.dot(columns, dmix, precision=precise)
        return (carry, (in_grad.astype(jnp.float32), second_part, decay_part, skip_part))
    dbasis, results = lax.scan(step, jnp.zeros((ORDER, LENGTH), jnp.float32), jnp.arange(blocks_count, dtype=jnp.int32))
    in_blocks, second_blocks, decay_blocks, skip_blocks = results
    input_grad = in_blocks.reshape(WIDTH, LENGTH)
    second_grad = jnp.transpose(second_blocks, (1, 0, 2)).reshape(ORDER, WIDTH)
    decay_grad = decay_blocks.reshape(WIDTH)
    skip_grad = skip_blocks.reshape(WIDTH)
    first_grad = jnp.dot(embed, (jnp.cos(before) * dbasis).T, precision=precise)
    return (input_grad, first_grad, second_grad, decay_grad, skip_grad)
```

```python
import math

import jax
import jax.numpy as jnp
import numpy as np
from jax import lax
from jax.experimental import pallas as pl
from jax.experimental.pallas import tpu as pltpu
from jax.sharding import PartitionSpec as P

ROWS = 256
COLS = 128
LENGTH = ROWS * COLS
NARROW = 4
TINY = 1e-06
f32 = jnp.float32
bf16 = jnp.bfloat16
highest = lax.Precision.HIGHEST


def halves(x):
    high = x.astype(bf16)
    low = (x - high.astype(np.float64)).astype(bf16)
    return high, low


def make_tables(embed):
    a = np.arange(ROWS)
    k = np.arange(ROWS)
    m = np.arange(COLS)
    bands = embed // 2
    turn = np.pi * ((a[None, :] * (4 * k + 1)[:, None]) % (4 * ROWS)) / (2 * ROWS)
    first = np.concatenate([np.cos(turn), -np.sin(turn)], axis=0)
    twist = np.pi * (4 * k + 1)[:, None] * m[None, :] / (2 * LENGTH)
    angle = 2.0 * np.pi * ((m[:, None] * m[None, :]) % COLS) / COLS
    c, s = np.cos(angle), np.sin(angle)
    second = np.concatenate(
        [np.concatenate([c, -s], axis=1), np.concatenate([s, c], axis=1)], axis=0
    )
    high, low = halves(first)
    forward_left = np.concatenate([high, low, high], axis=1)
    inverse_left = np.concatenate([high.T, low.T, high.T], axis=1)
    high, low = halves(second)
    forward_right = np.concatenate([high, high, low], axis=0)
    inverse_right = np.concatenate([high.T, high.T, low.T], axis=0)
    rows = np.zeros((ROWS, COLS))
    lanes = np.zeros((COLS, COLS))
    half = COLS // 2
    rows[:, 0] = a * COLS / LENGTH
    lanes[0] = 1.0
    rows[:, half] = 1.0
    lanes[half] = m / LENGTH
    for b in range(1, bands + 1):
        big = 2.0 * np.pi * ((b * COLS * a) % LENGTH) / LENGTH
        small = 2.0 * np.pi * b * m / LENGTH
        rows[:, b] = np.cos(big)
        rows[:, half + b] = -np.sin(big)
        rows[:, bands + b] = np.sin(big)
        rows[:, half + bands + b] = np.cos(big)
        lanes[b] = np.cos(small)
        lanes[half + b] = np.sin(small)
        lanes[bands + b] = np.cos(small)
        lanes[half + bands + b] = np.sin(small)
    high, low = halves(lanes.T)
    gather = np.concatenate([high, high, low], axis=0)
    return dict(
        forward_left=forward_left,
        inverse_left=inverse_left,
        forward_right=forward_right,
        inverse_right=inverse_right,
        twist_cos=np.cos(twist).astype(np.float32),
        twist_sin=np.sin(twist).astype(np.float32),
        rows=rows.astype(np.float32),
        lanes=lanes.astype(np.float32),
        gather=gather,
    )


def split(x):
    high = x.astype(bf16)
    low = (x - high.astype(f32)).astype(bf16)
    return high, low


def mm(left, right):
    return lax.dot_general(left, right, (((1,), (0,)), ((), ())), preferred_element_type=f32)


def dot_rows(table, x):
    high, low = split(x)
    return mm(table, jnp.concatenate([high, high, low], axis=0))


def dot_cols(x, table):
    high, low = split(x)
    return mm(jnp.concatenate([high, low, high], axis=1), table)


def forward_pair(x, y, left, right, twist_cos, twist_sin):
    u = dot_rows(left, jnp.concatenate([x, y], axis=1))
    spectra = []
    for n in range(2):
        re = u[:ROWS, n * COLS : (n + 1) * COLS]
        im = u[ROWS:, n * COLS : (n + 1) * COLS]
        v = jnp.concatenate(
            [re * twist_cos + im * twist_sin, im * twist_cos - re * twist_sin], axis=1
        )
        spectra.append(dot_cols(v, right))
    return spectra


def times_conj(f, c):
    fr, fi, cr, ci = f[:, :COLS], f[:, COLS:], c[:, :COLS], c[:, COLS:]
    return jnp.concatenate([fr * cr + fi * ci, fr * ci - fi * cr], axis=1)


def inverse_pair(g, h, left, right, twist_cos, twist_sin):
    parts = []
    for x in (g, h):
        w = dot_cols(x, right)
        re, im = w[:, :COLS], w[:, COLS:]
        parts.append(
            jnp.concatenate(
                [re * twist_cos - im * twist_sin, im * twist_cos + re * twist_sin], axis=0
            )
        )
    y = dot_rows(left, jnp.concatenate(parts, axis=1))
    return y[:, :COLS], y[:, COLS:]


def sin_and_cos(x):
    q = jnp.round(x * (2.0 / math.pi))
    r = x - q * 1.5703125
    r = r - q * 4.837512969970703e-4
    r = r - q * 7.549789954891882e-8
    z = r * r
    s = ((-1.9515295891e-4 * z + 8.3321608736e-3) * z - 1.6666654611e-1) * z * r + r
    c = ((2.443315711809948e-5 * z - 1.388731625493765e-3) * z + 4.166664568298827e-2) * (z * z)
    c = c - 0.5 * z + 1.0
    turns = q.astype(jnp.int32)
    odd = (turns & 1) == 1
    sin_x = jnp.where(odd, c, s)
    cos_x = jnp.where(odd, s, c)
    sin_x = jnp.where((turns & 2) == 2, -sin_x, sin_x)
    cos_x = jnp.where(((turns + 1) & 2) == 2, -cos_x, cos_x)
    return sin_x, cos_x


def fraction_rows(count, offset):
    a = lax.broadcasted_iota(jnp.int32, (count, COLS), 0) + offset
    m = lax.broadcasted_iota(jnp.int32, (count, COLS), 1)
    return (a * COLS + m).astype(f32) * (1.0 / LENGTH)


def filter_kernel(
    weights, columns, rates, rows, lanes, left, right, tcos, tsin,
    basis, slope, filt, window, norms, spectra,
):
    order = basis.shape[0]

    def fill(k, carry):
        scaled = rows[...] * weights[pl.ds(k, 1), :]
        basis[k] = jnp.dot(scaled, lanes[...], precision=highest, preferred_element_type=f32)
        return carry

    lax.fori_loop(0, order, fill, 0)
    chunk = 64

    def bend(k, carry):
        for n in range(ROWS // chunk):
            here = pl.ds(n * chunk, chunk)
            s, c = sin_and_cos(basis[k, here, :])
            basis[k, here, :] = s
            slope[k, here, :] = c
        return carry

    lax.fori_loop(0, order, bend, 0)
    part = 32

    def mix(n, totals):
        start = pl.multiple_of(n * part, part)
        here = pl.ds(start, part)

        def add(k, acc):
            b = basis[k, here, :]
            return tuple(acc[c] + columns[k, c] * b for c in range(NARROW))

        acc = lax.fori_loop(
            0, order, add, tuple(jnp.zeros((part, COLS), f32) for _ in range(NARROW)), unroll=2
        )
        fraction = fraction_rows(part, start)
        out = []
        for c in range(NARROW):
            win = jnp.exp(-rates[c] * fraction)
            raw = win * acc[c]
            window[c, here, :] = win
            filt[c, here, :] = raw
            out.append(totals[c] + (raw * raw).reshape(part // 8, 8, COLS).sum(0))
        return tuple(out)

    totals = lax.fori_loop(
        0, ROWS // part, mix, tuple(jnp.zeros((8, COLS), f32) for _ in range(NARROW))
    )
    for c in range(NARROW):
        norm = jnp.sqrt(jnp.sum(totals[c], keepdims=True) + TINY)
        norms[pl.ds(c, 1), :] = jnp.broadcast_to(norm, (1, COLS))
        filt[c] = filt[c] / norm
    for c in range(0, NARROW, 2):
        x, y = forward_pair(filt[c], filt[c + 1], left[...], right[...], tcos[...], tsin[...])
        spectra[c] = x
        spectra[c + 1] = y


def main_kernel(
    both, columns, gains, basis, slope, filt, window, norms, spectra, rows, gather,
    fleft, fright, ileft, iright, tcos, tsin,
    grad, small, first,
    dmix, second_rows, first_rows, staged,
):
    order = basis.shape[0]
    factor = 1.0 / math.sqrt(LENGTH)
    lane = lax.broadcasted_iota(jnp.int32, (1, COLS), 1)
    scalars = jnp.zeros((1, COLS), f32)
    fraction = fraction_rows(ROWS, 0)
    for c in range(NARROW):
        x = both[pl.ds(c, ROWS, stride=2 * NARROW), :]
        y = both[pl.ds(NARROW + c, ROWS, stride=2 * NARROW), :]
        skip = factor * jnp.sum(x * y, keepdims=True)
        val, cot = forward_pair(x, y, fleft[...], fright[...], tcos[...], tsin[...])
        back, into = inverse_pair(
            times_conj(val, cot), times_conj(spectra[c], cot),
            ileft[...], iright[...], tcos[...], tsin[...],
        )
        y = both[pl.ds(NARROW + c, ROWS, stride=2 * NARROW), :]
        staged[pl.ds(c, ROWS, stride=NARROW), :] = into * (1.0 / LENGTH) + gains[c] * y
        dfilt = back * (factor / LENGTH)
        project = jnp.sum(filt[c] * dfilt, keepdims=True)
        norm = norms[pl.ds(c, 1), :][:, :1]
        draw = (dfilt - filt[c] * project) / norm
        decay = -jnp.sum(draw * filt[c] * fraction, keepdims=True) * norm
        dmix[c] = draw * window[c]
        scalars = jnp.where(lane == c, decay, scalars)
        scalars = jnp.where(lane == NARROW + c, skip, scalars)
    grad[...] = staged[...].reshape(grad.shape)
    chunk = 64

    def tail(k, carry):
        acc = [jnp.zeros((8, COLS), f32) for _ in range(NARROW)]
        pieces = []
        for n in range(ROWS // chunk):
            here = pl.ds(n * chunk, chunk)
            b = basis[k, here, :]
            mixed = jnp.zeros((chunk, COLS), f32)
            for c in range(NARROW):
                d = dmix[c, here, :]
                acc[c] = acc[c] + (b * d).reshape(chunk // 8, 8, COLS).sum(0)
                mixed = mixed + columns[k, c] * d
            pieces.append(mixed * slope[k, here, :])
        r = dot_cols(jnp.concatenate(pieces, axis=0), gather[...])
        first_rows[pl.ds(k, 1), :] = jnp.sum(r * rows[...], axis=0, keepdims=True)
        for c in range(NARROW):
            second_rows[pl.ds(c * order + k, 1), :] = jnp.sum(acc[c], axis=0, keepdims=True)
        return carry

    lax.fori_loop(0, order, tail, 0, unroll=2)
    ones = jnp.ones((8, COLS), f32)
    for n in range(NARROW * order // COLS):
        block = second_rows[pl.ds(n * COLS, COLS), :]
        sums = lax.dot_general(
            ones, block, (((1,), (1,)), ((), ())), precision=highest, preferred_element_type=f32
        )
        small[pl.ds(n, 1), :] = sums[:1, :]
    small[pl.ds(2, 1), :] = scalars
    turned = jnp.transpose(first_rows[...], (1, 0))
    half = COLS // 2
    folded = turned[:half] + turned[half:]
    first[...] = jnp.concatenate([folded[:20], folded[20:40]], axis=1)


def pack(signal, cotangent, groups):
    def turn(x):
        return x.reshape(groups, NARROW, -1, COLS).transpose(0, 2, 1, 3)

    both = jnp.concatenate([turn(signal), turn(cotangent)], axis=2)
    return both.reshape(groups, -1, COLS)


def local(signal, cotangent, first_layer, second_layer, decay_rate, skip_gain):
    groups = lax.axis_size("batch")
    place = lax.axis_index("batch")
    side = lax.axis_index("chan")
    sides = lax.axis_size("chan")
    embed, order = first_layer.shape
    t = make_tables(embed)
    vmem = pl.BlockSpec(memory_space=pltpu.VMEM)
    smem = pl.BlockSpec(memory_space=pltpu.SMEM)

    sent = pack(signal, cotangent, groups)
    spread = lax.all_to_all(sent, "batch", split_axis=0, concat_axis=0, tiled=True)

    columns = lax.dynamic_slice_in_dim(second_layer, place * NARROW, NARROW, 1)
    rates = lax.dynamic_slice_in_dim(decay_rate, place * NARROW, NARROW, 0)
    gains = lax.dynamic_slice_in_dim(skip_gain, place * NARROW, NARROW, 0)
    weights = jnp.pad(first_layer.T, ((0, 0), (0, COLS // 2 - embed)))
    weights = jnp.concatenate([weights, weights], axis=1)

    cube = jax.ShapeDtypeStruct((order, ROWS, COLS), f32)
    four = jax.ShapeDtypeStruct((NARROW, ROWS, COLS), f32)
    basis, slope, filt, window, norms, spectra = pl.pallas_call(
        filter_kernel,
        out_shape=(
            cube, cube, four, four,
            jax.ShapeDtypeStruct((NARROW, COLS), f32),
            jax.ShapeDtypeStruct((NARROW, ROWS, 2 * COLS), f32),
        ),
        in_specs=[vmem, smem, smem] + [vmem] * 6,
        out_specs=(vmem,) * 6,
        cost_estimate=pl.CostEstimate(flops=20_000_000_000, bytes_accessed=20_000_000, transcendentals=0),
        name="make_filter",
    )(
        weights, columns, rates, t["rows"], t["lanes"],
        t["forward_left"], t["forward_right"], t["twist_cos"], t["twist_sin"],
    )

    grad, small, first = pl.pallas_call(
        main_kernel,
        out_shape=(
            jax.ShapeDtypeStruct((groups, 4 * NARROW, COLS), f32),
            jax.ShapeDtypeStruct((3, COLS), f32),
            jax.ShapeDtypeStruct((20, COLS), f32),
        ),
        in_specs=[vmem, smem, smem] + [vmem] * 14,
        out_specs=(vmem,) * 3,
        scratch_shapes=[
            pltpu.VMEM((NARROW, ROWS, COLS), f32),
            pltpu.VMEM((NARROW * order, COLS), f32),
            pltpu.VMEM((order, COLS), f32),
            pltpu.VMEM((NARROW * ROWS, COLS), f32),
        ],
        name="correlate",
    )(
        spread.reshape(-1, COLS), columns, gains, basis, slope, filt, window, norms, spectra,
        t["rows"], t["gather"], t["forward_left"], t["forward_right"],
        t["inverse_left"], t["inverse_right"], t["twist_cos"], t["twist_sin"],
    )

    quarter = first.shape[0] // sides
    own = lax.dynamic_slice_in_dim(first, side * quarter, quarter, 0)
    for step in range(1, sides):
        ring = [(i, (i + step) % sides) for i in range(sides)]
        piece = lax.dynamic_slice_in_dim(first, (side + step) % sides * quarter, quarter, 0)
        own = own + lax.ppermute(piece, "chan", ring)
    shared = jnp.concatenate([small, own], axis=0)
    back = jnp.concatenate([grad, jnp.broadcast_to(shared, (groups,) + shared.shape)], axis=1)
    home = lax.all_to_all(back, "batch", split_axis=0, concat_axis=0, tiled=True)

    rows = 4 * NARROW
    input_grad = (
        home[:, :rows].reshape(groups, 4, NARROW, COLS).transpose(0, 2, 1, 3)
        .reshape(groups * NARROW, 4 * COLS)
    )
    second_grad = home[:, rows : rows + 2].reshape(groups * NARROW, order).T
    decay_grad = home[:, rows + 2, :NARROW].reshape(groups * NARROW)
    skip_grad = home[:, rows + 2, NARROW : 2 * NARROW].reshape(groups * NARROW)
    mine = home[:, rows + 3 :].sum(0)
    gathered = [mine]
    for step in range(1, sides):
        ring = [((i + step) % sides, i) for i in range(sides)]
        gathered.append(lax.ppermute(mine, "chan", ring))
    twice = jnp.concatenate(gathered + gathered, axis=0)
    ordered = lax.dynamic_slice_in_dim(
        twice, (sides - side) % sides * quarter, sides * quarter, 0
    )
    first_grad = jnp.concatenate([ordered[:, :order], ordered[:, order:]], axis=0)[:embed]
    return (input_grad, first_grad, second_grad, decay_grad, skip_grad)


def solution(mesh):
    placed = (P("chan", "batch"), P("chan", "batch"), P(), P(None, "chan"), P("chan"), P("chan"))
    return jax.shard_map(
        local,
        mesh=mesh,
        in_specs=placed,
        out_specs=(P("chan", "batch"), P(), P(None, "chan"), P("chan"), P("chan")),
        check_vma=False,
    )
```

```python
import math

import jax
import jax.numpy as jnp
import numpy as np
from jax import lax
from jax.experimental import pallas as pl
from jax.experimental.pallas import tpu as pltpu
from jax.sharding import PartitionSpec as P

ROWS = 256
COLS = 128
LENGTH = ROWS * COLS
NARROW = 4
FILTER_MIB = 24
MAIN_MIB = 28
TINY = 1e-06
f32 = jnp.float32
bf16 = jnp.bfloat16
highest = lax.Precision.HIGHEST


def halves(x):
    high = x.astype(bf16)
    low = (x - high.astype(np.float64)).astype(bf16)
    return high, low


SIN = (6.28318528, -10.33542017, 5.100155046, -1.196582571, 0.1553153206)
COS = (0.9999999532, -4.934792831, 4.058411353, -1.331876568, 0.2196896111)


def make_tables(embed):
    a = np.arange(ROWS)
    k = np.arange(ROWS)
    m = np.arange(COLS)
    bands = embed // 2
    turn = np.pi * ((a[None, :] * (4 * k + 1)[:, None]) % (4 * ROWS)) / (2 * ROWS)
    first = np.concatenate([np.cos(turn), -np.sin(turn)], axis=0)
    twist = np.pi * (4 * k + 1)[:, None] * m[None, :] / (2 * LENGTH)
    angle = 2.0 * np.pi * ((m[:, None] * m[None, :]) % COLS) / COLS
    c, s = np.cos(angle), np.sin(angle)
    second = np.concatenate(
        [np.concatenate([c, -s], axis=1), np.concatenate([s, c], axis=1)], axis=0
    )
    high, low = halves(first)
    forward_left = np.concatenate([high, low], axis=1)
    inverse_left = np.concatenate([high.T, low.T], axis=1)
    high, low = halves(second)
    forward_right = np.concatenate([high, low], axis=0)
    inverse_right = np.concatenate([high.T, low.T], axis=0)
    rows = np.zeros((ROWS, COLS))
    lanes = np.zeros((COLS, COLS))
    half = COLS // 2
    rows[:, 0] = a * COLS / LENGTH
    lanes[0] = 1.0
    rows[:, half] = 1.0
    lanes[half] = m / LENGTH
    for b in range(1, bands + 1):
        big = 2.0 * np.pi * ((b * COLS * a) % LENGTH) / LENGTH
        small = 2.0 * np.pi * b * m / LENGTH
        rows[:, b] = np.cos(big)
        rows[:, half + b] = -np.sin(big)
        rows[:, bands + b] = np.sin(big)
        rows[:, half + bands + b] = np.cos(big)
        lanes[b] = np.cos(small)
        lanes[half + b] = np.sin(small)
        lanes[bands + b] = np.cos(small)
        lanes[half + bands + b] = np.sin(small)
    high, low = halves(lanes.T)
    gather = np.concatenate([high, low], axis=0)
    high, low = halves(lanes)
    lowest = (lanes - high.astype(np.float64) - low.astype(np.float64)).astype(bf16)
    spread = np.concatenate([high, low, lowest, high, low, high], axis=0)
    return dict(
        forward_left=forward_left,
        inverse_left=inverse_left,
        forward_right=forward_right,
        inverse_right=inverse_right,
        twist_cos=np.cos(twist).astype(np.float32),
        twist_sin=np.sin(twist).astype(np.float32),
        rows=rows.astype(np.float32),
        spread=spread,
        gather=gather,
    )


def split(x):
    high = x.astype(bf16)
    low = (x - high.astype(f32)).astype(bf16)
    return high, low


def mm(left, right):
    return lax.dot_general(left, right, (((1,), (0,)), ((), ())), preferred_element_type=f32)


def dot_rows(table, x):
    high, low = split(x)
    left = jnp.concatenate([table, table[:, : x.shape[0]]], axis=1)
    return mm(left, jnp.concatenate([high, high, low], axis=0))


def dot_cols(x, table):
    high, low = split(x)
    count = x.shape[1]
    right = jnp.concatenate([table[:count], table], axis=0)
    return mm(jnp.concatenate([high, low, high], axis=1), right)


def forward_pair(x, y, left, right, twist_cos, twist_sin):
    u = dot_rows(left, jnp.concatenate([x, y], axis=1))
    spectra = []
    for n in range(2):
        re = u[:ROWS, n * COLS : (n + 1) * COLS]
        im = u[ROWS:, n * COLS : (n + 1) * COLS]
        v = jnp.concatenate(
            [re * twist_cos + im * twist_sin, im * twist_cos - re * twist_sin], axis=1
        )
        spectra.append(dot_cols(v, right))
    return spectra


def times_conj(f, c):
    fr, fi, cr, ci = f[:, :COLS], f[:, COLS:], c[:, :COLS], c[:, COLS:]
    return jnp.concatenate([fr * cr + fi * ci, fr * ci - fi * cr], axis=1)


def inverse_pair(g, h, left, right, twist_cos, twist_sin):
    parts = []
    for x in (g, h):
        w = dot_cols(x, right)
        re, im = w[:, :COLS], w[:, COLS:]
        parts.append(
            jnp.concatenate(
                [re * twist_cos - im * twist_sin, im * twist_cos + re * twist_sin], axis=0
            )
        )
    y = dot_rows(left, jnp.concatenate(parts, axis=1))
    return y[:, :COLS], y[:, COLS:]


def sin_and_cos(x):
    r = x - ((x + 12582912.0) - 12582912.0)
    z = r * r
    s = SIN[4]
    for n in (3, 2, 1, 0):
        s = s * z + SIN[n]
    s = s * r
    c = COS[4]
    for n in (3, 2, 1, 0):
        c = c * z + COS[n]
    return s * c, 1.0 - 0.5 * (s * s)


def fraction_rows(count, offset):
    a = lax.broadcasted_iota(jnp.int32, (count, COLS), 0) + offset
    m = lax.broadcasted_iota(jnp.int32, (count, COLS), 1)
    return (a * COLS + m).astype(f32) * (1.0 / LENGTH)


def zip_rows(x, y):
    low = lax.broadcasted_iota(jnp.int32, x.shape, 0) % 8 < 4
    count = x.shape[0]
    return (
        jnp.where(low, x, pltpu.roll(y, 4, 0)),
        jnp.where(low, pltpu.roll(x, count - 4, 0), y),
    )


def pack_kernel(signal, cotangent, out):
    for q in range(signal.shape[1] // COLS):
        here = pl.ds(q * COLS, COLS)
        for n, part in enumerate(zip_rows(signal[:, here], cotangent[:, here])):
            out[:, n, 8 * q : 8 * q + 8, :] = part.reshape(-1, 8, COLS)


def filter_kernel(
    weights, columns, rates, rows, spread, left, right, tcos, tsin,
    basis, slope, filt, window, norms, spectra,
):
    order = basis.shape[0]
    batch = 4

    def fill(n, carry):
        scaled = jnp.concatenate(
            [rows[...] * weights[pl.ds(n * batch + i, 1), :] for i in range(batch)], axis=0
        )
        high = scaled.astype(bf16)
        rest = scaled - high.astype(f32)
        low = rest.astype(bf16)
        lowest = (rest - low.astype(f32)).astype(bf16)
        turns = mm(jnp.concatenate([high, high, high, low, low, lowest], axis=1), spread[...])
        for i in range(batch):
            basis[n * batch + i] = turns[i * ROWS : (i + 1) * ROWS]
        return carry

    lax.fori_loop(0, order // batch, fill, 0)
    chunk = 64

    def bend(k, carry):
        for n in range(ROWS // chunk):
            here = pl.ds(n * chunk, chunk)
            s, c = sin_and_cos(basis[k, here, :])
            basis[k, here, :] = s
            slope[k, here, :] = c
        return carry

    lax.fori_loop(0, order, bend, 0)
    part = 32

    def mix(n, totals):
        start = pl.multiple_of(n * part, part)
        here = pl.ds(start, part)

        def add(k, acc):
            b = basis[k, here, :]
            return tuple(acc[c] + columns[k, c] * b for c in range(NARROW))

        acc = lax.fori_loop(
            0, order, add, tuple(jnp.zeros((part, COLS), f32) for _ in range(NARROW)), unroll=4
        )
        fraction = fraction_rows(part, start)
        out = []
        for c in range(NARROW):
            win = jnp.exp(-rates[c] * fraction)
            raw = win * acc[c]
            window[c, here, :] = win
            filt[c, here, :] = raw
            out.append(totals[c] + (raw * raw).reshape(part // 8, 8, COLS).sum(0))
        return tuple(out)

    totals = lax.fori_loop(
        0, ROWS // part, mix, tuple(jnp.zeros((8, COLS), f32) for _ in range(NARROW))
    )
    for c in range(NARROW):
        norm = jnp.sqrt(jnp.sum(totals[c], keepdims=True) + TINY)
        norms[pl.ds(c, 1), :] = jnp.broadcast_to(norm, (1, COLS))
        filt[c] = filt[c] / norm
    for c in range(0, NARROW, 2):
        x, y = forward_pair(filt[c], filt[c + 1], left[...], right[...], tcos[...], tsin[...])
        spectra[c] = x
        spectra[c + 1] = y


def main_kernel(
    both, columns, basis, slope, filt, window, norms, rows, gather,
    fleft, fright, ileft, iright, tcos, tsin,
    small, first, cotan,
    dmix, product, second_rows, first_rows,
):
    order = basis.shape[0]
    factor = 1.0 / math.sqrt(LENGTH)
    lane = lax.broadcasted_iota(jnp.int32, (1, COLS), 1)
    scalars = jnp.zeros((1, COLS), f32)
    fraction = fraction_rows(ROWS, 0)
    for c in range(NARROW):
        x = both[pl.ds(c, ROWS, stride=2 * NARROW), :]
        y = both[pl.ds(NARROW + c, ROWS, stride=2 * NARROW), :]
        skip = factor * jnp.sum(x * y, keepdims=True)
        scalars = jnp.where(lane == NARROW + c, skip, scalars)
        val, cot = forward_pair(x, y, fleft[...], fright[...], tcos[...], tsin[...])
        cotan[c] = cot
        product[c] = times_conj(val, cot)
    for c in range(0, NARROW, 2):
        pair = inverse_pair(
            product[c], product[c + 1], ileft[...], iright[...], tcos[...], tsin[...]
        )
        for n in range(2):
            i = c + n
            dfilt = pair[n] * (factor / LENGTH)
            project = jnp.sum(filt[i] * dfilt, keepdims=True)
            norm = norms[pl.ds(i, 1), :][:, :1]
            draw = (dfilt - filt[i] * project) / norm
            decay = -jnp.sum(draw * filt[i] * fraction, keepdims=True) * norm
            dmix[i] = draw * window[i]
            scalars = jnp.where(lane == i, decay, scalars)
    chunk = 64

    def tail(k, carry):
        acc = [jnp.zeros((8, COLS), f32) for _ in range(NARROW)]
        pieces = []
        for n in range(ROWS // chunk):
            here = pl.ds(n * chunk, chunk)
            b = basis[k, here, :]
            mixed = None
            for c in range(NARROW):
                d = dmix[c, here, :]
                acc[c] = acc[c] + (b * d).reshape(chunk // 8, 8, COLS).sum(0)
                mixed = columns[k, c] * d if c == 0 else mixed + columns[k, c] * d
            pieces.append(mixed * slope[k, here, :])
        r = dot_cols(jnp.concatenate(pieces, axis=0), gather[...])
        first_rows[pl.ds(k, 1), :] = jnp.sum(r * rows[...], axis=0, keepdims=True)
        for c in range(NARROW):
            second_rows[pl.ds(c * order + k, 1), :] = jnp.sum(acc[c], axis=0, keepdims=True)
        return carry

    lax.fori_loop(0, order, tail, 0, unroll=2)
    ones = jnp.ones((8, COLS), f32)
    for n in range(NARROW * order // COLS):
        block = second_rows[pl.ds(n * COLS, COLS), :]
        sums = lax.dot_general(
            ones, block, (((1,), (1,)), ((), ())), precision=highest, preferred_element_type=f32
        )
        small[pl.ds(n, 1), :] = sums[:1, :]
    small[pl.ds(2, 1), :] = scalars
    turned = jnp.transpose(first_rows[...], (1, 0))
    half = COLS // 2
    folded = turned[:half] + turned[half:]
    first[...] = jnp.concatenate([folded[:20], folded[20:40]], axis=1)


def input_kernel(both, gains, spectra, cotan, ileft, iright, tcos, tsin, grad):
    for c in range(0, NARROW, 2):
        pair = inverse_pair(
            times_conj(spectra[c], cotan[c]), times_conj(spectra[c + 1], cotan[c + 1]),
            ileft[...], iright[...], tcos[...], tsin[...],
        )
        for n in range(2):
            i = c + n
            y = both[pl.ds(NARROW + i, ROWS, stride=2 * NARROW), :]
            grad[pl.ds(i, ROWS, stride=NARROW), :] = pair[n] * (1.0 / LENGTH) + gains[i] * y


def join_kernel(grad, small, own, one, two, three, out, tile):
    rows = grad.shape[0] // out.shape[0]
    tile[:3] = small[...]
    tile[3:] = own[...] + one[...] + two[...] + three[...]
    out[:, :rows, :] = grad[...].reshape(out.shape[0], rows, COLS)
    out[:, rows:, :] = jnp.broadcast_to(tile[...][None], (out.shape[0],) + tile.shape)


def unpack_kernel(pairs, home, grad, second, decay, skip):
    groups = grad.shape[0] // NARROW
    order = second.shape[0]
    rows = grad.shape[1] // COLS * NARROW
    block = rows + 8
    for p in range(rows // 8):
        even = pairs[:, 0, 8 * p : 8 * p + 8, :].reshape(-1, COLS)
        odd = pairs[:, 1, 8 * p : 8 * p + 8, :].reshape(-1, COLS)
        for n, part in enumerate(zip_rows(even, odd)):
            grad[:, pl.ds((2 * p + n) * COLS, COLS)] = part
    i = lax.broadcasted_iota(jnp.int32, (groups, groups * NARROW), 0)
    j = lax.broadcasted_iota(jnp.int32, (groups, groups * NARROW), 1)
    flat = [jnp.transpose(home[pl.ds(rows + n, groups, stride=block), :], (1, 0)) for n in range(3)]
    total = jnp.zeros(second.shape, f32)
    scalars = jnp.zeros((8, groups * NARROW), f32)
    line = lax.broadcasted_iota(jnp.int32, scalars.shape, 0)
    for c in range(NARROW):
        place = (j == NARROW * i + c).astype(f32)
        mine = flat[c // 2][(c % 2) * order : (c % 2 + 1) * order]
        total = total + jnp.dot(mine, place, precision=highest, preferred_element_type=f32)
        moved = jnp.dot(flat[2][:8], place, precision=highest, preferred_element_type=f32)
        scalars = scalars + jnp.where(line % NARROW == c, moved, 0.0)
    second[...] = total
    decay[...] = jnp.sum(scalars[:NARROW], axis=0, keepdims=True)
    skip[...] = jnp.sum(scalars[NARROW:], axis=0, keepdims=True)


def local(signal, cotangent, first_layer, second_layer, decay_rate, skip_gain):
    groups = lax.axis_size("batch")
    place = lax.axis_index("batch")
    side = lax.axis_index("chan")
    sides = lax.axis_size("chan")
    embed, order = first_layer.shape
    t = make_tables(embed)
    vmem = pl.BlockSpec(memory_space=pltpu.VMEM)
    smem = pl.BlockSpec(memory_space=pltpu.SMEM)
    shape = jax.ShapeDtypeStruct
    rows = signal.shape[1] // COLS * NARROW

    def call(body, name, outs, specs, args, mib, flops=0, scratch=()):
        return pl.pallas_call(
            body,
            out_shape=outs,
            in_specs=specs,
            out_specs=(vmem,) * len(outs),
            scratch_shapes=[pltpu.VMEM(s, f32) for s in scratch],
            compiler_params=pltpu.CompilerParams(vmem_limit_bytes=mib << 20),
            cost_estimate=pl.CostEstimate(flops=flops, bytes_accessed=0, transcendentals=0),
            name=name,
        )(*args)

    (sent,) = call(
        pack_kernel, "pack", (shape((groups // 2, 2, 2 * rows, COLS), f32),), [vmem] * 2,
        (signal, cotangent), 8,
    )
    spread = lax.all_to_all(
        sent.reshape(groups, 2 * rows, COLS), "batch", split_axis=0, concat_axis=0, tiled=True
    ).reshape(-1, COLS)

    columns = lax.dynamic_slice_in_dim(second_layer, place * NARROW, NARROW, 1)
    rates = lax.dynamic_slice_in_dim(decay_rate, place * NARROW, NARROW, 0)
    gains = lax.dynamic_slice_in_dim(skip_gain, place * NARROW, NARROW, 0)
    weights = jnp.pad(first_layer.T * (0.5 / math.pi), ((0, 0), (0, COLS // 2 - embed)))
    weights = jnp.concatenate([weights, weights], axis=1)

    cube = shape((order, ROWS, COLS), f32)
    four = shape((NARROW, ROWS, COLS), f32)
    wide = shape((NARROW, ROWS, 2 * COLS), f32)
    basis, slope, filt, window, norms, spectra = call(
        filter_kernel, "make_filter",
        (cube, cube, four, four, shape((NARROW, COLS), f32), wide),
        [vmem, smem, smem] + [vmem] * 6,
        (
            weights, columns, rates, t["rows"], t["spread"],
            t["forward_left"], t["forward_right"], t["twist_cos"], t["twist_sin"],
        ),
        FILTER_MIB, flops=20_000_000_000,
    )
    small, first, cotan = call(
        main_kernel, "correlate",
        (shape((3, COLS), f32), shape((20, COLS), f32), wide),
        [vmem, smem] + [vmem] * 13,
        (
            spread, columns, basis, slope, filt, window, norms, t["rows"], t["gather"],
            t["forward_left"], t["forward_right"], t["inverse_left"], t["inverse_right"],
            t["twist_cos"], t["twist_sin"],
        ),
        MAIN_MIB, flops=10_000_000_000,
        scratch=(
            (NARROW, ROWS, COLS), (NARROW, ROWS, 2 * COLS), (NARROW * order, COLS), (order, COLS)
        ),
    )

    quarter = first.shape[0] // sides
    pieces = [lax.dynamic_slice_in_dim(first, side * quarter, quarter, 0)]
    for step in range(1, sides):
        ring = [(i, (i + step) % sides) for i in range(sides)]
        piece = lax.dynamic_slice_in_dim(first, (side + step) % sides * quarter, quarter, 0)
        pieces.append(lax.ppermute(piece, "chan", ring))
    (grad,) = call(
        input_kernel, "input_grad", (shape((groups * rows, COLS), f32),),
        [vmem, smem] + [vmem] * 6,
        (
            spread, gains, spectra, cotan, t["inverse_left"], t["inverse_right"],
            t["twist_cos"], t["twist_sin"],
        ),
        16, flops=4_000_000_000,
    )
    (back,) = call(
        join_kernel, "join", (shape((groups, rows + 8, COLS), f32),), [vmem] * 6,
        (grad, small, *pieces), 8, scratch=((8, COLS),),
    )
    home = lax.all_to_all(back, "batch", split_axis=0, concat_axis=0, tiled=True)

    mine = home[:, rows + 3 :].sum(0)
    gathered = [mine]
    for step in range(1, sides):
        ring = [((i + step) % sides, i) for i in range(sides)]
        gathered.append(lax.ppermute(mine, "chan", ring))
    input_grad, second_grad, decay_grad, skip_grad = call(
        unpack_kernel, "unpack",
        (
            shape(signal.shape, f32), shape(second_layer.shape, f32),
            shape((1,) + decay_rate.shape, f32), shape((1,) + skip_gain.shape, f32),
        ),
        [vmem] * 2, (home.reshape(groups // 2, 2, -1, COLS), home.reshape(-1, COLS)), 8,
        flops=1_000_000_000,
    )
    twice = jnp.concatenate(gathered + gathered, axis=0)
    ordered = lax.dynamic_slice_in_dim(
        twice, (sides - side) % sides * quarter, sides * quarter, 0
    )
    first_grad = jnp.concatenate([ordered[:, :order], ordered[:, order:]], axis=0)[:embed]
    return (input_grad, first_grad, second_grad, decay_grad[0], skip_grad[0])


def solution(mesh):
    placed = (P("chan", "batch"), P("chan", "batch"), P(), P(None, "chan"), P("chan"), P("chan"))
    return jax.shard_map(
        local,
        mesh=mesh,
        in_specs=placed,
        out_specs=(P("chan", "batch"), P(), P(None, "chan"), P("chan"), P("chan")),
        check_vma=False,
    )
```

```python
import math

import jax
import jax.numpy as jnp
import numpy as np
from jax import lax
from jax.experimental import pallas as pl
from jax.experimental.pallas import tpu as pltpu
from jax.sharding import PartitionSpec as P

ROWS = 256
COLS = 128
LENGTH = ROWS * COLS
NARROW = 4
FILTER_BATCH = 16
TAIL_BATCH = 32
TINY = 1e-06
f32 = jnp.float32
bf16 = jnp.bfloat16
highest = lax.Precision.HIGHEST


def halves(x):
    high = x.astype(bf16)
    low = (x - high.astype(np.float64)).astype(bf16)
    return high, low


SIN = (6.28318528, -10.33542017, 5.100155046, -1.196582571, 0.1553153206)
COS = (0.9999999532, -4.934792831, 4.058411353, -1.331876568, 0.2196896111)


def make_tables(embed):
    a = np.arange(ROWS)
    k = np.arange(ROWS)
    m = np.arange(COLS)
    bands = embed // 2
    turn = np.pi * ((a[None, :] * (4 * k + 1)[:, None]) % (4 * ROWS)) / (2 * ROWS)
    first = np.concatenate([np.cos(turn), -np.sin(turn)], axis=0)
    twist = np.pi * (4 * k + 1)[:, None] * m[None, :] / (2 * LENGTH)
    angle = 2.0 * np.pi * ((m[:, None] * m[None, :]) % COLS) / COLS
    c, s = np.cos(angle), np.sin(angle)
    second = np.concatenate(
        [np.concatenate([c, -s], axis=1), np.concatenate([s, c], axis=1)], axis=0
    )
    high, low = halves(first)
    forward_left = np.concatenate([high, low], axis=1)
    inverse_left = np.concatenate([high.T, low.T], axis=1)
    high, low = halves(second)
    forward_right = np.concatenate([high, low], axis=0)
    inverse_right = np.concatenate([high.T, low.T], axis=0)
    rows = np.zeros((ROWS, COLS))
    lanes = np.zeros((COLS, COLS))
    half = COLS // 2
    rows[:, 0] = a * COLS / LENGTH
    lanes[0] = 1.0
    rows[:, half] = 1.0
    lanes[half] = m / LENGTH
    for b in range(1, bands + 1):
        big = 2.0 * np.pi * ((b * COLS * a) % LENGTH) / LENGTH
        small = 2.0 * np.pi * b * m / LENGTH
        rows[:, b] = np.cos(big)
        rows[:, half + b] = -np.sin(big)
        rows[:, bands + b] = np.sin(big)
        rows[:, half + bands + b] = np.cos(big)
        lanes[b] = np.cos(small)
        lanes[half + b] = np.sin(small)
        lanes[bands + b] = np.cos(small)
        lanes[half + bands + b] = np.sin(small)
    high, low = halves(lanes.T)
    gather = np.concatenate([high, low], axis=0)
    high, low = halves(lanes)
    lowest = (lanes - high.astype(np.float64) - low.astype(np.float64)).astype(bf16)
    spread = np.concatenate([high, low, lowest, high, low, high], axis=0)
    return dict(
        forward_left=forward_left,
        inverse_left=inverse_left,
        forward_right=forward_right,
        inverse_right=inverse_right,
        twist_cos=np.cos(twist).astype(np.float32),
        twist_sin=np.sin(twist).astype(np.float32),
        rows=rows.astype(np.float32),
        spread=spread,
        gather=gather,
    )


def split(x):
    high = x.astype(bf16)
    low = (x - high.astype(f32)).astype(bf16)
    return high, low


def mm(left, right):
    return lax.dot_general(left, right, (((1,), (0,)), ((), ())), preferred_element_type=f32)


def dot_rows(table, x):
    high, low = split(x)
    left = jnp.concatenate([table, table[:, : x.shape[0]]], axis=1)
    return mm(left, jnp.concatenate([high, high, low], axis=0))


def dot_cols(x, table):
    high, low = split(x)
    count = x.shape[1]
    right = jnp.concatenate([table[:count], table], axis=0)
    return mm(jnp.concatenate([high, low, high], axis=1), right)


def forward_pair(x, y, left, right, twist_cos, twist_sin):
    u = dot_rows(left, jnp.concatenate([x, y], axis=1))
    spectra = []
    for n in range(2):
        re = u[:ROWS, n * COLS : (n + 1) * COLS]
        im = u[ROWS:, n * COLS : (n + 1) * COLS]
        v = jnp.concatenate(
            [re * twist_cos + im * twist_sin, im * twist_cos - re * twist_sin], axis=1
        )
        spectra.append(dot_cols(v, right))
    return spectra


def times_conj(f, c):
    fr, fi, cr, ci = f[:, :COLS], f[:, COLS:], c[:, :COLS], c[:, COLS:]
    return jnp.concatenate([fr * cr + fi * ci, fr * ci - fi * cr], axis=1)


def inverse_pair(g, h, left, right, twist_cos, twist_sin):
    parts = []
    for x in (g, h):
        w = dot_cols(x, right)
        re, im = w[:, :COLS], w[:, COLS:]
        parts.append(
            jnp.concatenate(
                [re * twist_cos - im * twist_sin, im * twist_cos + re * twist_sin], axis=0
            )
        )
    y = dot_rows(left, jnp.concatenate(parts, axis=1))
    return y[:, :COLS], y[:, COLS:]


def sin_and_cos(x):
    r = x - ((x + 12582912.0) - 12582912.0)
    z = r * r
    s = SIN[4]
    for n in (3, 2, 1, 0):
        s = s * z + SIN[n]
    s = s * r
    c = COS[4]
    for n in (3, 2, 1, 0):
        c = c * z + COS[n]
    return s * c, 1.0 - 0.5 * (s * s)


def fraction_rows(count, offset):
    a = lax.broadcasted_iota(jnp.int32, (count, COLS), 0) + offset
    m = lax.broadcasted_iota(jnp.int32, (count, COLS), 1)
    return (a * COLS + m).astype(f32) * (1.0 / LENGTH)


def zip_rows(x, y):
    low = lax.broadcasted_iota(jnp.int32, x.shape, 0) % 8 < 4
    count = x.shape[0]
    return (
        jnp.where(low, x, pltpu.roll(y, 4, 0)),
        jnp.where(low, pltpu.roll(x, count - 4, 0), y),
    )


def pack_kernel(signal, cotangent, out):
    for q in range(signal.shape[1] // COLS):
        here = pl.ds(q * COLS, COLS)
        for n, part in enumerate(zip_rows(signal[:, here], cotangent[:, here])):
            out[:, n, 8 * q : 8 * q + 8, :] = part.reshape(-1, 8, COLS)


def filter_kernel(
    weights, columns, rates, rows, spread, left, right, tcos, tsin,
    high_out, low_out, slope_out, filt_out, window_out, norms, spectra_out,
    high, low, slope, filt, window, spectra, raws, wins, sems,
):
    order = weights.shape[0]
    batch = FILTER_BATCH
    wide = batch * COLS

    def copy(source, target, n, here=None):
        if here is not None:
            source, target = source.at[:, here], target.at[:, here]
        return pltpu.make_async_copy(source, target, sems.at[n])

    mixer = jnp.concatenate(split(columns[...]), axis=0)
    lane = lax.broadcasted_iota(jnp.int32, (8, COLS), 1)

    def block(n, total):
        scaled = jnp.concatenate(
            [weights[...] * rows[pl.ds(n * batch + i, 1), :] for i in range(batch)], axis=0
        )
        one = scaled.astype(bf16)
        rest = scaled - one.astype(f32)
        two = rest.astype(bf16)
        three = (rest - two.astype(f32)).astype(bf16)
        turns = mm(jnp.concatenate([one, one, one, two, two, three], axis=1), spread[...])
        for i in range(batch):
            here = pl.ds(pl.multiple_of(n * wide + i * COLS, COLS), COLS)
            s, c = sin_and_cos(turns[i * order : (i + 1) * order])
            slope[:, here] = c
            s_high, s_low = split(s)
            high[:, here] = s_high
            low[:, here] = s_low
        here = pl.ds(pl.multiple_of(n * wide, wide), wide)
        copy(high, high_out, 0, here).start()
        copy(low, low_out, 1, here).start()
        copy(slope, slope_out, 2, here).start()
        p = mm(mixer, high[:, here])
        r = mm(mixer, low[:, here])
        mixed = p[:8] + p[8:] + (r[:8] + r[8:])
        for i in range(batch):
            a = n * batch + i
            fraction = (a * COLS + lane).astype(f32) * (1.0 / LENGTH)
            win = jnp.exp(-rates[...] * fraction)
            raw = win * mixed[:, i * COLS : (i + 1) * COLS]
            raws[pl.ds(pl.multiple_of(a * 8, 8), 8), :] = raw
            wins[pl.ds(pl.multiple_of(a * 8, 8), 8), :] = win
            total = total + raw * raw
        return total

    total = lax.fori_loop(0, ROWS // batch, block, jnp.zeros((8, COLS), f32))
    norm = jnp.sqrt(jnp.sum(total, axis=1, keepdims=True) + TINY)
    norms[...] = jnp.broadcast_to(norm, norms.shape)
    for c in range(NARROW):
        filt[c] = raws[pl.ds(c, ROWS, stride=8), :] / norms[pl.ds(c, 1), :]
        window[c] = wins[pl.ds(c, ROWS, stride=8), :]
    copy(filt, filt_out, 3).start()
    copy(window, window_out, 4).start()
    for c in range(0, NARROW, 2):
        x, y = forward_pair(filt[c], filt[c + 1], left[...], right[...], tcos[...], tsin[...])
        spectra[c] = x
        spectra[c + 1] = y
    copy(spectra, spectra_out, 5).start()
    copy(high, high_out, 0).wait()
    copy(low, low_out, 1).wait()
    copy(slope, slope_out, 2).wait()
    copy(filt, filt_out, 3).wait()
    copy(window, window_out, 4).wait()
    copy(spectra, spectra_out, 5).wait()


def main_kernel(
    both, columns, norms, rows, gather, fleft, fright, ileft, iright, tcos, tsin,
    high_in, low_in, slope_in, filt_in, window_in,
    small, first, cotan,
    high, low, slope, filt, window, dmix, product, sems,
):
    order = slope.shape[0]
    factor = 1.0 / math.sqrt(LENGTH)
    copies = [
        pltpu.make_async_copy(source, target, sems.at[n])
        for n, (source, target) in enumerate((
            (filt_in, filt), (window_in, window),
            (high_in, high), (low_in, low), (slope_in, slope),
        ))
    ]
    for one in copies:
        one.start()
    lane = lax.broadcasted_iota(jnp.int32, (1, COLS), 1)
    scalars = jnp.zeros((1, COLS), f32)
    fraction = fraction_rows(ROWS, 0)
    dmix[...] = jnp.zeros(dmix.shape, f32)
    for c in range(NARROW):
        x = both[pl.ds(c, ROWS, stride=2 * NARROW), :]
        y = both[pl.ds(NARROW + c, ROWS, stride=2 * NARROW), :]
        skip = factor * jnp.sum(x * y, keepdims=True)
        scalars = jnp.where(lane == NARROW + c, skip, scalars)
        val, cot = forward_pair(x, y, fleft[...], fright[...], tcos[...], tsin[...])
        cotan[c] = cot
        product[c] = times_conj(val, cot)
    copies[0].wait()
    copies[1].wait()
    for c in range(0, NARROW, 2):
        pair = inverse_pair(
            product[c], product[c + 1], ileft[...], iright[...], tcos[...], tsin[...]
        )
        for n in range(2):
            i = c + n
            dfilt = pair[n] * (factor / LENGTH)
            project = jnp.sum(filt[i] * dfilt, keepdims=True)
            norm = norms[pl.ds(i, 1), :][:, :1]
            draw = (dfilt - filt[i] * project) / norm
            decay = -jnp.sum(draw * filt[i] * fraction, keepdims=True) * norm
            dmix[pl.ds(i, ROWS, stride=8), :] = draw * window[i]
            scalars = jnp.where(lane == i, decay, scalars)
    lanes = lax.broadcasted_iota(jnp.int32, columns.shape, 1)
    col_high = columns[...].astype(bf16).astype(f32)
    mixer = jnp.where(lanes // 8 == 2, columns[...] - col_high, col_high).astype(bf16)[:, :32]
    copies[2].wait()
    copies[3].wait()
    copies[4].wait()
    batch = TAIL_BATCH
    wide = batch * COLS
    contract = (((1,), (1,)), ((), ()))

    def tail(n, carry):
        firsts, seconds = carry
        stack = []
        for i in range(batch):
            d = dmix[pl.ds(pl.multiple_of((n * batch + i) * 8, 8), 8), :]
            d_high = d.astype(bf16).astype(f32)
            stack.append(
                jnp.concatenate([d_high, d - d_high, d_high, jnp.zeros_like(d)], axis=0).astype(bf16)
            )
        stack = jnp.concatenate(stack, axis=1)
        here = pl.ds(pl.multiple_of(n * wide, wide), wide)
        for part in (high, low):
            seconds = seconds + lax.dot_general(
                stack[:16], part[:, here], contract, preferred_element_type=f32
            )
        q = mm(mixer, stack) * slope[:, here]
        q = jnp.concatenate([q[:, i * COLS : (i + 1) * COLS] for i in range(batch)], axis=0)
        r = dot_cols(q, gather[...])
        for i in range(batch):
            firsts = firsts + r[i * order : (i + 1) * order] * rows[pl.ds(n * batch + i, 1), :]
        return firsts, seconds

    firsts, seconds = lax.fori_loop(
        0, ROWS // batch, tail, (jnp.zeros((order, COLS), f32), jnp.zeros((16, order), f32))
    )
    seconds = seconds[:8] + seconds[8:]
    small[:1] = jnp.concatenate([seconds[0:1], seconds[1:2]], axis=1)
    small[1:2] = jnp.concatenate([seconds[2:3], seconds[3:4]], axis=1)
    small[2:3] = scalars
    turned = jnp.transpose(firsts, (1, 0))
    half = COLS // 2
    folded = turned[:half] + turned[half:]
    first[...] = jnp.concatenate([folded[:20], folded[20:40]], axis=1)


def input_kernel(both, gains, spectra, cotan, ileft, iright, tcos, tsin, grad):
    for c in range(0, NARROW, 2):
        pair = inverse_pair(
            times_conj(spectra[c], cotan[c]), times_conj(spectra[c + 1], cotan[c + 1]),
            ileft[...], iright[...], tcos[...], tsin[...],
        )
        for n in range(2):
            i = c + n
            y = both[pl.ds(NARROW + i, ROWS, stride=2 * NARROW), :]
            grad[pl.ds(i, ROWS, stride=NARROW), :] = pair[n] * (1.0 / LENGTH) + gains[i] * y


def join_kernel(grad, small, own, one, two, three, out, tile):
    rows = grad.shape[0] // out.shape[0]
    tile[:3] = small[...]
    tile[3:] = own[...] + one[...] + two[...] + three[...]
    out[:, :rows, :] = grad[...].reshape(out.shape[0], rows, COLS)
    out[:, rows:, :] = jnp.broadcast_to(tile[...][None], (out.shape[0],) + tile.shape)


def unpack_kernel(pairs, home, grad, second, decay, skip):
    groups = grad.shape[0] // NARROW
    order = second.shape[0]
    rows = grad.shape[1] // COLS * NARROW
    block = rows + 8
    for p in range(rows // 8):
        even = pairs[:, 0, 8 * p : 8 * p + 8, :].reshape(-1, COLS)
        odd = pairs[:, 1, 8 * p : 8 * p + 8, :].reshape(-1, COLS)
        for n, part in enumerate(zip_rows(even, odd)):
            grad[:, pl.ds((2 * p + n) * COLS, COLS)] = part
    i = lax.broadcasted_iota(jnp.int32, (groups, groups * NARROW), 0)
    j = lax.broadcasted_iota(jnp.int32, (groups, groups * NARROW), 1)
    flat = [jnp.transpose(home[pl.ds(rows + n, groups, stride=block), :], (1, 0)) for n in range(3)]
    total = jnp.zeros(second.shape, f32)
    scalars = jnp.zeros((8, groups * NARROW), f32)
    line = lax.broadcasted_iota(jnp.int32, scalars.shape, 0)
    for c in range(NARROW):
        place = (j == NARROW * i + c).astype(f32)
        mine = flat[c // 2][(c % 2) * order : (c % 2 + 1) * order]
        total = total + jnp.dot(mine, place, precision=highest, preferred_element_type=f32)
        moved = jnp.dot(flat[2][:8], place, precision=highest, preferred_element_type=f32)
        scalars = scalars + jnp.where(line % NARROW == c, moved, 0.0)
    second[...] = total
    decay[...] = jnp.sum(scalars[:NARROW], axis=0, keepdims=True)
    skip[...] = jnp.sum(scalars[NARROW:], axis=0, keepdims=True)


def local(signal, cotangent, first_layer, second_layer, decay_rate, skip_gain):
    groups = lax.axis_size("batch")
    place = lax.axis_index("batch")
    side = lax.axis_index("chan")
    sides = lax.axis_size("chan")
    embed, order = first_layer.shape
    t = make_tables(embed)
    vmem = pl.BlockSpec(memory_space=pltpu.VMEM)
    smem = pl.BlockSpec(memory_space=pltpu.SMEM)
    hbm = pl.BlockSpec(memory_space=pltpu.HBM)
    shape = jax.ShapeDtypeStruct
    rows = signal.shape[1] // COLS * NARROW

    def call(body, name, outs, specs, args, mib, flops=0, scratch=(), out_specs=None):
        return pl.pallas_call(
            body,
            out_shape=outs,
            in_specs=specs,
            out_specs=out_specs or (vmem,) * len(outs),
            scratch_shapes=list(scratch),
            compiler_params=pltpu.CompilerParams(vmem_limit_bytes=mib << 20),
            cost_estimate=pl.CostEstimate(flops=flops, bytes_accessed=0, transcendentals=0),
            name=name,
        )(*args)

    (sent,) = call(
        pack_kernel, "pack", (shape((groups // 2, 2, 2 * rows, COLS), f32),), [vmem] * 2,
        (signal, cotangent), 8,
    )
    spread = lax.all_to_all(
        sent.reshape(groups, 2 * rows, COLS), "batch", split_axis=0, concat_axis=0, tiled=True
    ).reshape(-1, COLS)

    columns = lax.dynamic_slice_in_dim(second_layer, place * NARROW, NARROW, 1)
    rates = lax.dynamic_slice_in_dim(decay_rate, place * NARROW, NARROW, 0)
    gains = lax.dynamic_slice_in_dim(skip_gain, place * NARROW, NARROW, 0)
    weights = jnp.pad(first_layer.T * (0.5 / math.pi), ((0, 0), (0, COLS // 2 - embed)))
    weights = jnp.concatenate([weights, weights], axis=1)
    eight = jnp.pad(columns, ((0, 0), (0, 8 - NARROW)))
    tiled = jnp.pad(jnp.concatenate([eight] * 3, axis=1), ((0, 0), (0, COLS - 24)))
    rates = jnp.broadcast_to(jnp.pad(rates, (0, 8 - NARROW))[:, None], (8, COLS))

    full = (order, LENGTH)
    four = (NARROW, ROWS, COLS)
    wide = (NARROW, ROWS, 2 * COLS)
    kept = ((full, bf16), (full, bf16), (full, f32), (four, f32), (four, f32))
    tall = (ROWS * 8, COLS)
    *state, norms, spectra = call(
        filter_kernel, "make_filter",
        tuple(shape(*k) for k in kept) + (shape((8, COLS), f32), shape(wide, f32)),
        [vmem] * 9,
        (
            weights, eight.T, rates, t["rows"], t["spread"],
            t["forward_left"], t["forward_right"], t["twist_cos"], t["twist_sin"],
        ),
        40, flops=20_000_000_000,
        scratch=[pltpu.VMEM(*k) for k in kept] + [
            pltpu.VMEM(wide, f32), pltpu.VMEM(tall, f32), pltpu.VMEM(tall, f32),
            pltpu.SemaphoreType.DMA((6,)),
        ],
        out_specs=(hbm,) * 5 + (vmem, hbm),
    )
    small, first, cotan = call(
        main_kernel, "correlate",
        (shape((3, COLS), f32), shape((20, COLS), f32), shape(wide, f32)),
        [vmem] * 11 + [hbm] * 5,
        (
            spread, tiled, norms, t["rows"], t["gather"],
            t["forward_left"], t["forward_right"], t["inverse_left"], t["inverse_right"],
            t["twist_cos"], t["twist_sin"], *state,
        ),
        40, flops=10_000_000_000,
        scratch=[pltpu.VMEM(*k) for k in kept] + [
            pltpu.VMEM(tall, f32), pltpu.VMEM(wide, f32), pltpu.SemaphoreType.DMA((5,)),
        ],
    )

    quarter = first.shape[0] // sides
    pieces = [lax.dynamic_slice_in_dim(first, side * quarter, quarter, 0)]
    for step in range(1, sides):
        ring = [(i, (i + step) % sides) for i in range(sides)]
        piece = lax.dynamic_slice_in_dim(first, (side + step) % sides * quarter, quarter, 0)
        pieces.append(lax.ppermute(piece, "chan", ring))
    (grad,) = call(
        input_kernel, "input_grad", (shape((groups * rows, COLS), f32),),
        [vmem, smem] + [vmem] * 6,
        (
            spread, gains, spectra, cotan, t["inverse_left"], t["inverse_right"],
            t["twist_cos"], t["twist_sin"],
        ),
        16, flops=4_000_000_000,
    )
    (back,) = call(
        join_kernel, "join", (shape((groups, rows + 8, COLS), f32),), [vmem] * 6,
        (grad, small, *pieces), 8, scratch=[pltpu.VMEM((8, COLS), f32)],
    )
    home = lax.all_to_all(back, "batch", split_axis=0, concat_axis=0, tiled=True)

    mine = home[:, rows + 3 :].sum(0)
    gathered = [mine]
    for step in range(1, sides):
        ring = [((i + step) % sides, i) for i in range(sides)]
        gathered.append(lax.ppermute(mine, "chan", ring))
    input_grad, second_grad, decay_grad, skip_grad = call(
        unpack_kernel, "unpack",
        (
            shape(signal.shape, f32), shape(second_layer.shape, f32),
            shape((1,) + decay_rate.shape, f32), shape((1,) + skip_gain.shape, f32),
        ),
        [vmem] * 2, (home.reshape(groups // 2, 2, -1, COLS), home.reshape(-1, COLS)), 8,
        flops=1_000_000_000,
    )
    twice = jnp.concatenate(gathered + gathered, axis=0)
    ordered = lax.dynamic_slice_in_dim(
        twice, (sides - side) % sides * quarter, sides * quarter, 0
    )
    first_grad = jnp.concatenate([ordered[:, :order], ordered[:, order:]], axis=0)[:embed]
    return (input_grad, first_grad, second_grad, decay_grad[0], skip_grad[0])


def solution(mesh):
    placed = (P("chan", "batch"), P("chan", "batch"), P(), P(None, "chan"), P("chan"), P("chan"))
    return jax.shard_map(
        local,
        mesh=mesh,
        in_specs=placed,
        out_specs=(P("chan", "batch"), P(), P(None, "chan"), P("chan"), P("chan")),
        check_vma=False,
    )
```

```python
import math

import jax
import jax.numpy as jnp
import numpy as np
from jax import lax
from jax.experimental import pallas as pl
from jax.experimental.pallas import tpu as pltpu
from jax.sharding import PartitionSpec as P

ROWS = 256
COLS = 128
LENGTH = ROWS * COLS
NARROW = 4
FILTER_BATCH = 16
TAIL_BATCH = 32
TINY = 1e-06
f32 = jnp.float32
bf16 = jnp.bfloat16
highest = lax.Precision.HIGHEST


def halves(x):
    high = x.astype(bf16)
    low = (x - high.astype(np.float64)).astype(bf16)
    return high, low


SIN = (6.28318528, -10.33542017, 5.100155046, -1.196582571, 0.1553153206)
COS = (0.9999999532, -4.934792831, 4.058411353, -1.331876568, 0.2196896111)


def make_tables(embed):
    a = np.arange(ROWS)
    k = np.arange(ROWS)
    m = np.arange(COLS)
    bands = embed // 2
    turn = np.pi * ((a[None, :] * (4 * k + 1)[:, None]) % (4 * ROWS)) / (2 * ROWS)
    first = np.concatenate([np.cos(turn), -np.sin(turn)], axis=0)
    twist = np.pi * (4 * k + 1)[:, None] * m[None, :] / (2 * LENGTH)
    angle = 2.0 * np.pi * ((m[:, None] * m[None, :]) % COLS) / COLS
    c, s = np.cos(angle), np.sin(angle)
    second = np.concatenate(
        [np.concatenate([c, -s], axis=1), np.concatenate([s, c], axis=1)], axis=0
    )
    high, low = halves(first)
    forward_left = np.concatenate([high, low], axis=1)
    inverse_left = np.concatenate([high.T, low.T], axis=1)
    high, low = halves(second)
    forward_right = np.concatenate([high, low], axis=0)
    inverse_right = np.concatenate([high.T, low.T], axis=0)
    rows = np.zeros((ROWS, COLS))
    lanes = np.zeros((COLS, COLS))
    half = COLS // 2
    rows[:, 0] = a * COLS / LENGTH
    lanes[0] = 1.0
    rows[:, half] = 1.0
    lanes[half] = m / LENGTH
    for b in range(1, bands + 1):
        big = 2.0 * np.pi * ((b * COLS * a) % LENGTH) / LENGTH
        small = 2.0 * np.pi * b * m / LENGTH
        rows[:, b] = np.cos(big)
        rows[:, half + b] = -np.sin(big)
        rows[:, bands + b] = np.sin(big)
        rows[:, half + bands + b] = np.cos(big)
        lanes[b] = np.cos(small)
        lanes[half + b] = np.sin(small)
        lanes[bands + b] = np.cos(small)
        lanes[half + bands + b] = np.sin(small)
    high, low = halves(lanes.T)
    gather = np.concatenate([high, low], axis=0)
    high, low = halves(lanes)
    lowest = (lanes - high.astype(np.float64) - low.astype(np.float64)).astype(bf16)
    spread = np.concatenate([high, low, lowest, high, low, high], axis=0)
    return dict(
        forward_left=forward_left,
        inverse_left=inverse_left,
        forward_right=forward_right,
        inverse_right=inverse_right,
        twist_cos=np.cos(twist).astype(np.float32),
        twist_sin=np.sin(twist).astype(np.float32),
        rows=rows.astype(np.float32),
        spread=spread,
        gather=gather,
    )


def split(x):
    high = x.astype(bf16)
    low = (x - high.astype(f32)).astype(bf16)
    return high, low


def mm(left, right):
    return lax.dot_general(left, right, (((1,), (0,)), ((), ())), preferred_element_type=f32)


def dot_rows(table, x):
    high, low = split(x)
    left = jnp.concatenate([table, table[:, : x.shape[0]]], axis=1)
    return mm(left, jnp.concatenate([high, high, low], axis=0))


def dot_cols(x, table):
    high, low = split(x)
    count = x.shape[1]
    right = jnp.concatenate([table[:count], table], axis=0)
    return mm(jnp.concatenate([high, low, high], axis=1), right)


def forward_pair(x, y, left, right, twist_cos, twist_sin):
    u = dot_rows(left, jnp.concatenate([x, y], axis=1))
    spectra = []
    for n in range(2):
        re = u[:ROWS, n * COLS : (n + 1) * COLS]
        im = u[ROWS:, n * COLS : (n + 1) * COLS]
        v = jnp.concatenate(
            [re * twist_cos + im * twist_sin, im * twist_cos - re * twist_sin], axis=1
        )
        spectra.append(dot_cols(v, right))
    return spectra


def times_conj(f, c):
    fr, fi, cr, ci = f[:, :COLS], f[:, COLS:], c[:, :COLS], c[:, COLS:]
    return jnp.concatenate([fr * cr + fi * ci, fr * ci - fi * cr], axis=1)


def inverse_pair(g, h, left, right, twist_cos, twist_sin):
    parts = []
    for x in (g, h):
        w = dot_cols(x, right)
        re, im = w[:, :COLS], w[:, COLS:]
        parts.append(
            jnp.concatenate(
                [re * twist_cos - im * twist_sin, im * twist_cos + re * twist_sin], axis=0
            )
        )
    y = dot_rows(left, jnp.concatenate(parts, axis=1))
    return y[:, :COLS], y[:, COLS:]


def sin_and_cos(x):
    r = x - ((x + 12582912.0) - 12582912.0)
    z = r * r
    s = SIN[4]
    for n in (3, 2, 1, 0):
        s = s * z + SIN[n]
    s = s * r
    c = COS[4]
    for n in (3, 2, 1, 0):
        c = c * z + COS[n]
    return s * c, 1.0 - 0.5 * (s * s)


def fraction_rows(count, offset):
    a = lax.broadcasted_iota(jnp.int32, (count, COLS), 0) + offset
    m = lax.broadcasted_iota(jnp.int32, (count, COLS), 1)
    return (a * COLS + m).astype(f32) * (1.0 / LENGTH)


def zip_rows(x, y):
    low = lax.broadcasted_iota(jnp.int32, x.shape, 0) % 8 < 4
    count = x.shape[0]
    return (
        jnp.where(low, x, pltpu.roll(y, 4, 0)),
        jnp.where(low, pltpu.roll(x, count - 4, 0), y),
    )


def pack_kernel(signal, cotangent, out, values, turned, into, outof):
    quarters = signal.shape[1] // COLS
    reads, writes = [], []
    for q in range(quarters):
        here = pl.ds(q * COLS, COLS)
        for n, source in enumerate((signal, cotangent)):
            copy = pltpu.make_async_copy(source.at[:, here], values.at[q, n], into.at[q, n])
            copy.start()
            reads.append(copy)
    for q in range(quarters):
        for copy in reads[2 * q : 2 * q + 2]:
            copy.wait()
        for n, part in enumerate(zip_rows(values[q, 0], values[q, 1])):
            turned[q, :, n] = part.reshape(-1, 8, COLS)
        copy = pltpu.make_async_copy(
            turned.at[q], out.at[:, :, pl.ds(8 * q, 8), :], outof.at[q]
        )
        copy.start()
        writes.append(copy)
    for copy in writes:
        copy.wait()


def filter_kernel(
    weights, columns, rates, rows, spread, left, right, tcos, tsin,
    high_out, low_out, slope_out, filt_out, window_out, norms, spectra_out,
    high, low, slope, filt, window, spectra, raws, wins, sems,
):
    order = weights.shape[0]
    batch = FILTER_BATCH
    wide = batch * COLS

    def copy(source, target, n, here=None):
        if here is not None:
            source, target = source.at[:, here], target.at[:, here]
        return pltpu.make_async_copy(source, target, sems.at[n])

    mixer = jnp.concatenate(split(columns[...]), axis=0)
    lane = lax.broadcasted_iota(jnp.int32, (8, COLS), 1)

    def block(n, total):
        scaled = jnp.concatenate(
            [weights[...] * rows[pl.ds(n * batch + i, 1), :] for i in range(batch)], axis=0
        )
        one = scaled.astype(bf16)
        rest = scaled - one.astype(f32)
        two = rest.astype(bf16)
        three = (rest - two.astype(f32)).astype(bf16)
        turns = mm(jnp.concatenate([one, one, one, two, two, three], axis=1), spread[...])
        for i in range(batch):
            here = pl.ds(pl.multiple_of(n * wide + i * COLS, COLS), COLS)
            s, c = sin_and_cos(turns[i * order : (i + 1) * order])
            slope[:, here] = c
            s_high, s_low = split(s)
            high[:, here] = s_high
            low[:, here] = s_low
        here = pl.ds(pl.multiple_of(n * wide, wide), wide)
        copy(high, high_out, 0, here).start()
        copy(low, low_out, 1, here).start()
        copy(slope, slope_out, 2, here).start()
        p = mm(mixer, high[:, here])
        r = mm(mixer, low[:, here])
        mixed = p[:8] + p[8:] + (r[:8] + r[8:])
        for i in range(batch):
            a = n * batch + i
            fraction = (a * COLS + lane).astype(f32) * (1.0 / LENGTH)
            win = jnp.exp(-rates[...] * fraction)
            raw = win * mixed[:, i * COLS : (i + 1) * COLS]
            raws[pl.ds(pl.multiple_of(a * 8, 8), 8), :] = raw
            wins[pl.ds(pl.multiple_of(a * 8, 8), 8), :] = win
            total = total + raw * raw
        return total

    total = lax.fori_loop(0, ROWS // batch, block, jnp.zeros((8, COLS), f32))
    norm = jnp.sqrt(jnp.sum(total, axis=1, keepdims=True) + TINY)
    norms[...] = jnp.broadcast_to(norm, norms.shape)
    for c in range(NARROW):
        filt[c] = raws[pl.ds(c, ROWS, stride=8), :] / norms[pl.ds(c, 1), :]
        window[c] = wins[pl.ds(c, ROWS, stride=8), :]
    copy(filt, filt_out, 3).start()
    copy(window, window_out, 4).start()
    for c in range(0, NARROW, 2):
        x, y = forward_pair(filt[c], filt[c + 1], left[...], right[...], tcos[...], tsin[...])
        spectra[c] = x
        spectra[c + 1] = y
    copy(spectra, spectra_out, 5).start()
    copy(high, high_out, 0).wait()
    copy(low, low_out, 1).wait()
    copy(slope, slope_out, 2).wait()
    copy(filt, filt_out, 3).wait()
    copy(window, window_out, 4).wait()
    copy(spectra, spectra_out, 5).wait()


def main_kernel(
    both, columns, norms, rows, gather, fleft, fright, ileft, iright, tcos, tsin,
    high_in, low_in, slope_in, filt_in, window_in,
    small, first, cotan,
    high, low, slope, filt, window, dmix, product, sems,
):
    order = slope.shape[0]
    factor = 1.0 / math.sqrt(LENGTH)
    copies = [
        pltpu.make_async_copy(source, target, sems.at[n])
        for n, (source, target) in enumerate((
            (filt_in, filt), (window_in, window),
            (high_in, high), (low_in, low), (slope_in, slope),
        ))
    ]
    for one in copies:
        one.start()
    lane = lax.broadcasted_iota(jnp.int32, (1, COLS), 1)
    scalars = jnp.zeros((1, COLS), f32)
    fraction = fraction_rows(ROWS, 0)
    dmix[...] = jnp.zeros(dmix.shape, f32)
    for c in range(NARROW):
        x = both[pl.ds(c, ROWS, stride=2 * NARROW), :]
        y = both[pl.ds(NARROW + c, ROWS, stride=2 * NARROW), :]
        skip = factor * jnp.sum(x * y, keepdims=True)
        scalars = jnp.where(lane == NARROW + c, skip, scalars)
        val, cot = forward_pair(x, y, fleft[...], fright[...], tcos[...], tsin[...])
        cotan[c] = cot
        product[c] = times_conj(val, cot)
    copies[0].wait()
    copies[1].wait()
    for c in range(0, NARROW, 2):
        pair = inverse_pair(
            product[c], product[c + 1], ileft[...], iright[...], tcos[...], tsin[...]
        )
        for n in range(2):
            i = c + n
            dfilt = pair[n] * (factor / LENGTH)
            project = jnp.sum(filt[i] * dfilt, keepdims=True)
            norm = norms[pl.ds(i, 1), :][:, :1]
            draw = (dfilt - filt[i] * project) / norm
            decay = -jnp.sum(draw * filt[i] * fraction, keepdims=True) * norm
            dmix[pl.ds(i, ROWS, stride=8), :] = draw * window[i]
            scalars = jnp.where(lane == i, decay, scalars)
    lanes = lax.broadcasted_iota(jnp.int32, columns.shape, 1)
    col_high = columns[...].astype(bf16).astype(f32)
    mixer = jnp.where(lanes // 8 == 2, columns[...] - col_high, col_high).astype(bf16)[:, :32]
    copies[2].wait()
    copies[3].wait()
    copies[4].wait()
    batch = TAIL_BATCH
    wide = batch * COLS
    contract = (((1,), (1,)), ((), ()))

    def tail(n, carry):
        firsts, seconds = carry
        stack = []
        for i in range(batch):
            d = dmix[pl.ds(pl.multiple_of((n * batch + i) * 8, 8), 8), :]
            d_high = d.astype(bf16).astype(f32)
            stack.append(
                jnp.concatenate([d_high, d - d_high, d_high, jnp.zeros_like(d)], axis=0).astype(bf16)
            )
        stack = jnp.concatenate(stack, axis=1)
        here = pl.ds(pl.multiple_of(n * wide, wide), wide)
        for part in (high, low):
            seconds = seconds + lax.dot_general(
                stack[:16], part[:, here], contract, preferred_element_type=f32
            )
        q = mm(mixer, stack) * slope[:, here]
        q = jnp.concatenate([q[:, i * COLS : (i + 1) * COLS] for i in range(batch)], axis=0)
        r = dot_cols(q, gather[...])
        for i in range(batch):
            firsts = firsts + r[i * order : (i + 1) * order] * rows[pl.ds(n * batch + i, 1), :]
        return firsts, seconds

    firsts, seconds = lax.fori_loop(
        0, ROWS // batch, tail, (jnp.zeros((order, COLS), f32), jnp.zeros((16, order), f32))
    )
    seconds = seconds[:8] + seconds[8:]
    small[:1] = jnp.concatenate([seconds[0:1], seconds[1:2]], axis=1)
    small[1:2] = jnp.concatenate([seconds[2:3], seconds[3:4]], axis=1)
    small[2:3] = scalars
    turned = jnp.transpose(firsts, (1, 0))
    half = COLS // 2
    folded = turned[:half] + turned[half:]
    first[...] = jnp.concatenate([folded[:20], folded[20:40]], axis=1)


def input_kernel(both, gains, spectra, cotan, ileft, iright, tcos, tsin, grad):
    for c in range(0, NARROW, 2):
        pair = inverse_pair(
            times_conj(spectra[c], cotan[c]), times_conj(spectra[c + 1], cotan[c + 1]),
            ileft[...], iright[...], tcos[...], tsin[...],
        )
        for n in range(2):
            i = c + n
            y = both[pl.ds(NARROW + i, ROWS, stride=2 * NARROW), :]
            grad[pl.ds(i, ROWS, stride=NARROW), :] = pair[n] * (1.0 / LENGTH) + gains[i] * y


def join_kernel(grad, small, own, one, two, three, out, tile):
    rows = grad.shape[0] // out.shape[0]
    tile[:3] = small[...]
    tile[3:] = own[...] + one[...] + two[...] + three[...]
    out[:, :rows, :] = grad[...].reshape(out.shape[0], rows, COLS)
    out[:, rows:, :] = jnp.broadcast_to(tile[...][None], (out.shape[0],) + tile.shape)


def unpack_kernel(pairs, home, grad, second, decay, skip):
    groups = grad.shape[0] // NARROW
    order = second.shape[0]
    rows = grad.shape[1] // COLS * NARROW
    block = rows + 8
    for p in range(rows // 8):
        even = pairs[:, 0, 8 * p : 8 * p + 8, :].reshape(-1, COLS)
        odd = pairs[:, 1, 8 * p : 8 * p + 8, :].reshape(-1, COLS)
        for n, part in enumerate(zip_rows(even, odd)):
            grad[:, pl.ds((2 * p + n) * COLS, COLS)] = part
    i = lax.broadcasted_iota(jnp.int32, (groups, groups * NARROW), 0)
    j = lax.broadcasted_iota(jnp.int32, (groups, groups * NARROW), 1)
    flat = [jnp.transpose(home[pl.ds(rows + n, groups, stride=block), :], (1, 0)) for n in range(3)]
    total = jnp.zeros(second.shape, f32)
    scalars = jnp.zeros((8, groups * NARROW), f32)
    line = lax.broadcasted_iota(jnp.int32, scalars.shape, 0)
    for c in range(NARROW):
        place = (j == NARROW * i + c).astype(f32)
        mine = flat[c // 2][(c % 2) * order : (c % 2 + 1) * order]
        total = total + jnp.dot(mine, place, precision=highest, preferred_element_type=f32)
        moved = jnp.dot(flat[2][:8], place, precision=highest, preferred_element_type=f32)
        scalars = scalars + jnp.where(line % NARROW == c, moved, 0.0)
    second[...] = total
    decay[...] = jnp.sum(scalars[:NARROW], axis=0, keepdims=True)
    skip[...] = jnp.sum(scalars[NARROW:], axis=0, keepdims=True)


def local(signal, cotangent, first_layer, second_layer, decay_rate, skip_gain):
    groups = lax.axis_size("batch")
    place = lax.axis_index("batch")
    side = lax.axis_index("chan")
    sides = lax.axis_size("chan")
    embed, order = first_layer.shape
    t = make_tables(embed)
    vmem = pl.BlockSpec(memory_space=pltpu.VMEM)
    smem = pl.BlockSpec(memory_space=pltpu.SMEM)
    hbm = pl.BlockSpec(memory_space=pltpu.HBM)
    shape = jax.ShapeDtypeStruct
    rows = signal.shape[1] // COLS * NARROW

    def keep(x):
        return pltpu.with_memory_space_constraint(x, pltpu.HBM)

    def call(body, name, outs, specs, args, mib, flops=0, scratch=(), out_specs=None):
        return pl.pallas_call(
            body,
            out_shape=outs,
            in_specs=specs,
            out_specs=out_specs or (vmem,) * len(outs),
            scratch_shapes=list(scratch),
            compiler_params=pltpu.CompilerParams(vmem_limit_bytes=mib << 20),
            cost_estimate=pl.CostEstimate(flops=flops, bytes_accessed=0, transcendentals=0),
            name=name,
        )(*args)

    quarters = signal.shape[1] // COLS
    (sent,) = call(
        pack_kernel, "pack", (pltpu.HBM((groups // 2, 2, 2 * rows, COLS), f32),), [hbm] * 2,
        (keep(signal), keep(cotangent)), 8, out_specs=(hbm,),
        scratch=[
            pltpu.VMEM((quarters, 2, signal.shape[0], COLS), f32),
            pltpu.VMEM((quarters, groups // 2, 2, 8, COLS), f32),
            pltpu.SemaphoreType.DMA((quarters, 2)),
            pltpu.SemaphoreType.DMA((quarters,)),
        ],
    )
    spread = lax.all_to_all(
        sent.reshape(groups, 2 * rows, COLS), "batch", split_axis=0, concat_axis=0, tiled=True
    ).reshape(-1, COLS)

    columns = lax.dynamic_slice_in_dim(second_layer, place * NARROW, NARROW, 1)
    rates = lax.dynamic_slice_in_dim(decay_rate, place * NARROW, NARROW, 0)
    gains = lax.dynamic_slice_in_dim(skip_gain, place * NARROW, NARROW, 0)
    weights = jnp.pad(first_layer.T * (0.5 / math.pi), ((0, 0), (0, COLS // 2 - embed)))
    weights = jnp.concatenate([weights, weights], axis=1)
    eight = jnp.pad(columns, ((0, 0), (0, 8 - NARROW)))
    tiled = jnp.pad(jnp.concatenate([eight] * 3, axis=1), ((0, 0), (0, COLS - 24)))
    rates = jnp.broadcast_to(jnp.pad(rates, (0, 8 - NARROW))[:, None], (8, COLS))

    full = (order, LENGTH)
    four = (NARROW, ROWS, COLS)
    wide = (NARROW, ROWS, 2 * COLS)
    kept = ((full, bf16), (full, bf16), (full, f32), (four, f32), (four, f32))
    tall = (ROWS * 8, COLS)
    *state, norms, spectra = call(
        filter_kernel, "make_filter",
        tuple(pltpu.HBM(*k) for k in kept) + (shape((8, COLS), f32), pltpu.HBM(wide, f32)),
        [vmem] * 9,
        (
            weights, eight.T, rates, t["rows"], t["spread"],
            t["forward_left"], t["forward_right"], t["twist_cos"], t["twist_sin"],
        ),
        40, flops=20_000_000_000,
        scratch=[pltpu.VMEM(*k) for k in kept] + [
            pltpu.VMEM(wide, f32), pltpu.VMEM(tall, f32), pltpu.VMEM(tall, f32),
            pltpu.SemaphoreType.DMA((6,)),
        ],
        out_specs=(hbm,) * 5 + (vmem, hbm),
    )
    small, first, cotan = call(
        main_kernel, "correlate",
        (shape((3, COLS), f32), shape((20, COLS), f32), shape(wide, f32)),
        [vmem] * 11 + [hbm] * 5,
        (
            spread, tiled, norms, t["rows"], t["gather"],
            t["forward_left"], t["forward_right"], t["inverse_left"], t["inverse_right"],
            t["twist_cos"], t["twist_sin"], *map(keep, state),
        ),
        40, flops=10_000_000_000,
        scratch=[pltpu.VMEM(*k) for k in kept] + [
            pltpu.VMEM(tall, f32), pltpu.VMEM(wide, f32), pltpu.SemaphoreType.DMA((5,)),
        ],
    )

    quarter = first.shape[0] // sides
    pieces = [lax.dynamic_slice_in_dim(first, side * quarter, quarter, 0)]
    for step in range(1, sides):
        ring = [(i, (i + step) % sides) for i in range(sides)]
        piece = lax.dynamic_slice_in_dim(first, (side + step) % sides * quarter, quarter, 0)
        pieces.append(lax.ppermute(piece, "chan", ring))
    (grad,) = call(
        input_kernel, "input_grad", (shape((groups * rows, COLS), f32),),
        [vmem, smem] + [vmem] * 6,
        (
            spread, gains, spectra, cotan, t["inverse_left"], t["inverse_right"],
            t["twist_cos"], t["twist_sin"],
        ),
        16, flops=4_000_000_000,
    )
    (back,) = call(
        join_kernel, "join", (shape((groups, rows + 8, COLS), f32),), [vmem] * 6,
        (grad, small, *pieces), 8, scratch=[pltpu.VMEM((8, COLS), f32)],
    )
    home = lax.all_to_all(back, "batch", split_axis=0, concat_axis=0, tiled=True)

    mine = home[:, rows + 3 :].sum(0)
    gathered = [mine]
    for step in range(1, sides):
        ring = [((i + step) % sides, i) for i in range(sides)]
        gathered.append(lax.ppermute(mine, "chan", ring))
    input_grad, second_grad, decay_grad, skip_grad = call(
        unpack_kernel, "unpack",
        (
            shape(signal.shape, f32), shape(second_layer.shape, f32),
            shape((1,) + decay_rate.shape, f32), shape((1,) + skip_gain.shape, f32),
        ),
        [vmem] * 2, (home.reshape(groups // 2, 2, -1, COLS), home.reshape(-1, COLS)), 8,
        flops=1_000_000_000,
    )
    twice = jnp.concatenate(gathered + gathered, axis=0)
    ordered = lax.dynamic_slice_in_dim(
        twice, (sides - side) % sides * quarter, sides * quarter, 0
    )
    first_grad = jnp.concatenate([ordered[:, :order], ordered[:, order:]], axis=0)[:embed]
    return (input_grad, first_grad, second_grad, decay_grad[0], skip_grad[0])


def solution(mesh):
    placed = (P("chan", "batch"), P("chan", "batch"), P(), P(None, "chan"), P("chan"), P("chan"))
    return jax.shard_map(
        local,
        mesh=mesh,
        in_specs=placed,
        out_specs=(P("chan", "batch"), P(), P(None, "chan"), P("chan"), P("chan")),
        check_vma=False,
    )
```

```python
import math

import jax
import jax.numpy as jnp
import numpy as np
from jax import lax
from jax.experimental import pallas as pl
from jax.experimental.pallas import tpu as pltpu
from jax.sharding import PartitionSpec as P

ROWS = 256
COLS = 128
LENGTH = ROWS * COLS
NARROW = 4
FILTER_BATCH = 16
TAIL_BATCH = 32
TINY = 1e-06
f32 = jnp.float32
bf16 = jnp.bfloat16
highest = lax.Precision.HIGHEST


def halves(x):
    high = x.astype(bf16)
    low = (x - high.astype(np.float64)).astype(bf16)
    return high, low


SIN = (6.28318528, -10.33542017, 5.100155046, -1.196582571, 0.1553153206)
COS = (0.9999999532, -4.934792831, 4.058411353, -1.331876568, 0.2196896111)


def make_tables(embed):
    a = np.arange(ROWS)
    k = np.arange(ROWS)
    m = np.arange(COLS)
    bands = embed // 2
    turn = np.pi * ((a[None, :] * (4 * k + 1)[:, None]) % (4 * ROWS)) / (2 * ROWS)
    first = np.concatenate([np.cos(turn), -np.sin(turn)], axis=0)
    twist = np.pi * (4 * k + 1)[:, None] * m[None, :] / (2 * LENGTH)
    angle = 2.0 * np.pi * ((m[:, None] * m[None, :]) % COLS) / COLS
    c, s = np.cos(angle), np.sin(angle)
    second = np.concatenate(
        [np.concatenate([c, -s], axis=1), np.concatenate([s, c], axis=1)], axis=0
    )
    high, low = halves(first)
    forward_left = np.concatenate([high, low], axis=1)
    inverse_left = np.concatenate([high.T, low.T], axis=1)
    high, low = halves(second)
    forward_right = np.concatenate([high, low], axis=0)
    inverse_right = np.concatenate([high.T, low.T], axis=0)
    rows = np.zeros((ROWS, COLS))
    lanes = np.zeros((COLS, COLS))
    half = COLS // 2
    rows[:, 0] = a * COLS / LENGTH
    lanes[0] = 1.0
    rows[:, half] = 1.0
    lanes[half] = m / LENGTH
    for b in range(1, bands + 1):
        big = 2.0 * np.pi * ((b * COLS * a) % LENGTH) / LENGTH
        small = 2.0 * np.pi * b * m / LENGTH
        rows[:, b] = np.cos(big)
        rows[:, half + b] = -np.sin(big)
        rows[:, bands + b] = np.sin(big)
        rows[:, half + bands + b] = np.cos(big)
        lanes[b] = np.cos(small)
        lanes[half + b] = np.sin(small)
        lanes[bands + b] = np.cos(small)
        lanes[half + bands + b] = np.sin(small)
    high, low = halves(lanes.T)
    gather = np.tile(np.concatenate([high, low], axis=1), (2, 1))
    high, low = halves(lanes)
    lowest = (lanes - high.astype(np.float64) - low.astype(np.float64)).astype(bf16)
    spread = np.concatenate([high, low, lowest, high, low, high], axis=0)
    return dict(
        forward_left=forward_left,
        inverse_left=inverse_left,
        forward_right=forward_right,
        inverse_right=inverse_right,
        twist_cos=np.cos(twist).astype(np.float32),
        twist_sin=np.sin(twist).astype(np.float32),
        rows=rows.astype(np.float32),
        spread=spread,
        gather=gather,
    )


def split(x):
    high = x.astype(bf16)
    low = (x - high.astype(f32)).astype(bf16)
    return high, low


def mm(left, right):
    return lax.dot_general(left, right, (((1,), (0,)), ((), ())), preferred_element_type=f32)


def dot_rows(table, x):
    high, low = split(x)
    left = jnp.concatenate([table, table[:, : x.shape[0]]], axis=1)
    return mm(left, jnp.concatenate([high, high, low], axis=0))


def dot_cols(x, table):
    high, low = split(x)
    count = x.shape[1]
    right = jnp.concatenate([table[:count], table], axis=0)
    return mm(jnp.concatenate([high, low, high], axis=1), right)


def forward_pair(x, y, left, right, twist_cos, twist_sin):
    u = dot_rows(left, jnp.concatenate([x, y], axis=1))
    spectra = []
    for n in range(2):
        re = u[:ROWS, n * COLS : (n + 1) * COLS]
        im = u[ROWS:, n * COLS : (n + 1) * COLS]
        v = jnp.concatenate(
            [re * twist_cos + im * twist_sin, im * twist_cos - re * twist_sin], axis=1
        )
        spectra.append(dot_cols(v, right))
    return spectra


def times_conj(f, c):
    fr, fi, cr, ci = f[:, :COLS], f[:, COLS:], c[:, :COLS], c[:, COLS:]
    return jnp.concatenate([fr * cr + fi * ci, fr * ci - fi * cr], axis=1)


def inverse_pair(g, h, left, right, twist_cos, twist_sin):
    parts = []
    for x in (g, h):
        w = dot_cols(x, right)
        re, im = w[:, :COLS], w[:, COLS:]
        parts.append(
            jnp.concatenate(
                [re * twist_cos - im * twist_sin, im * twist_cos + re * twist_sin], axis=0
            )
        )
    y = dot_rows(left, jnp.concatenate(parts, axis=1))
    return y[:, :COLS], y[:, COLS:]


def sin_and_cos(x):
    r = x - ((x + 12582912.0) - 12582912.0)
    z = r * r
    s = SIN[4]
    for n in (3, 2, 1, 0):
        s = s * z + SIN[n]
    s = s * r
    c = COS[4]
    for n in (3, 2, 1, 0):
        c = c * z + COS[n]
    return s * c, 1.0 - 0.5 * (s * s)


def fraction_rows(count, offset):
    a = lax.broadcasted_iota(jnp.int32, (count, COLS), 0) + offset
    m = lax.broadcasted_iota(jnp.int32, (count, COLS), 1)
    return (a * COLS + m).astype(f32) * (1.0 / LENGTH)


def zip_rows(x, y):
    low = lax.broadcasted_iota(jnp.int32, x.shape, 0) % 8 < 4
    count = x.shape[0]
    return (
        jnp.where(low, x, pltpu.roll(y, 4, 0)),
        jnp.where(low, pltpu.roll(x, count - 4, 0), y),
    )


def pack_kernel(signal, cotangent, out, values, turned, into, outof):
    quarters = signal.shape[1] // COLS
    reads, writes = [], []
    for q in range(quarters):
        here = pl.ds(q * COLS, COLS)
        for n, source in enumerate((signal, cotangent)):
            copy = pltpu.make_async_copy(source.at[:, here], values.at[q, n], into.at[q, n])
            copy.start()
            reads.append(copy)
    for q in range(quarters):
        for copy in reads[2 * q : 2 * q + 2]:
            copy.wait()
        for n, part in enumerate(zip_rows(values[q, 0], values[q, 1])):
            turned[q, :, n] = part.reshape(-1, 8, COLS)
        copy = pltpu.make_async_copy(
            turned.at[q], out.at[:, :, pl.ds(8 * q, 8), :], outof.at[q]
        )
        copy.start()
        writes.append(copy)
    for copy in writes:
        copy.wait()


def filter_kernel(
    weights, columns, rates, rows, spread, left, right, tcos, tsin,
    high_out, low_out, slope_out, filt_out, window_out, norms, spectra_out,
    high, low, slope, filt, window, spectra, raws, wins, sems,
):
    order = weights.shape[0]
    batch = FILTER_BATCH
    wide = batch * COLS

    def copy(source, target, n, here=None):
        if here is not None:
            source, target = source.at[:, here], target.at[:, here]
        return pltpu.make_async_copy(source, target, sems.at[n])

    mixer = jnp.concatenate(split(columns[...]), axis=0)
    lane = lax.broadcasted_iota(jnp.int32, (8, COLS), 1)

    def block(n, total):
        scaled = jnp.concatenate(
            [weights[...] * rows[pl.ds(n * batch + i, 1), :] for i in range(batch)], axis=0
        )
        one = scaled.astype(bf16)
        rest = scaled - one.astype(f32)
        two = rest.astype(bf16)
        three = (rest - two.astype(f32)).astype(bf16)
        turns = mm(jnp.concatenate([one, one, one, two, two, three], axis=1), spread[...])
        for i in range(batch):
            here = pl.ds(pl.multiple_of(n * wide + i * COLS, COLS), COLS)
            s, c = sin_and_cos(turns[i * order : (i + 1) * order])
            slope[:, here] = c
            s_high, s_low = split(s)
            high[:, here] = s_high
            low[:, here] = s_low
        here = pl.ds(pl.multiple_of(n * wide, wide), wide)
        copy(high, high_out, 0, here).start()
        copy(low, low_out, 1, here).start()
        copy(slope, slope_out, 2, here).start()
        p = mm(mixer, high[:, here])
        r = mm(mixer, low[:, here])
        mixed = p[:8] + p[8:] + (r[:8] + r[8:])
        for i in range(batch):
            a = n * batch + i
            fraction = (a * COLS + lane).astype(f32) * (1.0 / LENGTH)
            win = jnp.exp(-rates[...] * fraction)
            raw = win * mixed[:, i * COLS : (i + 1) * COLS]
            raws[pl.ds(pl.multiple_of(a * 8, 8), 8), :] = raw
            wins[pl.ds(pl.multiple_of(a * 8, 8), 8), :] = win
            total = total + raw * raw
        return total

    total = lax.fori_loop(0, ROWS // batch, block, jnp.zeros((8, COLS), f32))
    norm = jnp.sqrt(jnp.sum(total, axis=1, keepdims=True) + TINY)
    norms[...] = jnp.broadcast_to(norm, norms.shape)
    for c in range(NARROW):
        filt[c] = raws[pl.ds(c, ROWS, stride=8), :] / norms[pl.ds(c, 1), :]
        window[c] = wins[pl.ds(c, ROWS, stride=8), :]
    copy(filt, filt_out, 3).start()
    copy(window, window_out, 4).start()
    for c in range(0, NARROW, 2):
        x, y = forward_pair(filt[c], filt[c + 1], left[...], right[...], tcos[...], tsin[...])
        spectra[c] = x
        spectra[c + 1] = y
    copy(spectra, spectra_out, 5).start()
    copy(high, high_out, 0).wait()
    copy(low, low_out, 1).wait()
    copy(slope, slope_out, 2).wait()
    copy(filt, filt_out, 3).wait()
    copy(window, window_out, 4).wait()
    copy(spectra, spectra_out, 5).wait()


def main_kernel(
    both, columns, gains, norms, rows, gather, fleft, fright, ileft, iright, tcos, tsin,
    high_in, low_in, slope_in, filt_in, window_in, spectra_in,
    small, first, grad,
    high, low, slope, filt, window, spectra, dmix, product, early, late,
):
    order = slope.shape[0]
    factor = 1.0 / math.sqrt(LENGTH)
    batch = TAIL_BATCH
    wide = batch * COLS
    starts = [
        pltpu.make_async_copy(source, target, early.at[n])
        for n, (source, target) in enumerate(
            ((filt_in, filt), (window_in, window), (spectra_in, spectra))
        )
    ]

    def fetch(n):
        here = pl.ds(pl.multiple_of(n * wide, wide), wide)
        return [
            pltpu.make_async_copy(source.at[:, here], target.at[:, here], late.at[m, n])
            for m, (source, target) in enumerate(((high_in, high), (low_in, low), (slope_in, slope)))
        ]

    for copy in starts:
        copy.start()
    for n in range(ROWS // batch):
        for copy in fetch(n):
            copy.start()
    lane = lax.broadcasted_iota(jnp.int32, (1, COLS), 1)
    scalars = jnp.zeros((1, COLS), f32)
    fraction = fraction_rows(ROWS, 0)
    dmix[...] = jnp.zeros(dmix.shape, f32)
    for c in range(NARROW):
        x = both[pl.ds(c, ROWS, stride=2 * NARROW), :]
        y = both[pl.ds(NARROW + c, ROWS, stride=2 * NARROW), :]
        skip = factor * jnp.sum(x * y, keepdims=True)
        scalars = jnp.where(lane == NARROW + c, skip, scalars)
        val, cot = forward_pair(x, y, fleft[...], fright[...], tcos[...], tsin[...])
        if c == 0:
            for copy in starts:
                copy.wait()
        product[c] = times_conj(val, cot)
        product[NARROW + c] = times_conj(spectra[c], cot)
    for c in range(NARROW):
        back, into = inverse_pair(
            product[c], product[NARROW + c], ileft[...], iright[...], tcos[...], tsin[...]
        )
        y = both[pl.ds(NARROW + c, ROWS, stride=2 * NARROW), :]
        grad[pl.ds(c, ROWS, stride=NARROW), :] = into * (1.0 / LENGTH) + gains[c] * y
        dfilt = back * (factor / LENGTH)
        project = jnp.sum(filt[c] * dfilt, keepdims=True)
        norm = norms[pl.ds(c, 1), :][:, :1]
        draw = (dfilt - filt[c] * project) / norm
        decay = -jnp.sum(draw * filt[c] * fraction, keepdims=True) * norm
        dmix[pl.ds(c, ROWS, stride=8), :] = draw * window[c]
        scalars = jnp.where(lane == c, decay, scalars)
    lanes = lax.broadcasted_iota(jnp.int32, columns.shape, 1)
    col_high = columns[...].astype(bf16).astype(f32)
    mixer = jnp.where(lanes // 8 == 2, columns[...] - col_high, col_high).astype(bf16)[:, :32]

    def tail(n, carry):
        firsts, seconds = carry
        for copy in fetch(n):
            copy.wait()
        stack = []
        for i in range(batch):
            d = dmix[pl.ds(pl.multiple_of((n * batch + i) * 8, 8), 8), :]
            d_high = d.astype(bf16).astype(f32)
            stack.append(
                jnp.concatenate([d_high, d - d_high, d_high, jnp.zeros_like(d)], axis=0).astype(bf16)
            )
        stack = jnp.concatenate(stack, axis=1)
        here = pl.ds(pl.multiple_of(n * wide, wide), wide)
        both_halves = jnp.concatenate([high[:, here], low[:, here]], axis=0)
        seconds = seconds + lax.dot_general(
            both_halves, stack[:16], (((1,), (1,)), ((), ())), preferred_element_type=f32
        )
        q = mm(mixer, stack) * slope[:, here]
        q = jnp.concatenate([q[:, i * COLS : (i + 1) * COLS] for i in range(batch)], axis=0)
        r = mm(jnp.concatenate(split(q), axis=1), gather[...])
        r = r[:, :COLS] + r[:, COLS:]
        for i in range(batch):
            firsts = firsts + r[i * order : (i + 1) * order] * rows[pl.ds(n * batch + i, 1), :]
        return firsts, seconds

    firsts, seconds = lax.fori_loop(
        0, ROWS // batch, tail,
        (jnp.zeros((order, COLS), f32), jnp.zeros((2 * order, 16), f32)),
    )
    seconds = jnp.transpose(seconds[:order] + seconds[order:], (1, 0))
    seconds = seconds[:8] + seconds[8:]
    small[:1] = jnp.concatenate([seconds[0:1], seconds[1:2]], axis=1)
    small[1:2] = jnp.concatenate([seconds[2:3], seconds[3:4]], axis=1)
    small[2:3] = scalars
    turned = jnp.transpose(firsts, (1, 0))
    half = COLS // 2
    folded = turned[:half] + turned[half:]
    first[...] = jnp.concatenate([folded[:20], folded[20:40]], axis=1)


def join_kernel(grad, small, own, one, two, three, out, tile):
    rows = grad.shape[0] // out.shape[0]
    tile[:3] = small[...]
    tile[3:] = own[...] + one[...] + two[...] + three[...]
    out[:, :rows, :] = grad[...].reshape(out.shape[0], rows, COLS)
    out[:, rows:, :] = jnp.broadcast_to(tile[...][None], (out.shape[0],) + tile.shape)


def unpack_kernel(pairs, home, grad, second, decay, skip):
    groups = grad.shape[0] // NARROW
    order = second.shape[0]
    rows = grad.shape[1] // COLS * NARROW
    block = rows + 8
    for p in range(rows // 8):
        even = pairs[:, 0, 8 * p : 8 * p + 8, :].reshape(-1, COLS)
        odd = pairs[:, 1, 8 * p : 8 * p + 8, :].reshape(-1, COLS)
        for n, part in enumerate(zip_rows(even, odd)):
            grad[:, pl.ds((2 * p + n) * COLS, COLS)] = part
    i = lax.broadcasted_iota(jnp.int32, (groups, groups * NARROW), 0)
    j = lax.broadcasted_iota(jnp.int32, (groups, groups * NARROW), 1)
    flat = [jnp.transpose(home[pl.ds(rows + n, groups, stride=block), :], (1, 0)) for n in range(3)]
    total = jnp.zeros(second.shape, f32)
    scalars = jnp.zeros((8, groups * NARROW), f32)
    line = lax.broadcasted_iota(jnp.int32, scalars.shape, 0)
    for c in range(NARROW):
        place = (j == NARROW * i + c).astype(f32)
        mine = flat[c // 2][(c % 2) * order : (c % 2 + 1) * order]
        total = total + jnp.dot(mine, place, precision=highest, preferred_element_type=f32)
        moved = jnp.dot(flat[2][:8], place, precision=highest, preferred_element_type=f32)
        scalars = scalars + jnp.where(line % NARROW == c, moved, 0.0)
    second[...] = total
    decay[...] = jnp.sum(scalars[:NARROW], axis=0, keepdims=True)
    skip[...] = jnp.sum(scalars[NARROW:], axis=0, keepdims=True)


def local(signal, cotangent, first_layer, second_layer, decay_rate, skip_gain):
    groups = lax.axis_size("batch")
    place = lax.axis_index("batch")
    side = lax.axis_index("chan")
    sides = lax.axis_size("chan")
    embed, order = first_layer.shape
    t = make_tables(embed)
    vmem = pl.BlockSpec(memory_space=pltpu.VMEM)
    smem = pl.BlockSpec(memory_space=pltpu.SMEM)
    hbm = pl.BlockSpec(memory_space=pltpu.HBM)
    shape = jax.ShapeDtypeStruct
    rows = signal.shape[1] // COLS * NARROW

    def keep(x):
        return pltpu.with_memory_space_constraint(x, pltpu.HBM)

    def call(body, name, outs, specs, args, mib, flops=0, scratch=(), out_specs=None):
        return pl.pallas_call(
            body,
            out_shape=outs,
            in_specs=specs,
            out_specs=out_specs or (vmem,) * len(outs),
            scratch_shapes=list(scratch),
            compiler_params=pltpu.CompilerParams(vmem_limit_bytes=mib << 20),
            cost_estimate=pl.CostEstimate(flops=flops, bytes_accessed=0, transcendentals=0),
            name=name,
        )(*args)

    quarters = signal.shape[1] // COLS
    (sent,) = call(
        pack_kernel, "pack", (pltpu.HBM((groups // 2, 2, 2 * rows, COLS), f32),), [hbm] * 2,
        (keep(signal), keep(cotangent)), 8, out_specs=(hbm,),
        scratch=[
            pltpu.VMEM((quarters, 2, signal.shape[0], COLS), f32),
            pltpu.VMEM((quarters, groups // 2, 2, 8, COLS), f32),
            pltpu.SemaphoreType.DMA((quarters, 2)),
            pltpu.SemaphoreType.DMA((quarters,)),
        ],
    )
    spread = lax.all_to_all(
        sent.reshape(groups, 2 * rows, COLS), "batch", split_axis=0, concat_axis=0, tiled=True
    ).reshape(-1, COLS)

    columns = lax.dynamic_slice_in_dim(second_layer, place * NARROW, NARROW, 1)
    rates = lax.dynamic_slice_in_dim(decay_rate, place * NARROW, NARROW, 0)
    gains = lax.dynamic_slice_in_dim(skip_gain, place * NARROW, NARROW, 0)
    weights = jnp.pad(first_layer.T * (0.5 / math.pi), ((0, 0), (0, COLS // 2 - embed)))
    weights = jnp.concatenate([weights, weights], axis=1)
    eight = jnp.pad(columns, ((0, 0), (0, 8 - NARROW)))
    tiled = jnp.pad(jnp.concatenate([eight] * 3, axis=1), ((0, 0), (0, COLS - 24)))
    rates = jnp.broadcast_to(jnp.pad(rates, (0, 8 - NARROW))[:, None], (8, COLS))

    full = (order, LENGTH)
    four = (NARROW, ROWS, COLS)
    wide = (NARROW, ROWS, 2 * COLS)
    kept = ((full, bf16), (full, bf16), (full, f32), (four, f32), (four, f32))
    tall = (ROWS * 8, COLS)
    *state, norms, spectra = call(
        filter_kernel, "make_filter",
        tuple(pltpu.HBM(*k) for k in kept) + (shape((8, COLS), f32), pltpu.HBM(wide, f32)),
        [vmem] * 9,
        (
            weights, eight.T, rates, t["rows"], t["spread"],
            t["forward_left"], t["forward_right"], t["twist_cos"], t["twist_sin"],
        ),
        40, flops=20_000_000_000,
        scratch=[pltpu.VMEM(*k) for k in kept] + [
            pltpu.VMEM(wide, f32), pltpu.VMEM(tall, f32), pltpu.VMEM(tall, f32),
            pltpu.SemaphoreType.DMA((6,)),
        ],
        out_specs=(hbm,) * 5 + (vmem, hbm),
    )
    small, first, grad = call(
        main_kernel, "correlate",
        (shape((3, COLS), f32), shape((20, COLS), f32), shape((groups * rows, COLS), f32)),
        [vmem] * 2 + [smem] + [vmem] * 9 + [hbm] * 6,
        (
            spread, tiled, gains, norms, t["rows"], t["gather"],
            t["forward_left"], t["forward_right"], t["inverse_left"], t["inverse_right"],
            t["twist_cos"], t["twist_sin"], *map(keep, state), keep(spectra),
        ),
        40, flops=10_000_000_000,
        scratch=[pltpu.VMEM(*k) for k in kept] + [
            pltpu.VMEM(wide, f32), pltpu.VMEM(tall, f32),
            pltpu.VMEM((2 * NARROW, ROWS, 2 * COLS), f32),
            pltpu.SemaphoreType.DMA((3,)), pltpu.SemaphoreType.DMA((3, ROWS // TAIL_BATCH)),
        ],
    )

    quarter = first.shape[0] // sides
    pieces = [lax.dynamic_slice_in_dim(first, side * quarter, quarter, 0)]
    for step in range(1, sides):
        ring = [(i, (i + step) % sides) for i in range(sides)]
        piece = lax.dynamic_slice_in_dim(first, (side + step) % sides * quarter, quarter, 0)
        pieces.append(lax.ppermute(piece, "chan", ring))
    (back,) = call(
        join_kernel, "join", (shape((groups, rows + 8, COLS), f32),), [vmem] * 6,
        (grad, small, *pieces), 8, scratch=[pltpu.VMEM((8, COLS), f32)],
    )
    home = lax.all_to_all(back, "batch", split_axis=0, concat_axis=0, tiled=True)

    mine = home[:, rows + 3 :].sum(0)
    gathered = [mine]
    for step in range(1, sides):
        ring = [((i + step) % sides, i) for i in range(sides)]
        gathered.append(lax.ppermute(mine, "chan", ring))
    input_grad, second_grad, decay_grad, skip_grad = call(
        unpack_kernel, "unpack",
        (
            shape(signal.shape, f32), shape(second_layer.shape, f32),
            shape((1,) + decay_rate.shape, f32), shape((1,) + skip_gain.shape, f32),
        ),
        [vmem] * 2, (home.reshape(groups // 2, 2, -1, COLS), home.reshape(-1, COLS)), 8,
        flops=1_000_000_000,
    )
    twice = jnp.concatenate(gathered + gathered, axis=0)
    ordered = lax.dynamic_slice_in_dim(
        twice, (sides - side) % sides * quarter, sides * quarter, 0
    )
    first_grad = jnp.concatenate([ordered[:, :order], ordered[:, order:]], axis=0)[:embed]
    return (input_grad, first_grad, second_grad, decay_grad[0], skip_grad[0])


def solution(mesh):
    placed = (P("chan", "batch"), P("chan", "batch"), P(), P(None, "chan"), P("chan"), P("chan"))
    return jax.shard_map(
        local,
        mesh=mesh,
        in_specs=placed,
        out_specs=(P("chan", "batch"), P(), P(None, "chan"), P("chan"), P("chan")),
        check_vma=False,
    )
```

```python
import math

import jax
import jax.numpy as jnp
import numpy as np
from jax import lax
from jax.experimental import pallas as pl
from jax.experimental.pallas import tpu as pltpu
from jax.sharding import PartitionSpec as P

ROWS = 256
COLS = 128
LENGTH = ROWS * COLS
NARROW = 4
FILTER_BATCH = 16
TAIL_BATCH = 32
TINY = 1e-06
f32 = jnp.float32
bf16 = jnp.bfloat16
highest = lax.Precision.HIGHEST


def halves(x):
    high = x.astype(bf16)
    low = (x - high.astype(np.float64)).astype(bf16)
    return high, low


SIN = (6.28318528, -10.33542017, 5.100155046, -1.196582571, 0.1553153206)
COS = (0.9999999532, -4.934792831, 4.058411353, -1.331876568, 0.2196896111)


def make_tables(embed):
    a = np.arange(ROWS)
    k = np.arange(ROWS)
    m = np.arange(COLS)
    bands = embed // 2
    turn = np.pi * ((a[None, :] * (4 * k + 1)[:, None]) % (4 * ROWS)) / (2 * ROWS)
    first = np.concatenate([np.cos(turn), -np.sin(turn)], axis=0)
    twist = np.pi * (4 * k + 1)[:, None] * m[None, :] / (2 * LENGTH)
    angle = 2.0 * np.pi * ((m[:, None] * m[None, :]) % COLS) / COLS
    c, s = np.cos(angle), np.sin(angle)
    second = np.concatenate(
        [np.concatenate([c, -s], axis=1), np.concatenate([s, c], axis=1)], axis=0
    )
    high, low = halves(first)
    forward_left = np.concatenate([high, low], axis=1)
    inverse_left = np.concatenate([high.T, low.T], axis=1)
    high, low = halves(second)
    forward_right = np.concatenate([high, low], axis=0)
    inverse_right = np.concatenate([high.T, low.T], axis=0)
    rows = np.zeros((ROWS, COLS))
    lanes = np.zeros((COLS, COLS))
    half = COLS // 2
    rows[:, 0] = a * COLS / LENGTH
    lanes[0] = 1.0
    rows[:, half] = 1.0
    lanes[half] = m / LENGTH
    for b in range(1, bands + 1):
        big = 2.0 * np.pi * ((b * COLS * a) % LENGTH) / LENGTH
        small = 2.0 * np.pi * b * m / LENGTH
        rows[:, b] = np.cos(big)
        rows[:, half + b] = -np.sin(big)
        rows[:, bands + b] = np.sin(big)
        rows[:, half + bands + b] = np.cos(big)
        lanes[b] = np.cos(small)
        lanes[half + b] = np.sin(small)
        lanes[bands + b] = np.cos(small)
        lanes[half + bands + b] = np.sin(small)
    high, low = halves(lanes.T)
    gather = np.tile(np.concatenate([high, low], axis=1), (2, 1))
    high, low = halves(lanes)
    lowest = (lanes - high.astype(np.float64) - low.astype(np.float64)).astype(bf16)
    spread = np.concatenate([high, low, lowest, high, low, high], axis=0)
    return dict(
        forward_left=forward_left,
        inverse_left=inverse_left,
        forward_right=forward_right,
        inverse_right=inverse_right,
        twist_cos=np.cos(twist).astype(np.float32),
        twist_sin=np.sin(twist).astype(np.float32),
        rows=rows.astype(np.float32),
        spread=spread,
        gather=gather,
    )


def split(x):
    high = x.astype(bf16)
    low = (x - high.astype(f32)).astype(bf16)
    return high, low


def mm(left, right):
    return lax.dot_general(left, right, (((1,), (0,)), ((), ())), preferred_element_type=f32)


def dot_rows(table, x):
    high, low = split(x)
    left = jnp.concatenate([table, table[:, : x.shape[0]]], axis=1)
    return mm(left, jnp.concatenate([high, high, low], axis=0))


def dot_cols(x, table):
    high, low = split(x)
    count = x.shape[1]
    right = jnp.concatenate([table[:count], table], axis=0)
    return mm(jnp.concatenate([high, low, high], axis=1), right)


def forward_pair(x, y, left, right, twist_cos, twist_sin):
    u = dot_rows(left, jnp.concatenate([x, y], axis=1))
    spectra = []
    for n in range(2):
        re = u[:ROWS, n * COLS : (n + 1) * COLS]
        im = u[ROWS:, n * COLS : (n + 1) * COLS]
        v = jnp.concatenate(
            [re * twist_cos + im * twist_sin, im * twist_cos - re * twist_sin], axis=1
        )
        spectra.append(dot_cols(v, right))
    return spectra


def times_conj(f, c):
    fr, fi, cr, ci = f[:, :COLS], f[:, COLS:], c[:, :COLS], c[:, COLS:]
    return jnp.concatenate([fr * cr + fi * ci, fr * ci - fi * cr], axis=1)


def inverse_pair(g, h, left, right, twist_cos, twist_sin):
    parts = []
    for x in (g, h):
        w = dot_cols(x, right)
        re, im = w[:, :COLS], w[:, COLS:]
        parts.append(
            jnp.concatenate(
                [re * twist_cos - im * twist_sin, im * twist_cos + re * twist_sin], axis=0
            )
        )
    y = dot_rows(left, jnp.concatenate(parts, axis=1))
    return y[:, :COLS], y[:, COLS:]


def sin_and_cos(x):
    r = x - ((x + 12582912.0) - 12582912.0)
    z = r * r
    s = SIN[4]
    for n in (3, 2, 1, 0):
        s = s * z + SIN[n]
    s = s * r
    c = COS[4]
    for n in (3, 2, 1, 0):
        c = c * z + COS[n]
    return s * c, 1.0 - 0.5 * (s * s)


def fraction_rows(count, offset):
    a = lax.broadcasted_iota(jnp.int32, (count, COLS), 0) + offset
    m = lax.broadcasted_iota(jnp.int32, (count, COLS), 1)
    return (a * COLS + m).astype(f32) * (1.0 / LENGTH)


def zip_rows(x, y):
    low = lax.broadcasted_iota(jnp.int32, x.shape, 0) % 8 < 4
    count = x.shape[0]
    return (
        jnp.where(low, x, pltpu.roll(y, 4, 0)),
        jnp.where(low, pltpu.roll(x, count - 4, 0), y),
    )


def pack_kernel(signal, cotangent, out, values, turned, into, outof):
    quarters = signal.shape[1] // COLS
    reads, writes = [], []
    for q in range(quarters):
        here = pl.ds(q * COLS, COLS)
        for n, source in enumerate((signal, cotangent)):
            copy = pltpu.make_async_copy(source.at[:, here], values.at[q, n], into.at[q, n])
            copy.start()
            reads.append(copy)
    for q in range(quarters):
        for copy in reads[2 * q : 2 * q + 2]:
            copy.wait()
        for n, part in enumerate(zip_rows(values[q, 0], values[q, 1])):
            turned[q, :, n] = part.reshape(-1, 8, COLS)
        copy = pltpu.make_async_copy(
            turned.at[q], out.at[:, :, pl.ds(8 * q, 8), :], outof.at[q]
        )
        copy.start()
        writes.append(copy)
    for copy in writes:
        copy.wait()


def filter_kernel(
    weights, columns, rates, rows, spread, left, right, tcos, tsin,
    high_out, low_out, slope_out, filt_out, window_out, norms, spectra_out,
    high, low, slope, filt, window, spectra, raws, wins, sems,
):
    order = weights.shape[0]
    batch = FILTER_BATCH
    wide = batch * COLS

    def copy(source, target, n, here=None):
        if here is not None:
            source, target = source.at[:, here], target.at[:, here]
        return pltpu.make_async_copy(source, target, sems.at[n])

    mixer = jnp.concatenate(split(columns[...]), axis=0)
    lane = lax.broadcasted_iota(jnp.int32, (8, COLS), 1)

    def block(n, total):
        scaled = jnp.concatenate(
            [weights[...] * rows[pl.ds(n * batch + i, 1), :] for i in range(batch)], axis=0
        )
        one = scaled.astype(bf16)
        rest = scaled - one.astype(f32)
        two = rest.astype(bf16)
        three = (rest - two.astype(f32)).astype(bf16)
        turns = mm(jnp.concatenate([one, one, one, two, two, three], axis=1), spread[...])
        for i in range(batch):
            here = pl.ds(pl.multiple_of(n * wide + i * COLS, COLS), COLS)
            s, c = sin_and_cos(turns[i * order : (i + 1) * order])
            slope[:, here] = c
            s_high, s_low = split(s)
            high[:, here] = s_high
            low[:, here] = s_low
        here = pl.ds(pl.multiple_of(n * wide, wide), wide)
        copy(high, high_out, 0, here).start()
        copy(low, low_out, 1, here).start()
        copy(slope, slope_out, 2, here).start()
        p = mm(mixer, high[:, here])
        r = mm(mixer, low[:, here])
        mixed = p[:8] + p[8:] + (r[:8] + r[8:])
        for i in range(batch):
            a = n * batch + i
            fraction = (a * COLS + lane).astype(f32) * (1.0 / LENGTH)
            win = jnp.exp(-rates[...] * fraction)
            raw = win * mixed[:, i * COLS : (i + 1) * COLS]
            raws[pl.ds(pl.multiple_of(a * 8, 8), 8), :] = raw
            wins[pl.ds(pl.multiple_of(a * 8, 8), 8), :] = win
            total = total + raw * raw
        return total

    total = lax.fori_loop(0, ROWS // batch, block, jnp.zeros((8, COLS), f32))
    norm = jnp.sqrt(jnp.sum(total, axis=1, keepdims=True) + TINY)
    norms[...] = jnp.broadcast_to(norm, norms.shape)
    for c in range(NARROW):
        filt[c] = raws[pl.ds(c, ROWS, stride=8), :] / norms[pl.ds(c, 1), :]
        window[c] = wins[pl.ds(c, ROWS, stride=8), :]
    copy(filt, filt_out, 3).start()
    copy(window, window_out, 4).start()
    for c in range(0, NARROW, 2):
        x, y = forward_pair(filt[c], filt[c + 1], left[...], right[...], tcos[...], tsin[...])
        spectra[c] = x
        spectra[c + 1] = y
    copy(spectra, spectra_out, 5).start()
    copy(high, high_out, 0).wait()
    copy(low, low_out, 1).wait()
    copy(slope, slope_out, 2).wait()
    copy(filt, filt_out, 3).wait()
    copy(window, window_out, 4).wait()
    copy(spectra, spectra_out, 5).wait()


def main_kernel(
    both, columns, norms, rows, gather, fleft, fright, ileft, iright, tcos, tsin,
    high_in, low_in, slope_in, filt_in, window_in,
    small, first, cotan,
    high, low, slope, filt, window, dmix, product, early, late,
):
    order = slope.shape[0]
    factor = 1.0 / math.sqrt(LENGTH)
    batch = TAIL_BATCH
    wide = batch * COLS
    starts = [
        pltpu.make_async_copy(source, target, early.at[n])
        for n, (source, target) in enumerate(((filt_in, filt), (window_in, window)))
    ]

    def fetch(n):
        here = pl.ds(pl.multiple_of(n * wide, wide), wide)
        return [
            pltpu.make_async_copy(source.at[:, here], target.at[:, here], late.at[m, n])
            for m, (source, target) in enumerate(((high_in, high), (low_in, low), (slope_in, slope)))
        ]

    for copy in starts:
        copy.start()
    lane = lax.broadcasted_iota(jnp.int32, (1, COLS), 1)
    scalars = jnp.zeros((1, COLS), f32)
    fraction = fraction_rows(ROWS, 0)
    dmix[...] = jnp.zeros(dmix.shape, f32)
    for c in range(NARROW):
        x = both[pl.ds(c, ROWS, stride=2 * NARROW), :]
        y = both[pl.ds(NARROW + c, ROWS, stride=2 * NARROW), :]
        skip = factor * jnp.sum(x * y, keepdims=True)
        scalars = jnp.where(lane == NARROW + c, skip, scalars)
        val, cot = forward_pair(x, y, fleft[...], fright[...], tcos[...], tsin[...])
        if c == 0:
            for copy in starts:
                copy.wait()
            for n in range(ROWS // batch):
                for copy in fetch(n):
                    copy.start()
        cotan[c] = cot
        product[c] = times_conj(val, cot)
    for c in range(0, NARROW, 2):
        pair = inverse_pair(
            product[c], product[c + 1], ileft[...], iright[...], tcos[...], tsin[...]
        )
        for n in range(2):
            i = c + n
            dfilt = pair[n] * (factor / LENGTH)
            project = jnp.sum(filt[i] * dfilt, keepdims=True)
            norm = norms[pl.ds(i, 1), :][:, :1]
            draw = (dfilt - filt[i] * project) / norm
            decay = -jnp.sum(draw * filt[i] * fraction, keepdims=True) * norm
            dmix[pl.ds(i, ROWS, stride=8), :] = draw * window[i]
            scalars = jnp.where(lane == i, decay, scalars)
    lanes = lax.broadcasted_iota(jnp.int32, columns.shape, 1)
    col_high = columns[...].astype(bf16).astype(f32)
    mixer = jnp.where(lanes // 8 == 2, columns[...] - col_high, col_high).astype(bf16)[:, :32]

    def tail(n, carry):
        firsts, seconds = carry
        for copy in fetch(n):
            copy.wait()
        stack = []
        for i in range(batch):
            d = dmix[pl.ds(pl.multiple_of((n * batch + i) * 8, 8), 8), :]
            d_high = d.astype(bf16).astype(f32)
            stack.append(
                jnp.concatenate([d_high, d - d_high, d_high, jnp.zeros_like(d)], axis=0).astype(bf16)
            )
        stack = jnp.concatenate(stack, axis=1)
        here = pl.ds(pl.multiple_of(n * wide, wide), wide)
        both_halves = jnp.concatenate([high[:, here], low[:, here]], axis=0)
        seconds = seconds + lax.dot_general(
            both_halves, stack[:16], (((1,), (1,)), ((), ())), preferred_element_type=f32
        )
        q = mm(mixer, stack) * slope[:, here]
        q = jnp.concatenate([q[:, i * COLS : (i + 1) * COLS] for i in range(batch)], axis=0)
        r = mm(jnp.concatenate(split(q), axis=1), gather[...])
        r = r[:, :COLS] + r[:, COLS:]
        for i in range(batch):
            firsts = firsts + r[i * order : (i + 1) * order] * rows[pl.ds(n * batch + i, 1), :]
        return firsts, seconds

    firsts, seconds = lax.fori_loop(
        0, ROWS // batch, tail,
        (jnp.zeros((order, COLS), f32), jnp.zeros((2 * order, 16), f32)),
    )
    seconds = jnp.transpose(seconds[:order] + seconds[order:], (1, 0))
    seconds = seconds[:8] + seconds[8:]
    small[:1] = jnp.concatenate([seconds[0:1], seconds[1:2]], axis=1)
    small[1:2] = jnp.concatenate([seconds[2:3], seconds[3:4]], axis=1)
    small[2:3] = scalars
    turned = jnp.transpose(firsts, (1, 0))
    half = COLS // 2
    folded = turned[:half] + turned[half:]
    first[...] = jnp.concatenate([folded[:20], folded[20:40]], axis=1)


def input_kernel(both, gains, spectra, cotan, ileft, iright, tcos, tsin, grad):
    for c in range(0, NARROW, 2):
        pair = inverse_pair(
            times_conj(spectra[c], cotan[c]), times_conj(spectra[c + 1], cotan[c + 1]),
            ileft[...], iright[...], tcos[...], tsin[...],
        )
        for n in range(2):
            i = c + n
            y = both[pl.ds(NARROW + i, ROWS, stride=2 * NARROW), :]
            grad[pl.ds(i, ROWS, stride=NARROW), :] = pair[n] * (1.0 / LENGTH) + gains[i] * y


def join_kernel(grad, small, own, one, two, three, out, tile):
    rows = grad.shape[0] // out.shape[0]
    tile[:3] = small[...]
    tile[3:] = own[...] + one[...] + two[...] + three[...]
    out[:, :rows, :] = grad[...].reshape(out.shape[0], rows, COLS)
    out[:, rows:, :] = jnp.broadcast_to(tile[...][None], (out.shape[0],) + tile.shape)


def unpack_kernel(pairs, home, grad, second, decay, skip):
    groups = grad.shape[0] // NARROW
    order = second.shape[0]
    rows = grad.shape[1] // COLS * NARROW
    block = rows + 8
    for p in range(rows // 8):
        even = pairs[:, 0, 8 * p : 8 * p + 8, :].reshape(-1, COLS)
        odd = pairs[:, 1, 8 * p : 8 * p + 8, :].reshape(-1, COLS)
        for n, part in enumerate(zip_rows(even, odd)):
            grad[:, pl.ds((2 * p + n) * COLS, COLS)] = part
    i = lax.broadcasted_iota(jnp.int32, (groups, groups * NARROW), 0)
    j = lax.broadcasted_iota(jnp.int32, (groups, groups * NARROW), 1)
    flat = [jnp.transpose(home[pl.ds(rows + n, groups, stride=block), :], (1, 0)) for n in range(3)]
    total = jnp.zeros(second.shape, f32)
    scalars = jnp.zeros((8, groups * NARROW), f32)
    line = lax.broadcasted_iota(jnp.int32, scalars.shape, 0)
    for c in range(NARROW):
        place = (j == NARROW * i + c).astype(f32)
        mine = flat[c // 2][(c % 2) * order : (c % 2 + 1) * order]
        total = total + jnp.dot(mine, place, precision=highest, preferred_element_type=f32)
        moved = jnp.dot(flat[2][:8], place, precision=highest, preferred_element_type=f32)
        scalars = scalars + jnp.where(line % NARROW == c, moved, 0.0)
    second[...] = total
    decay[...] = jnp.sum(scalars[:NARROW], axis=0, keepdims=True)
    skip[...] = jnp.sum(scalars[NARROW:], axis=0, keepdims=True)


def finish_kernel(side, own, one, two, three, out, table):
    pieces = (own[...], one[...], two[...], three[...])
    count = own.shape[0]
    order = out.shape[1]
    for n in range(len(pieces)):
        chosen = jnp.zeros(own.shape, f32)
        for i, piece in enumerate(pieces):
            chosen = jnp.where((side[0] + i) % len(pieces) == n, piece, chosen)
        table[n * count : (n + 1) * count] = chosen
    total = table.shape[0]
    out[:total] = table[:, :order]
    out[total:] = table[: out.shape[0] - total, order:]


def local(signal, cotangent, first_layer, second_layer, decay_rate, skip_gain):
    groups = lax.axis_size("batch")
    place = lax.axis_index("batch")
    side = lax.axis_index("chan")
    sides = lax.axis_size("chan")
    embed, order = first_layer.shape
    t = make_tables(embed)
    vmem = pl.BlockSpec(memory_space=pltpu.VMEM)
    smem = pl.BlockSpec(memory_space=pltpu.SMEM)
    hbm = pl.BlockSpec(memory_space=pltpu.HBM)
    shape = jax.ShapeDtypeStruct
    rows = signal.shape[1] // COLS * NARROW

    def keep(x):
        return pltpu.with_memory_space_constraint(x, pltpu.HBM)

    def call(body, name, outs, specs, args, mib, flops=0, scratch=(), out_specs=None):
        return pl.pallas_call(
            body,
            out_shape=outs,
            in_specs=specs,
            out_specs=out_specs or (vmem,) * len(outs),
            scratch_shapes=list(scratch),
            compiler_params=pltpu.CompilerParams(vmem_limit_bytes=mib << 20),
            cost_estimate=pl.CostEstimate(flops=flops, bytes_accessed=0, transcendentals=0),
            name=name,
        )(*args)

    quarters = signal.shape[1] // COLS
    (sent,) = call(
        pack_kernel, "pack", (pltpu.HBM((groups // 2, 2, 2 * rows, COLS), f32),), [hbm] * 2,
        (keep(signal), keep(cotangent)), 8, out_specs=(hbm,),
        scratch=[
            pltpu.VMEM((quarters, 2, signal.shape[0], COLS), f32),
            pltpu.VMEM((quarters, groups // 2, 2, 8, COLS), f32),
            pltpu.SemaphoreType.DMA((quarters, 2)),
            pltpu.SemaphoreType.DMA((quarters,)),
        ],
    )
    spread = lax.all_to_all(
        sent.reshape(groups, 2 * rows, COLS), "batch", split_axis=0, concat_axis=0, tiled=True
    ).reshape(-1, COLS)

    columns = lax.dynamic_slice_in_dim(second_layer, place * NARROW, NARROW, 1)
    rates = lax.dynamic_slice_in_dim(decay_rate, place * NARROW, NARROW, 0)
    gains = lax.dynamic_slice_in_dim(skip_gain, place * NARROW, NARROW, 0)
    weights = jnp.pad(first_layer.T * (0.5 / math.pi), ((0, 0), (0, COLS // 2 - embed)))
    weights = jnp.concatenate([weights, weights], axis=1)
    eight = jnp.pad(columns, ((0, 0), (0, 8 - NARROW)))
    tiled = jnp.pad(jnp.concatenate([eight] * 3, axis=1), ((0, 0), (0, COLS - 24)))
    rates = jnp.broadcast_to(jnp.pad(rates, (0, 8 - NARROW))[:, None], (8, COLS))

    full = (order, LENGTH)
    four = (NARROW, ROWS, COLS)
    wide = (NARROW, ROWS, 2 * COLS)
    kept = ((full, bf16), (full, bf16), (full, f32), (four, f32), (four, f32))
    tall = (ROWS * 8, COLS)
    *state, norms, spectra = call(
        filter_kernel, "make_filter",
        tuple(pltpu.HBM(*k) for k in kept) + (shape((8, COLS), f32), pltpu.HBM(wide, f32)),
        [vmem] * 9,
        (
            weights, eight.T, rates, t["rows"], t["spread"],
            t["forward_left"], t["forward_right"], t["twist_cos"], t["twist_sin"],
        ),
        40, flops=20_000_000_000,
        scratch=[pltpu.VMEM(*k) for k in kept] + [
            pltpu.VMEM(wide, f32), pltpu.VMEM(tall, f32), pltpu.VMEM(tall, f32),
            pltpu.SemaphoreType.DMA((6,)),
        ],
        out_specs=(hbm,) * 5 + (vmem, hbm),
    )
    small, first, cotan = call(
        main_kernel, "correlate",
        (shape((3, COLS), f32), shape((20, COLS), f32), shape(wide, f32)),
        [vmem] * 11 + [hbm] * 5,
        (
            spread, tiled, norms, t["rows"], t["gather"],
            t["forward_left"], t["forward_right"], t["inverse_left"], t["inverse_right"],
            t["twist_cos"], t["twist_sin"], *map(keep, state),
        ),
        40, flops=10_000_000_000,
        scratch=[pltpu.VMEM(*k) for k in kept] + [
            pltpu.VMEM(tall, f32), pltpu.VMEM(wide, f32),
            pltpu.SemaphoreType.DMA((2,)), pltpu.SemaphoreType.DMA((3, ROWS // TAIL_BATCH)),
        ],
    )

    quarter = first.shape[0] // sides
    pieces = [lax.dynamic_slice_in_dim(first, side * quarter, quarter, 0)]
    for step in range(1, sides):
        ring = [(i, (i + step) % sides) for i in range(sides)]
        piece = lax.dynamic_slice_in_dim(first, (side + step) % sides * quarter, quarter, 0)
        pieces.append(lax.ppermute(piece, "chan", ring))
    (grad,) = call(
        input_kernel, "input_grad", (shape((groups * rows, COLS), f32),),
        [vmem, smem] + [vmem] * 6,
        (
            spread, gains, spectra, cotan, t["inverse_left"], t["inverse_right"],
            t["twist_cos"], t["twist_sin"],
        ),
        16, flops=4_000_000_000,
    )
    (back,) = call(
        join_kernel, "join", (shape((groups, rows + 8, COLS), f32),), [vmem] * 6,
        (grad, small, *pieces), 8, scratch=[pltpu.VMEM((8, COLS), f32)],
    )
    home = lax.all_to_all(back, "batch", split_axis=0, concat_axis=0, tiled=True)

    mine = home[:, rows + 3 :].sum(0)
    gathered = [mine]
    for step in range(1, sides):
        ring = [((i + step) % sides, i) for i in range(sides)]
        gathered.append(lax.ppermute(mine, "chan", ring))
    input_grad, second_grad, decay_grad, skip_grad = call(
        unpack_kernel, "unpack",
        (
            shape(signal.shape, f32), shape(second_layer.shape, f32),
            shape((1,) + decay_rate.shape, f32), shape((1,) + skip_gain.shape, f32),
        ),
        [vmem] * 2, (home.reshape(groups // 2, 2, -1, COLS), home.reshape(-1, COLS)), 8,
        flops=1_000_000_000,
    )
    (first_grad,) = call(
        finish_kernel, "finish", (shape((embed, order), f32),), [smem] + [vmem] * 4,
        (side.reshape(1), *gathered), 4,
        scratch=[pltpu.VMEM((sides * quarter, 2 * order), f32)],
    )
    return (input_grad, first_grad, second_grad, decay_grad[0], skip_grad[0])


def solution(mesh):
    placed = (P("chan", "batch"), P("chan", "batch"), P(), P(None, "chan"), P("chan"), P("chan"))
    return jax.shard_map(
        local,
        mesh=mesh,
        in_specs=placed,
        out_specs=(P("chan", "batch"), P(), P(None, "chan"), P("chan"), P("chan")),
        check_vma=False,
    )
```

```python
import math

import jax
import jax.numpy as jnp
import numpy as np
from jax import lax
from jax.experimental import pallas as pl
from jax.experimental.pallas import tpu as pltpu
from jax.sharding import PartitionSpec as P

ROWS = 256
COLS = 128
LENGTH = ROWS * COLS
NARROW = 4
FILTER_BATCH = 16
TAIL_BATCH = 64
TINY = 1e-06
f32 = jnp.float32
bf16 = jnp.bfloat16
highest = lax.Precision.HIGHEST


def halves(x):
    high = x.astype(bf16)
    low = (x - high.astype(np.float64)).astype(bf16)
    return high, low


SIN = (6.28318528, -10.33542017, 5.100155046, -1.196582571, 0.1553153206)
COS = (0.9999999532, -4.934792831, 4.058411353, -1.331876568, 0.2196896111)


def make_tables(embed):
    a = np.arange(ROWS)
    k = np.arange(ROWS)
    m = np.arange(COLS)
    bands = embed // 2
    turn = np.pi * ((a[None, :] * (4 * k + 1)[:, None]) % (4 * ROWS)) / (2 * ROWS)
    first = np.concatenate([np.cos(turn), -np.sin(turn)], axis=0)
    twist = np.pi * (4 * k + 1)[:, None] * m[None, :] / (2 * LENGTH)
    angle = 2.0 * np.pi * ((m[:, None] * m[None, :]) % COLS) / COLS
    c, s = np.cos(angle), np.sin(angle)
    second = np.concatenate(
        [np.concatenate([c, -s], axis=1), np.concatenate([s, c], axis=1)], axis=0
    )
    high, low = halves(first)
    forward_left = np.concatenate([high, low], axis=1)
    inverse_left = np.concatenate([high.T, low.T], axis=1)
    high, low = halves(second)
    forward_right = np.concatenate([high, low], axis=0)
    inverse_right = np.concatenate([high.T, low.T], axis=0)
    rows = np.zeros((ROWS, COLS))
    lanes = np.zeros((COLS, COLS))
    half = COLS // 2
    rows[:, 0] = a * COLS / LENGTH
    lanes[0] = 1.0
    rows[:, half] = 1.0
    lanes[half] = m / LENGTH
    for b in range(1, bands + 1):
        big = 2.0 * np.pi * ((b * COLS * a) % LENGTH) / LENGTH
        small = 2.0 * np.pi * b * m / LENGTH
        rows[:, b] = np.cos(big)
        rows[:, half + b] = -np.sin(big)
        rows[:, bands + b] = np.sin(big)
        rows[:, half + bands + b] = np.cos(big)
        lanes[b] = np.cos(small)
        lanes[half + b] = np.sin(small)
        lanes[bands + b] = np.cos(small)
        lanes[half + bands + b] = np.sin(small)
    high, low = halves(lanes.T)
    gather = np.concatenate([high, low], axis=1)
    high, low = halves(lanes)
    lowest = (lanes - high.astype(np.float64) - low.astype(np.float64)).astype(bf16)
    spread = np.concatenate([high, low, lowest], axis=0)
    return dict(
        forward_left=forward_left,
        inverse_left=inverse_left,
        forward_right=forward_right,
        inverse_right=inverse_right,
        twist_cos=np.cos(twist).astype(np.float32),
        twist_sin=np.sin(twist).astype(np.float32),
        rows=rows.astype(np.float32),
        spread=spread,
        gather=gather,
    )


def split(x):
    high = x.astype(bf16)
    low = (x - high.astype(f32)).astype(bf16)
    return high, low


def mm(left, right):
    return lax.dot_general(left, right, (((1,), (0,)), ((), ())), preferred_element_type=f32)


def dot_rows(table, x):
    high, low = split(x)
    left = jnp.concatenate([table, table[:, : x.shape[0]]], axis=1)
    return mm(left, jnp.concatenate([high, high, low], axis=0))


def dot_cols(x, table):
    high, low = split(x)
    count = x.shape[1]
    right = jnp.concatenate([table[:count], table], axis=0)
    return mm(jnp.concatenate([high, low, high], axis=1), right)


def forward_pair(x, y, left, right, twist_cos, twist_sin):
    u = dot_rows(left, jnp.concatenate([x, y], axis=1))
    spectra = []
    for n in range(2):
        re = u[:ROWS, n * COLS : (n + 1) * COLS]
        im = u[ROWS:, n * COLS : (n + 1) * COLS]
        v = jnp.concatenate(
            [re * twist_cos + im * twist_sin, im * twist_cos - re * twist_sin], axis=1
        )
        spectra.append(dot_cols(v, right))
    return spectra


def times_conj(f, c):
    fr, fi, cr, ci = f[:, :COLS], f[:, COLS:], c[:, :COLS], c[:, COLS:]
    return jnp.concatenate([fr * cr + fi * ci, fr * ci - fi * cr], axis=1)


def inverse_pair(g, h, left, right, twist_cos, twist_sin):
    parts = []
    for x in (g, h):
        w = dot_cols(x, right)
        re, im = w[:, :COLS], w[:, COLS:]
        parts.append(
            jnp.concatenate(
                [re * twist_cos - im * twist_sin, im * twist_cos + re * twist_sin], axis=0
            )
        )
    y = dot_rows(left, jnp.concatenate(parts, axis=1))
    return y[:, :COLS], y[:, COLS:]


def sin_and_cos(x):
    r = x - ((x + 12582912.0) - 12582912.0)
    z = r * r
    s = SIN[4]
    for n in (3, 2, 1, 0):
        s = s * z + SIN[n]
    s = s * r
    c = COS[4]
    for n in (3, 2, 1, 0):
        c = c * z + COS[n]
    return s * c, 1.0 - 0.5 * (s * s)


def fraction_rows(count, offset):
    a = lax.broadcasted_iota(jnp.int32, (count, COLS), 0) + offset
    m = lax.broadcasted_iota(jnp.int32, (count, COLS), 1)
    return (a * COLS + m).astype(f32) * (1.0 / LENGTH)


def zip_rows(x, y):
    low = lax.broadcasted_iota(jnp.int32, x.shape, 0) % 8 < 4
    count = x.shape[0]
    return (
        jnp.where(low, x, pltpu.roll(y, 4, 0)),
        jnp.where(low, pltpu.roll(x, count - 4, 0), y),
    )


def pack_kernel(signal, cotangent, out, values, turned, into, outof):
    quarters = signal.shape[1] // COLS
    reads, writes = [], []
    for q in range(quarters):
        here = pl.ds(q * COLS, COLS)
        for n, source in enumerate((signal, cotangent)):
            copy = pltpu.make_async_copy(source.at[:, here], values.at[q, n], into.at[q, n])
            copy.start()
            reads.append(copy)
    for q in range(quarters):
        for copy in reads[2 * q : 2 * q + 2]:
            copy.wait()
        for n, part in enumerate(zip_rows(values[q, 0], values[q, 1])):
            turned[q, :, n] = part.reshape(-1, 8, COLS)
        copy = pltpu.make_async_copy(
            turned.at[q], out.at[:, :, pl.ds(8 * q, 8), :], outof.at[q]
        )
        copy.start()
        writes.append(copy)
    for copy in writes:
        copy.wait()


def filter_kernel(
    weights, columns, rates, rows, spread, left, right, tcos, tsin,
    high_out, low_out, slope_out, filt_out, window_out, norms, spectra_out,
    high, low, slope, filt, window, spectra, raws, wins, sems,
):
    order = weights.shape[0]
    batch = FILTER_BATCH
    wide = batch * COLS

    def copy(source, target, n, here=None):
        if here is not None:
            source, target = source.at[:, here], target.at[:, here]
        return pltpu.make_async_copy(source, target, sems.at[n])

    mixer = jnp.concatenate(split(columns[...]), axis=0)
    table = jnp.concatenate([spread[...], spread[: 2 * COLS], spread[:COLS]], axis=0)
    lane = lax.broadcasted_iota(jnp.int32, (8, COLS), 1)

    def block(n, total):
        scaled = jnp.concatenate(
            [weights[...] * rows[pl.ds(n * batch + i, 1), :] for i in range(batch)], axis=0
        )
        one = scaled.astype(bf16)
        rest = scaled - one.astype(f32)
        two = rest.astype(bf16)
        three = (rest - two.astype(f32)).astype(bf16)
        turns = mm(jnp.concatenate([one, one, one, two, two, three], axis=1), table)
        for i in range(batch):
            here = pl.ds(pl.multiple_of(n * wide + i * COLS, COLS), COLS)
            s, c = sin_and_cos(turns[i * order : (i + 1) * order])
            slope[:, here] = c
            s_high, s_low = split(s)
            high[:, here] = s_high
            low[:, here] = s_low
        here = pl.ds(pl.multiple_of(n * wide, wide), wide)
        copy(high, high_out, 0, here).start()
        copy(low, low_out, 1, here).start()
        copy(slope, slope_out, 2, here).start()
        p = mm(mixer, high[:, here])
        r = mm(mixer, low[:, here])
        mixed = p[:8] + p[8:] + (r[:8] + r[8:])
        for i in range(batch):
            a = n * batch + i
            fraction = (a * COLS + lane).astype(f32) * (1.0 / LENGTH)
            win = jnp.exp(-rates[...] * fraction)
            raw = win * mixed[:, i * COLS : (i + 1) * COLS]
            raws[pl.ds(pl.multiple_of(a * 8, 8), 8), :] = raw
            wins[pl.ds(pl.multiple_of(a * 8, 8), 8), :] = win
            total = total + raw * raw
        return total

    total = lax.fori_loop(0, ROWS // batch, block, jnp.zeros((8, COLS), f32))
    norm = jnp.sqrt(jnp.sum(total, axis=1, keepdims=True) + TINY)
    norms[...] = jnp.broadcast_to(norm, norms.shape)
    for c in range(NARROW):
        filt[c] = raws[pl.ds(c, ROWS, stride=8), :] / norms[pl.ds(c, 1), :]
        window[c] = wins[pl.ds(c, ROWS, stride=8), :]
    copy(filt, filt_out, 3).start()
    copy(window, window_out, 4).start()
    for c in range(0, NARROW, 2):
        x, y = forward_pair(filt[c], filt[c + 1], left[...], right[...], tcos[...], tsin[...])
        spectra[c] = x
        spectra[c + 1] = y
    copy(spectra, spectra_out, 5).start()
    copy(high, high_out, 0).wait()
    copy(low, low_out, 1).wait()
    copy(slope, slope_out, 2).wait()
    copy(filt, filt_out, 3).wait()
    copy(window, window_out, 4).wait()
    copy(spectra, spectra_out, 5).wait()


def main_kernel(
    both, columns, norms, rows, gather, fleft, fright, ileft, iright, tcos, tsin,
    high_in, low_in, slope_in, filt_in, window_in,
    small, first, cotan,
    high, low, slope, filt, window, dmix, product, early, late,
):
    order = slope.shape[0]
    factor = 1.0 / math.sqrt(LENGTH)
    batch = TAIL_BATCH
    wide = batch * COLS
    starts = [
        pltpu.make_async_copy(source, target, early.at[n])
        for n, (source, target) in enumerate(((filt_in, filt), (window_in, window)))
    ]

    def fetch(n):
        here = pl.ds(pl.multiple_of(n * wide, wide), wide)
        return [
            pltpu.make_async_copy(source.at[:, here], target.at[:, here], late.at[m, n])
            for m, (source, target) in enumerate(((high_in, high), (low_in, low), (slope_in, slope)))
        ]

    for copy in starts:
        copy.start()
    lane = lax.broadcasted_iota(jnp.int32, (1, COLS), 1)
    scalars = jnp.zeros((1, COLS), f32)
    fraction = fraction_rows(ROWS, 0)
    dmix[...] = jnp.zeros(dmix.shape, f32)
    for c in range(NARROW):
        x = both[pl.ds(c, ROWS, stride=2 * NARROW), :]
        y = both[pl.ds(NARROW + c, ROWS, stride=2 * NARROW), :]
        skip = factor * jnp.sum(x * y, keepdims=True)
        scalars = jnp.where(lane == NARROW + c, skip, scalars)
        val, cot = forward_pair(x, y, fleft[...], fright[...], tcos[...], tsin[...])
        if c == 0:
            for copy in starts:
                copy.wait()
            for n in range(ROWS // batch):
                for copy in fetch(n):
                    copy.start()
        cotan[c] = cot
        product[c] = times_conj(val, cot)
    for c in range(0, NARROW, 2):
        pair = inverse_pair(
            product[c], product[c + 1], ileft[...], iright[...], tcos[...], tsin[...]
        )
        for n in range(2):
            i = c + n
            dfilt = pair[n] * (factor / LENGTH)
            project = jnp.sum(filt[i] * dfilt, keepdims=True)
            norm = norms[pl.ds(i, 1), :][:, :1]
            draw = (dfilt - filt[i] * project) / norm
            decay = -jnp.sum(draw * filt[i] * fraction, keepdims=True) * norm
            dmix[pl.ds(i, ROWS, stride=8), :] = draw * window[i]
            scalars = jnp.where(lane == i, decay, scalars)
    doubled = jnp.concatenate([gather[...], gather[...]], axis=0)
    lanes = lax.broadcasted_iota(jnp.int32, columns.shape, 1)
    col_high = columns[...].astype(bf16).astype(f32)
    mixer = jnp.where(lanes // 8 == 2, columns[...] - col_high, col_high).astype(bf16)[:, :32]

    def tail(n, carry):
        firsts, seconds = carry
        for copy in fetch(n):
            copy.wait()
        stack = []
        for i in range(batch):
            d = dmix[pl.ds(pl.multiple_of((n * batch + i) * 8, 8), 8), :]
            d_high = d.astype(bf16).astype(f32)
            stack.append(
                jnp.concatenate([d_high, d - d_high, d_high, jnp.zeros_like(d)], axis=0).astype(bf16)
            )
        stack = jnp.concatenate(stack, axis=1)
        here = pl.ds(pl.multiple_of(n * wide, wide), wide)
        both_halves = jnp.concatenate([high[:, here], low[:, here]], axis=0)
        seconds = seconds + lax.dot_general(
            both_halves, stack[:16], (((1,), (1,)), ((), ())), preferred_element_type=f32
        )
        q = mm(mixer, stack) * slope[:, here]
        q = jnp.concatenate([q[:, i * COLS : (i + 1) * COLS] for i in range(batch)], axis=0)
        r = mm(jnp.concatenate(split(q), axis=1), doubled)
        r = r[:, :COLS] + r[:, COLS:]
        for i in range(batch):
            firsts = firsts + r[i * order : (i + 1) * order] * rows[pl.ds(n * batch + i, 1), :]
        return firsts, seconds

    firsts, seconds = lax.fori_loop(
        0, ROWS // batch, tail,
        (jnp.zeros((order, COLS), f32), jnp.zeros((2 * order, 16), f32)),
    )
    seconds = jnp.transpose(seconds[:order] + seconds[order:], (1, 0))
    seconds = seconds[:8] + seconds[8:]
    small[:1] = jnp.concatenate([seconds[0:1], seconds[1:2]], axis=1)
    small[1:2] = jnp.concatenate([seconds[2:3], seconds[3:4]], axis=1)
    small[2:3] = scalars
    turned = jnp.transpose(firsts, (1, 0))
    half = COLS // 2
    folded = turned[:half] + turned[half:]
    first[...] = jnp.concatenate([folded[:20], folded[20:40]], axis=1)


def input_kernel(both, gains, spectra, cotan, ileft, iright, tcos, tsin, grad):
    for c in range(0, NARROW, 2):
        pair = inverse_pair(
            times_conj(spectra[c], cotan[c]), times_conj(spectra[c + 1], cotan[c + 1]),
            ileft[...], iright[...], tcos[...], tsin[...],
        )
        for n in range(2):
            i = c + n
            y = both[pl.ds(NARROW + i, ROWS, stride=2 * NARROW), :]
            grad[pl.ds(i, ROWS, stride=NARROW), :] = pair[n] * (1.0 / LENGTH) + gains[i] * y


def join_kernel(grad, small, own, one, two, three, out, tile):
    rows = grad.shape[0] // out.shape[0]
    tile[:3] = small[...]
    tile[3:] = own[...] + one[...] + two[...] + three[...]
    out[:, :rows, :] = grad[...].reshape(out.shape[0], rows, COLS)
    out[:, rows:, :] = jnp.broadcast_to(tile[...][None], (out.shape[0],) + tile.shape)


def unpack_kernel(pairs, home, grad, second, decay, skip):
    groups = grad.shape[0] // NARROW
    order = second.shape[0]
    rows = grad.shape[1] // COLS * NARROW
    block = rows + 8
    for p in range(rows // 8):
        even = pairs[:, 0, 8 * p : 8 * p + 8, :].reshape(-1, COLS)
        odd = pairs[:, 1, 8 * p : 8 * p + 8, :].reshape(-1, COLS)
        for n, part in enumerate(zip_rows(even, odd)):
            grad[:, pl.ds((2 * p + n) * COLS, COLS)] = part
    i = lax.broadcasted_iota(jnp.int32, (groups, groups * NARROW), 0)
    j = lax.broadcasted_iota(jnp.int32, (groups, groups * NARROW), 1)
    flat = [jnp.transpose(home[pl.ds(rows + n, groups, stride=block), :], (1, 0)) for n in range(3)]
    total = jnp.zeros(second.shape, f32)
    scalars = jnp.zeros((8, groups * NARROW), f32)
    line = lax.broadcasted_iota(jnp.int32, scalars.shape, 0)
    for c in range(NARROW):
        place = (j == NARROW * i + c).astype(f32)
        mine = flat[c // 2][(c % 2) * order : (c % 2 + 1) * order]
        total = total + jnp.dot(mine, place, precision=highest, preferred_element_type=f32)
        moved = jnp.dot(flat[2][:8], place, precision=highest, preferred_element_type=f32)
        scalars = scalars + jnp.where(line % NARROW == c, moved, 0.0)
    second[...] = total
    decay[...] = jnp.sum(scalars[:NARROW], axis=0, keepdims=True)
    skip[...] = jnp.sum(scalars[NARROW:], axis=0, keepdims=True)


def finish_kernel(side, own, one, two, three, out, table):
    pieces = (own[...], one[...], two[...], three[...])
    count = own.shape[0]
    order = out.shape[1]
    for n in range(len(pieces)):
        chosen = jnp.zeros(own.shape, f32)
        for i, piece in enumerate(pieces):
            chosen = jnp.where((side[0] + i) % len(pieces) == n, piece, chosen)
        table[n * count : (n + 1) * count] = chosen
    total = table.shape[0]
    out[:total] = table[:, :order]
    out[total:] = table[: out.shape[0] - total, order:]


def local(signal, cotangent, first_layer, second_layer, decay_rate, skip_gain):
    groups = lax.axis_size("batch")
    place = lax.axis_index("batch")
    side = lax.axis_index("chan")
    sides = lax.axis_size("chan")
    embed, order = first_layer.shape
    t = make_tables(embed)
    vmem = pl.BlockSpec(memory_space=pltpu.VMEM)
    smem = pl.BlockSpec(memory_space=pltpu.SMEM)
    hbm = pl.BlockSpec(memory_space=pltpu.HBM)
    shape = jax.ShapeDtypeStruct
    rows = signal.shape[1] // COLS * NARROW

    def keep(x):
        return pltpu.with_memory_space_constraint(x, pltpu.HBM)

    def call(body, name, outs, specs, args, mib, flops=0, scratch=(), out_specs=None, lp=True):
        return pl.pallas_call(
            body,
            out_shape=outs,
            in_specs=specs,
            out_specs=out_specs or (vmem,) * len(outs),
            scratch_shapes=list(scratch),
            compiler_params=pltpu.CompilerParams(
                vmem_limit_bytes=mib << 20
            ),
            cost_estimate=pl.CostEstimate(flops=flops, bytes_accessed=0, transcendentals=0),
            name=name,
        )(*args)

    quarters = signal.shape[1] // COLS
    (sent,) = call(
        pack_kernel, "pack", (pltpu.HBM((groups // 2, 2, 2 * rows, COLS), f32),), [hbm] * 2,
        (keep(signal), keep(cotangent)), 8, out_specs=(hbm,),
        scratch=[
            pltpu.VMEM((quarters, 2, signal.shape[0], COLS), f32),
            pltpu.VMEM((quarters, groups // 2, 2, 8, COLS), f32),
            pltpu.SemaphoreType.DMA((quarters, 2)),
            pltpu.SemaphoreType.DMA((quarters,)),
        ],
    )
    spread = lax.all_to_all(
        sent.reshape(groups, 2 * rows, COLS), "batch", split_axis=0, concat_axis=0, tiled=True
    ).reshape(-1, COLS)

    columns = lax.dynamic_slice_in_dim(second_layer, place * NARROW, NARROW, 1)
    rates = lax.dynamic_slice_in_dim(decay_rate, place * NARROW, NARROW, 0)
    gains = lax.dynamic_slice_in_dim(skip_gain, place * NARROW, NARROW, 0)
    weights = jnp.pad(first_layer.T * (0.5 / math.pi), ((0, 0), (0, COLS // 2 - embed)))
    weights = jnp.concatenate([weights, weights], axis=1)
    eight = jnp.pad(columns, ((0, 0), (0, 8 - NARROW)))
    tiled = jnp.pad(jnp.concatenate([eight] * 3, axis=1), ((0, 0), (0, COLS - 24)))
    rates = jnp.broadcast_to(jnp.pad(rates, (0, 8 - NARROW))[:, None], (8, COLS))

    full = (order, LENGTH)
    four = (NARROW, ROWS, COLS)
    wide = (NARROW, ROWS, 2 * COLS)
    kept = ((full, bf16), (full, bf16), (full, f32), (four, f32), (four, f32))
    tall = (ROWS * 8, COLS)
    *state, norms, spectra = call(
        filter_kernel, "make_filter",
        tuple(pltpu.HBM(*k) for k in kept) + (shape((8, COLS), f32), pltpu.HBM(wide, f32)),
        [vmem] * 9,
        (
            weights, eight.T, rates, t["rows"], t["spread"],
            t["forward_left"], t["forward_right"], t["twist_cos"], t["twist_sin"],
        ),
        40, flops=20_000_000_000,
        scratch=[pltpu.VMEM(*k) for k in kept] + [
            pltpu.VMEM(wide, f32), pltpu.VMEM(tall, f32), pltpu.VMEM(tall, f32),
            pltpu.SemaphoreType.DMA((6,)),
        ],
        out_specs=(hbm,) * 5 + (vmem, hbm), lp=False,
    )
    small, first, cotan = call(
        main_kernel, "correlate",
        (shape((3, COLS), f32), shape((20, COLS), f32), shape(wide, f32)),
        [vmem] * 11 + [hbm] * 5,
        (
            spread, tiled, norms, t["rows"], t["gather"],
            t["forward_left"], t["forward_right"], t["inverse_left"], t["inverse_right"],
            t["twist_cos"], t["twist_sin"], *map(keep, state),
        ),
        40, flops=10_000_000_000,
        scratch=[pltpu.VMEM(*k) for k in kept] + [
            pltpu.VMEM(tall, f32), pltpu.VMEM(wide, f32),
            pltpu.SemaphoreType.DMA((2,)), pltpu.SemaphoreType.DMA((3, ROWS // TAIL_BATCH)),
        ],
    )

    quarter = first.shape[0] // sides
    pieces = [lax.dynamic_slice_in_dim(first, side * quarter, quarter, 0)]
    for step in range(1, sides):
        ring = [(i, (i + step) % sides) for i in range(sides)]
        piece = lax.dynamic_slice_in_dim(first, (side + step) % sides * quarter, quarter, 0)
        pieces.append(lax.ppermute(piece, "chan", ring))
    (grad,) = call(
        input_kernel, "input_grad", (shape((groups * rows, COLS), f32),),
        [vmem, smem] + [vmem] * 6,
        (
            spread, gains, spectra, cotan, t["inverse_left"], t["inverse_right"],
            t["twist_cos"], t["twist_sin"],
        ),
        16, flops=4_000_000_000,
    )
    (back,) = call(
        join_kernel, "join", (shape((groups, rows + 8, COLS), f32),), [vmem] * 6,
        (grad, small, *pieces), 8, scratch=[pltpu.VMEM((8, COLS), f32)],
    )
    home = lax.all_to_all(back, "batch", split_axis=0, concat_axis=0, tiled=True)

    mine = home[:, rows + 3 :].sum(0)
    gathered = [mine]
    for step in range(1, sides):
        ring = [((i + step) % sides, i) for i in range(sides)]
        gathered.append(lax.ppermute(mine, "chan", ring))
    input_grad, second_grad, decay_grad, skip_grad = call(
        unpack_kernel, "unpack",
        (
            shape(signal.shape, f32), shape(second_layer.shape, f32),
            shape((1,) + decay_rate.shape, f32), shape((1,) + skip_gain.shape, f32),
        ),
        [vmem] * 2, (home.reshape(groups // 2, 2, -1, COLS), home.reshape(-1, COLS)), 8,
        flops=1_000_000_000,
    )
    (first_grad,) = call(
        finish_kernel, "finish", (shape((embed, order), f32),), [smem] + [vmem] * 4,
        (side.reshape(1), *gathered), 4,
        scratch=[pltpu.VMEM((sides * quarter, 2 * order), f32)],
    )
    return (input_grad, first_grad, second_grad, decay_grad[0], skip_grad[0])


def solution(mesh):
    placed = (P("chan", "batch"), P("chan", "batch"), P(), P(None, "chan"), P("chan"), P("chan"))
    return jax.shard_map(
        local,
        mesh=mesh,
        in_specs=placed,
        out_specs=(P("chan", "batch"), P(), P(None, "chan"), P("chan"), P("chan")),
        check_vma=False,
    )
```

```python
import math

import jax
import jax.numpy as jnp
import numpy as np
from jax import lax
from jax.experimental import pallas as pl
from jax.experimental.pallas import tpu as pltpu
from jax.sharding import PartitionSpec as P

ROWS = 256
COLS = 128
LENGTH = ROWS * COLS
NARROW = 4
FILTER_BATCH = 16
TAIL_BATCH = 64
TINY = 1e-06
f32 = jnp.float32
bf16 = jnp.bfloat16
highest = lax.Precision.HIGHEST


def halves(x):
    high = x.astype(bf16)
    low = (x - high.astype(np.float64)).astype(bf16)
    return high, low


SIN = (6.28318528, -10.33542017, 5.100155046, -1.196582571, 0.1553153206)
COS = (0.9999999532, -4.934792831, 4.058411353, -1.331876568, 0.2196896111)


def make_tables(embed):
    a = np.arange(ROWS)
    k = np.arange(ROWS)
    m = np.arange(COLS)
    bands = embed // 2
    turn = np.pi * ((a[None, :] * (4 * k + 1)[:, None]) % (4 * ROWS)) / (2 * ROWS)
    first = np.concatenate([np.cos(turn), -np.sin(turn)], axis=0)
    twist = np.pi * (4 * k + 1)[:, None] * m[None, :] / (2 * LENGTH)
    angle = 2.0 * np.pi * ((m[:, None] * m[None, :]) % COLS) / COLS
    c, s = np.cos(angle), np.sin(angle)
    second = np.concatenate(
        [np.concatenate([c, -s], axis=1), np.concatenate([s, c], axis=1)], axis=0
    )
    high, low = halves(first)
    forward_left = np.concatenate([high, low], axis=1)
    inverse_left = np.concatenate([high.T, low.T], axis=1)
    high, low = halves(second)
    forward_right = np.concatenate([high, low], axis=0)
    inverse_right = np.concatenate([high.T, low.T], axis=0)
    rows = np.zeros((ROWS, COLS))
    lanes = np.zeros((COLS, COLS))
    half = COLS // 2
    rows[:, 0] = a * COLS / LENGTH
    lanes[0] = 1.0
    rows[:, half] = 1.0
    lanes[half] = m / LENGTH
    for b in range(1, bands + 1):
        big = 2.0 * np.pi * ((b * COLS * a) % LENGTH) / LENGTH
        small = 2.0 * np.pi * b * m / LENGTH
        rows[:, b] = np.cos(big)
        rows[:, half + b] = -np.sin(big)
        rows[:, bands + b] = np.sin(big)
        rows[:, half + bands + b] = np.cos(big)
        lanes[b] = np.cos(small)
        lanes[half + b] = np.sin(small)
        lanes[bands + b] = np.cos(small)
        lanes[half + bands + b] = np.sin(small)
    high, low = halves(lanes.T)
    gather = np.concatenate([high, low], axis=1)
    high, low = halves(lanes)
    lowest = (lanes - high.astype(np.float64) - low.astype(np.float64)).astype(bf16)
    spread = np.concatenate([high, low, lowest], axis=0)
    return dict(
        forward_left=forward_left,
        inverse_left=inverse_left,
        forward_right=forward_right,
        inverse_right=inverse_right,
        twist_cos=np.cos(twist).astype(np.float32),
        twist_sin=np.sin(twist).astype(np.float32),
        rows=rows.astype(np.float32),
        spread=spread,
        gather=gather,
    )


def split(x):
    high = x.astype(bf16)
    low = (x - high.astype(f32)).astype(bf16)
    return high, low


def mm(left, right):
    return lax.dot_general(left, right, (((1,), (0,)), ((), ())), preferred_element_type=f32)


def dot_rows(table, x):
    high, low = split(x)
    left = jnp.concatenate([table, table[:, : x.shape[0]]], axis=1)
    return mm(left, jnp.concatenate([high, high, low], axis=0))


def dot_cols(x, table):
    high, low = split(x)
    count = x.shape[1]
    right = jnp.concatenate([table[:count], table], axis=0)
    return mm(jnp.concatenate([high, low, high], axis=1), right)


def forward_pair(x, y, left, right, twist_cos, twist_sin):
    u = dot_rows(left, jnp.concatenate([x, y], axis=1))
    spectra = []
    for n in range(2):
        re = u[:ROWS, n * COLS : (n + 1) * COLS]
        im = u[ROWS:, n * COLS : (n + 1) * COLS]
        v = jnp.concatenate(
            [re * twist_cos + im * twist_sin, im * twist_cos - re * twist_sin], axis=1
        )
        spectra.append(dot_cols(v, right))
    return spectra


def times_conj(f, c):
    fr, fi, cr, ci = f[:, :COLS], f[:, COLS:], c[:, :COLS], c[:, COLS:]
    return jnp.concatenate([fr * cr + fi * ci, fr * ci - fi * cr], axis=1)


def inverse_pair(g, h, left, right, twist_cos, twist_sin):
    parts = []
    for x in (g, h):
        w = dot_cols(x, right)
        re, im = w[:, :COLS], w[:, COLS:]
        parts.append(
            jnp.concatenate(
                [re * twist_cos - im * twist_sin, im * twist_cos + re * twist_sin], axis=0
            )
        )
    y = dot_rows(left, jnp.concatenate(parts, axis=1))
    return y[:, :COLS], y[:, COLS:]


def sin_and_cos(x):
    r = x - ((x + 12582912.0) - 12582912.0)
    z = r * r
    s = SIN[4]
    for n in (3, 2, 1, 0):
        s = s * z + SIN[n]
    s = s * r
    c = COS[4]
    for n in (3, 2, 1, 0):
        c = c * z + COS[n]
    return s * c, 1.0 - 0.5 * (s * s)


def fraction_rows(count, offset):
    a = lax.broadcasted_iota(jnp.int32, (count, COLS), 0) + offset
    m = lax.broadcasted_iota(jnp.int32, (count, COLS), 1)
    return (a * COLS + m).astype(f32) * (1.0 / LENGTH)


def zip_rows(x, y):
    low = lax.broadcasted_iota(jnp.int32, x.shape, 0) % 8 < 4
    count = x.shape[0]
    return (
        jnp.where(low, x, pltpu.roll(y, 4, 0)),
        jnp.where(low, pltpu.roll(x, count - 4, 0), y),
    )


def pack_kernel(signal, cotangent, out, values, turned, into, outof):
    quarters = signal.shape[1] // COLS
    reads, writes = [], []
    for q in range(quarters):
        here = pl.ds(q * COLS, COLS)
        for n, source in enumerate((signal, cotangent)):
            copy = pltpu.make_async_copy(source.at[:, here], values.at[q, n], into.at[q, n])
            copy.start()
            reads.append(copy)
    for q in range(quarters):
        for copy in reads[2 * q : 2 * q + 2]:
            copy.wait()
        for n, part in enumerate(zip_rows(values[q, 0], values[q, 1])):
            turned[q, :, n] = part.reshape(-1, 8, COLS)
        copy = pltpu.make_async_copy(
            turned.at[q], out.at[:, :, pl.ds(8 * q, 8), :], outof.at[q]
        )
        copy.start()
        writes.append(copy)
    for copy in writes:
        copy.wait()


def filter_kernel(
    weights, columns, rates, rows, spread, left, right, tcos, tsin,
    high_out, low_out, slope_out, filt_out, window_out, norms, spectra_out,
    high, low, slope, filt, window, spectra, raws, wins, sems,
):
    order = weights.shape[0]
    batch = FILTER_BATCH
    wide = batch * COLS

    def copy(source, target, n, here=None):
        if here is not None:
            source, target = source.at[:, here], target.at[:, here]
        return pltpu.make_async_copy(source, target, sems.at[n])

    mixer = jnp.concatenate(split(columns[...]), axis=0)
    table = jnp.concatenate([spread[...], spread[: 2 * COLS], spread[:COLS]], axis=0)
    lane = lax.broadcasted_iota(jnp.int32, (8, COLS), 1)

    def block(n, total):
        scaled = jnp.concatenate(
            [weights[...] * rows[pl.ds(n * batch + i, 1), :] for i in range(batch)], axis=0
        )
        one = scaled.astype(bf16)
        rest = scaled - one.astype(f32)
        two = rest.astype(bf16)
        three = (rest - two.astype(f32)).astype(bf16)
        turns = mm(jnp.concatenate([one, one, one, two, two, three], axis=1), table)
        for i in range(batch):
            here = pl.ds(pl.multiple_of(n * wide + i * COLS, COLS), COLS)
            s, c = sin_and_cos(turns[i * order : (i + 1) * order])
            slope[:, here] = c
            s_high, s_low = split(s)
            high[:, here] = s_high
            low[:, here] = s_low
        here = pl.ds(pl.multiple_of(n * wide, wide), wide)
        copy(high, high_out, 0, here).start()
        copy(low, low_out, 1, here).start()
        copy(slope, slope_out, 2, here).start()
        p = mm(mixer, high[:, here])
        r = mm(mixer, low[:, here])
        mixed = p[:8] + p[8:] + (r[:8] + r[8:])
        for i in range(batch):
            a = n * batch + i
            fraction = (a * COLS + lane).astype(f32) * (1.0 / LENGTH)
            win = jnp.exp(-rates[...] * fraction)
            raw = win * mixed[:, i * COLS : (i + 1) * COLS]
            raws[pl.ds(pl.multiple_of(a * 8, 8), 8), :] = raw
            wins[pl.ds(pl.multiple_of(a * 8, 8), 8), :] = win
            total = total + raw * raw
        return total

    total = lax.fori_loop(0, ROWS // batch, block, jnp.zeros((8, COLS), f32))
    norm = jnp.sqrt(jnp.sum(total, axis=1, keepdims=True) + TINY)
    norms[...] = jnp.broadcast_to(norm, norms.shape)
    for c in range(NARROW):
        filt[c] = raws[pl.ds(c, ROWS, stride=8), :] / norms[pl.ds(c, 1), :]
        window[c] = wins[pl.ds(c, ROWS, stride=8), :]
    copy(filt, filt_out, 3).start()
    copy(window, window_out, 4).start()
    for c in range(0, NARROW, 2):
        x, y = forward_pair(filt[c], filt[c + 1], left[...], right[...], tcos[...], tsin[...])
        spectra[c] = x
        spectra[c + 1] = y
    copy(spectra, spectra_out, 5).start()
    copy(high, high_out, 0).wait()
    copy(low, low_out, 1).wait()
    copy(slope, slope_out, 2).wait()
    copy(filt, filt_out, 3).wait()
    copy(window, window_out, 4).wait()
    copy(spectra, spectra_out, 5).wait()


def main_kernel(
    both, columns, norms, rows, gather, fleft, fright, ileft, iright, tcos, tsin,
    high_in, low_in, slope_in, filt_in, window_in,
    small, first, cotan,
    high, low, slope, filt, window, dmix, product, early, late,
):
    order = slope.shape[0]
    factor = 1.0 / math.sqrt(LENGTH)
    batch = TAIL_BATCH
    wide = batch * COLS
    starts = [
        pltpu.make_async_copy(source, target, early.at[n])
        for n, (source, target) in enumerate(((filt_in, filt), (window_in, window)))
    ]

    def fetch(n):
        here = pl.ds(pl.multiple_of(n * wide, wide), wide)
        return [
            pltpu.make_async_copy(source.at[:, here], target.at[:, here], late.at[m, n])
            for m, (source, target) in enumerate(((high_in, high), (low_in, low), (slope_in, slope)))
        ]

    for copy in starts:
        copy.start()
    lane = lax.broadcasted_iota(jnp.int32, (1, COLS), 1)
    scalars = jnp.zeros((1, COLS), f32)
    fraction = fraction_rows(ROWS, 0)
    dmix[...] = jnp.zeros(dmix.shape, f32)
    for c in range(NARROW):
        x = both[pl.ds(c, ROWS, stride=2 * NARROW), :]
        y = both[pl.ds(NARROW + c, ROWS, stride=2 * NARROW), :]
        skip = factor * jnp.sum(x * y, keepdims=True)
        scalars = jnp.where(lane == NARROW + c, skip, scalars)
        val, cot = forward_pair(x, y, fleft[...], fright[...], tcos[...], tsin[...])
        if c == 0:
            for copy in starts:
                copy.wait()
            for n in range(ROWS // batch):
                for copy in fetch(n):
                    copy.start()
        cotan[c] = cot
        product[c] = times_conj(val, cot)
    for c in range(0, NARROW, 2):
        pair = inverse_pair(
            product[c], product[c + 1], ileft[...], iright[...], tcos[...], tsin[...]
        )
        for n in range(2):
            i = c + n
            dfilt = pair[n] * (factor / LENGTH)
            project = jnp.sum(filt[i] * dfilt, keepdims=True)
            norm = norms[pl.ds(i, 1), :][:, :1]
            draw = (dfilt - filt[i] * project) / norm
            decay = -jnp.sum(draw * filt[i] * fraction, keepdims=True) * norm
            dmix[pl.ds(i, ROWS, stride=8), :] = draw * window[i]
            scalars = jnp.where(lane == i, decay, scalars)
    doubled = jnp.concatenate([gather[...], gather[...]], axis=0)
    lanes = lax.broadcasted_iota(jnp.int32, columns.shape, 1)
    col_high = columns[...].astype(bf16).astype(f32)
    mixer = jnp.where(lanes // 8 == 2, columns[...] - col_high, col_high).astype(bf16)[:, :32]

    def tail(n, carry):
        firsts, seconds = carry
        for copy in fetch(n):
            copy.wait()
        stack = []
        for i in range(batch):
            d = dmix[pl.ds(pl.multiple_of((n * batch + i) * 8, 8), 8), :]
            d_high = d.astype(bf16).astype(f32)
            stack.append(
                jnp.concatenate([d_high, d - d_high, d_high, jnp.zeros_like(d)], axis=0).astype(bf16)
            )
        stack = jnp.concatenate(stack, axis=1)
        here = pl.ds(pl.multiple_of(n * wide, wide), wide)
        both_halves = jnp.concatenate([high[:, here], low[:, here]], axis=0)
        seconds = seconds + lax.dot_general(
            both_halves, stack[:16], (((1,), (1,)), ((), ())), preferred_element_type=f32
        )
        q = mm(mixer, stack) * slope[:, here]
        q = jnp.concatenate([q[:, i * COLS : (i + 1) * COLS] for i in range(batch)], axis=0)
        r = mm(jnp.concatenate(split(q), axis=1), doubled)
        r = r[:, :COLS] + r[:, COLS:]
        for i in range(batch):
            firsts = firsts + r[i * order : (i + 1) * order] * rows[pl.ds(n * batch + i, 1), :]
        return firsts, seconds

    firsts, seconds = lax.fori_loop(
        0, ROWS // batch, tail,
        (jnp.zeros((order, COLS), f32), jnp.zeros((2 * order, 16), f32)),
    )
    seconds = jnp.transpose(seconds[:order] + seconds[order:], (1, 0))
    seconds = seconds[:8] + seconds[8:]
    small[:1] = jnp.concatenate([seconds[0:1], seconds[1:2]], axis=1)
    small[1:2] = jnp.concatenate([seconds[2:3], seconds[3:4]], axis=1)
    small[2:3] = scalars
    turned = jnp.transpose(firsts, (1, 0))
    half = COLS // 2
    folded = turned[:half] + turned[half:]
    first[...] = jnp.concatenate([folded[:20], folded[20:40]], axis=1)


def input_kernel(both, gains, spectra, cotan, ileft, iright, tcos, tsin, grad):
    for c in range(0, NARROW, 2):
        pair = inverse_pair(
            times_conj(spectra[c], cotan[c]), times_conj(spectra[c + 1], cotan[c + 1]),
            ileft[...], iright[...], tcos[...], tsin[...],
        )
        for n in range(2):
            i = c + n
            y = both[pl.ds(NARROW + i, ROWS, stride=2 * NARROW), :]
            grad[pl.ds(i, ROWS, stride=NARROW), :] = pair[n] * (1.0 / LENGTH) + gains[i] * y


def join_kernel(grad, small, own, one, two, three, out, tile):
    rows = grad.shape[0] // out.shape[0]
    tile[:3] = small[...]
    tile[3:] = own[...] + one[...] + two[...] + three[...]
    out[:, :rows, :] = grad[...].reshape(out.shape[0], rows, COLS)
    out[:, rows:, :] = jnp.broadcast_to(tile[...][None], (out.shape[0],) + tile.shape)


def unpack_kernel(pairs, home, grad, second, decay, skip):
    groups = grad.shape[0] // NARROW
    order = second.shape[0]
    rows = grad.shape[1] // COLS * NARROW
    block = rows + 8
    for p in range(rows // 8):
        even = pairs[:, 0, 8 * p : 8 * p + 8, :].reshape(-1, COLS)
        odd = pairs[:, 1, 8 * p : 8 * p + 8, :].reshape(-1, COLS)
        for n, part in enumerate(zip_rows(even, odd)):
            grad[:, pl.ds((2 * p + n) * COLS, COLS)] = part
    i = lax.broadcasted_iota(jnp.int32, (groups, groups * NARROW), 0)
    j = lax.broadcasted_iota(jnp.int32, (groups, groups * NARROW), 1)
    flat = [jnp.transpose(home[pl.ds(rows + n, groups, stride=block), :], (1, 0)) for n in range(3)]
    total = jnp.zeros(second.shape, f32)
    scalars = jnp.zeros((8, groups * NARROW), f32)
    line = lax.broadcasted_iota(jnp.int32, scalars.shape, 0)
    for c in range(NARROW):
        place = (j == NARROW * i + c).astype(f32)
        mine = flat[c // 2][(c % 2) * order : (c % 2 + 1) * order]
        total = total + jnp.dot(mine, place, precision=highest, preferred_element_type=f32)
        moved = jnp.dot(flat[2][:8], place, precision=highest, preferred_element_type=f32)
        scalars = scalars + jnp.where(line % NARROW == c, moved, 0.0)
    second[...] = total
    decay[...] = jnp.sum(scalars[:NARROW], axis=0, keepdims=True)
    skip[...] = jnp.sum(scalars[NARROW:], axis=0, keepdims=True)


def finish_kernel(side, own, three, two, one, out, table):
    pieces = (own[...], one[...], two[...], three[...])
    count = own.shape[0]
    order = out.shape[1]
    for n in range(len(pieces)):
        chosen = jnp.zeros(own.shape, f32)
        for i, piece in enumerate(pieces):
            chosen = jnp.where((side[0] ^ i) == n, piece, chosen)
        table[n * count : (n + 1) * count] = chosen
    total = table.shape[0]
    out[:total] = table[:, :order]
    out[total:] = table[: out.shape[0] - total, order:]


def local(signal, cotangent, first_layer, second_layer, decay_rate, skip_gain):
    groups = lax.axis_size("batch")
    place = lax.axis_index("batch")
    side = lax.axis_index("chan")
    sides = lax.axis_size("chan")
    embed, order = first_layer.shape
    t = make_tables(embed)
    vmem = pl.BlockSpec(memory_space=pltpu.VMEM)
    smem = pl.BlockSpec(memory_space=pltpu.SMEM)
    hbm = pl.BlockSpec(memory_space=pltpu.HBM)
    shape = jax.ShapeDtypeStruct
    rows = signal.shape[1] // COLS * NARROW

    def keep(x):
        return pltpu.with_memory_space_constraint(x, pltpu.HBM)

    def call(body, name, outs, specs, args, mib, flops=0, scratch=(), out_specs=None, lp=False):
        return pl.pallas_call(
            body,
            out_shape=outs,
            in_specs=specs,
            out_specs=out_specs or (vmem,) * len(outs),
            scratch_shapes=list(scratch),
            compiler_params=pltpu.CompilerParams(
                vmem_limit_bytes=mib << 20
            ),
            cost_estimate=pl.CostEstimate(flops=flops, bytes_accessed=0, transcendentals=0),
            name=name,
        )(*args)

    quarters = signal.shape[1] // COLS
    (sent,) = call(
        pack_kernel, "pack", (pltpu.HBM((groups // 2, 2, 2 * rows, COLS), f32),), [hbm] * 2,
        (keep(signal), keep(cotangent)), 8, out_specs=(hbm,),
        scratch=[
            pltpu.VMEM((quarters, 2, signal.shape[0], COLS), f32),
            pltpu.VMEM((quarters, groups // 2, 2, 8, COLS), f32),
            pltpu.SemaphoreType.DMA((quarters, 2)),
            pltpu.SemaphoreType.DMA((quarters,)),
        ],
    )
    spread = lax.all_to_all(
        sent.reshape(groups, 2 * rows, COLS), "batch", split_axis=0, concat_axis=0, tiled=True
    ).reshape(-1, COLS)

    columns = lax.dynamic_slice_in_dim(second_layer, place * NARROW, NARROW, 1)
    rates = lax.dynamic_slice_in_dim(decay_rate, place * NARROW, NARROW, 0)
    gains = lax.dynamic_slice_in_dim(skip_gain, place * NARROW, NARROW, 0)
    weights = jnp.pad(first_layer.T * (0.5 / math.pi), ((0, 0), (0, COLS // 2 - embed)))
    weights = jnp.concatenate([weights, weights], axis=1)
    eight = jnp.pad(columns, ((0, 0), (0, 8 - NARROW)))
    tiled = jnp.pad(jnp.concatenate([eight] * 3, axis=1), ((0, 0), (0, COLS - 24)))
    rates = jnp.broadcast_to(jnp.pad(rates, (0, 8 - NARROW))[:, None], (8, COLS))

    full = (order, LENGTH)
    four = (NARROW, ROWS, COLS)
    wide = (NARROW, ROWS, 2 * COLS)
    kept = ((full, bf16), (full, bf16), (full, f32), (four, f32), (four, f32))
    tall = (ROWS * 8, COLS)
    *state, norms, spectra = call(
        filter_kernel, "make_filter",
        tuple(pltpu.HBM(*k) for k in kept) + (shape((8, COLS), f32), pltpu.HBM(wide, f32)),
        [vmem] * 9,
        (
            weights, eight.T, rates, t["rows"], t["spread"],
            t["forward_left"], t["forward_right"], t["twist_cos"], t["twist_sin"],
        ),
        40, flops=20_000_000_000,
        scratch=[pltpu.VMEM(*k) for k in kept] + [
            pltpu.VMEM(wide, f32), pltpu.VMEM(tall, f32), pltpu.VMEM(tall, f32),
            pltpu.SemaphoreType.DMA((6,)),
        ],
        out_specs=(hbm,) * 5 + (vmem, hbm),
    )
    small, first, cotan = call(
        main_kernel, "correlate",
        (shape((3, COLS), f32), shape((20, COLS), f32), shape(wide, f32)),
        [vmem] * 11 + [hbm] * 5,
        (
            spread, tiled, norms, t["rows"], t["gather"],
            t["forward_left"], t["forward_right"], t["inverse_left"], t["inverse_right"],
            t["twist_cos"], t["twist_sin"], *map(keep, state),
        ),
        40, flops=10_000_000_000, lp=True,
        scratch=[pltpu.VMEM(*k) for k in kept] + [
            pltpu.VMEM(tall, f32), pltpu.VMEM(wide, f32),
            pltpu.SemaphoreType.DMA((2,)), pltpu.SemaphoreType.DMA((3, ROWS // TAIL_BATCH)),
        ],
    )

    quarter = first.shape[0] // sides
    pieces = [lax.dynamic_slice_in_dim(first, side * quarter, quarter, 0)]
    for step in reversed(range(1, sides)):
        swap = [(i, i ^ step) for i in range(sides)]
        piece = lax.dynamic_slice_in_dim(first, (side ^ step) * quarter, quarter, 0)
        pieces.append(lax.ppermute(piece, "chan", swap))
    (grad,) = call(
        input_kernel, "input_grad", (shape((groups * rows, COLS), f32),),
        [vmem, smem] + [vmem] * 6,
        (
            spread, gains, spectra, cotan, t["inverse_left"], t["inverse_right"],
            t["twist_cos"], t["twist_sin"],
        ),
        16, flops=4_000_000_000,
    )
    (back,) = call(
        join_kernel, "join", (shape((groups, rows + 8, COLS), f32),), [vmem] * 6,
        (grad, small, *pieces), 8, scratch=[pltpu.VMEM((8, COLS), f32)],
    )
    home = lax.all_to_all(back, "batch", split_axis=0, concat_axis=0, tiled=True)

    mine = home[:, rows + 3 :].sum(0)
    gathered = [mine]
    for step in reversed(range(1, sides)):
        gathered.append(lax.ppermute(mine, "chan", [(i, i ^ step) for i in range(sides)]))
    input_grad, second_grad, decay_grad, skip_grad = call(
        unpack_kernel, "unpack",
        (
            shape(signal.shape, f32), shape(second_layer.shape, f32),
            shape((1,) + decay_rate.shape, f32), shape((1,) + skip_gain.shape, f32),
        ),
        [vmem] * 2, (home.reshape(groups // 2, 2, -1, COLS), home.reshape(-1, COLS)), 8,
        flops=1_000_000_000,
    )
    (first_grad,) = call(
        finish_kernel, "finish", (shape((embed, order), f32),), [smem] + [vmem] * 4,
        (side.reshape(1), *gathered), 4,
        scratch=[pltpu.VMEM((sides * quarter, 2 * order), f32)],
    )
    return (input_grad, first_grad, second_grad, decay_grad[0], skip_grad[0])


def solution(mesh):
    placed = (P("chan", "batch"), P("chan", "batch"), P(), P(None, "chan"), P("chan"), P("chan"))
    return jax.shard_map(
        local,
        mesh=mesh,
        in_specs=placed,
        out_specs=(P("chan", "batch"), P(), P(None, "chan"), P("chan"), P("chan")),
        check_vma=False,
    )
```

```python
import math

import jax
import jax.numpy as jnp
import numpy as np
from jax import lax
from jax.experimental import pallas as pl
from jax.experimental.pallas import tpu as pltpu
from jax.sharding import PartitionSpec as P

ROWS = 256
COLS = 128
LENGTH = ROWS * COLS
NARROW = 4
FILTER_BATCH = 16
TAIL_BATCH = 128
TINY = 1e-06
f32 = jnp.float32
bf16 = jnp.bfloat16
highest = lax.Precision.HIGHEST


def halves(x):
    high = x.astype(bf16)
    low = (x - high.astype(np.float64)).astype(bf16)
    return high, low


SIN = (6.28318528, -10.33542017, 5.100155046, -1.196582571, 0.1553153206)
COS = (0.9999999532, -4.934792831, 4.058411353, -1.331876568, 0.2196896111)


def make_tables(embed):
    a = np.arange(ROWS)
    k = np.arange(ROWS)
    m = np.arange(COLS)
    bands = embed // 2
    turn = np.pi * ((a[None, :] * (4 * k + 1)[:, None]) % (4 * ROWS)) / (2 * ROWS)
    first = np.concatenate([np.cos(turn), -np.sin(turn)], axis=0)
    twist = np.pi * (4 * k + 1)[:, None] * m[None, :] / (2 * LENGTH)
    angle = 2.0 * np.pi * ((m[:, None] * m[None, :]) % COLS) / COLS
    c, s = np.cos(angle), np.sin(angle)
    second = np.concatenate(
        [np.concatenate([c, -s], axis=1), np.concatenate([s, c], axis=1)], axis=0
    )
    high, low = halves(first)
    forward_left = np.concatenate([high, low], axis=1)
    inverse_left = np.concatenate([high.T, low.T], axis=1)
    high, low = halves(second)
    forward_right = np.concatenate([high, low], axis=0)
    inverse_right = np.concatenate([high.T, low.T], axis=0)
    rows = np.zeros((ROWS, COLS))
    lanes = np.zeros((COLS, COLS))
    half = COLS // 2
    rows[:, 0] = a * COLS / LENGTH
    lanes[0] = 1.0
    rows[:, half] = 1.0
    lanes[half] = m / LENGTH
    for b in range(1, bands + 1):
        big = 2.0 * np.pi * ((b * COLS * a) % LENGTH) / LENGTH
        small = 2.0 * np.pi * b * m / LENGTH
        rows[:, b] = np.cos(big)
        rows[:, half + b] = -np.sin(big)
        rows[:, bands + b] = np.sin(big)
        rows[:, half + bands + b] = np.cos(big)
        lanes[b] = np.cos(small)
        lanes[half + b] = np.sin(small)
        lanes[bands + b] = np.cos(small)
        lanes[half + bands + b] = np.sin(small)
    high, low = halves(lanes.T)
    gather = np.concatenate([high, low], axis=1)
    high, low = halves(lanes)
    lowest = (lanes - high.astype(np.float64) - low.astype(np.float64)).astype(bf16)
    spread = np.concatenate([high, low, lowest], axis=0)
    return dict(
        forward_left=forward_left,
        inverse_left=inverse_left,
        forward_right=forward_right,
        inverse_right=inverse_right,
        twist_cos=np.cos(twist).astype(np.float32),
        twist_sin=np.sin(twist).astype(np.float32),
        rows=rows.astype(np.float32),
        spread=spread,
        gather=gather,
    )


def split(x):
    high = x.astype(bf16)
    low = (x - high.astype(f32)).astype(bf16)
    return high, low


def mm(left, right):
    return lax.dot_general(left, right, (((1,), (0,)), ((), ())), preferred_element_type=f32)


def dot_rows(table, x):
    high, low = split(x)
    left = jnp.concatenate([table, table[:, : x.shape[0]]], axis=1)
    return mm(left, jnp.concatenate([high, high, low], axis=0))


def dot_cols(x, table):
    high, low = split(x)
    count = x.shape[1]
    right = jnp.concatenate([table[:count], table], axis=0)
    return mm(jnp.concatenate([high, low, high], axis=1), right)


def forward_pair(x, y, left, right, twist_cos, twist_sin):
    u = dot_rows(left, jnp.concatenate([x, y], axis=1))
    turned = []
    for n in range(2):
        re = u[:ROWS, n * COLS : (n + 1) * COLS]
        im = u[ROWS:, n * COLS : (n + 1) * COLS]
        turned.append(
            jnp.concatenate(
                [re * twist_cos + im * twist_sin, im * twist_cos - re * twist_sin], axis=1
            )
        )
    both = dot_cols(jnp.concatenate(turned, axis=0), right)
    return both[:ROWS], both[ROWS:]


def times_conj(f, c):
    fr, fi, cr, ci = f[:, :COLS], f[:, COLS:], c[:, :COLS], c[:, COLS:]
    return jnp.concatenate([fr * cr + fi * ci, fr * ci - fi * cr], axis=1)


def inverse_pair(g, h, left, right, twist_cos, twist_sin):
    parts = []
    both = dot_cols(jnp.concatenate([g, h], axis=0), right)
    for w in (both[:ROWS], both[ROWS:]):
        re, im = w[:, :COLS], w[:, COLS:]
        parts.append(
            jnp.concatenate(
                [re * twist_cos - im * twist_sin, im * twist_cos + re * twist_sin], axis=0
            )
        )
    y = dot_rows(left, jnp.concatenate(parts, axis=1))
    return y[:, :COLS], y[:, COLS:]


def sin_and_cos(x):
    r = x - ((x + 12582912.0) - 12582912.0)
    z = r * r
    s = SIN[4]
    for n in (3, 2, 1, 0):
        s = s * z + SIN[n]
    s = s * r
    c = COS[4]
    for n in (3, 2, 1, 0):
        c = c * z + COS[n]
    return s * c, 1.0 - 0.5 * (s * s)


def fraction_rows(count, offset):
    a = lax.broadcasted_iota(jnp.int32, (count, COLS), 0) + offset
    m = lax.broadcasted_iota(jnp.int32, (count, COLS), 1)
    return (a * COLS + m).astype(f32) * (1.0 / LENGTH)


def zip_rows(x, y):
    low = lax.broadcasted_iota(jnp.int32, x.shape, 0) % 8 < 4
    count = x.shape[0]
    return (
        jnp.where(low, x, pltpu.roll(y, 4, 0)),
        jnp.where(low, pltpu.roll(x, count - 4, 0), y),
    )


def pack_kernel(signal, cotangent, out, values, turned, into, outof):
    quarters = signal.shape[1] // COLS
    reads, writes = [], []
    for q in range(quarters):
        here = pl.ds(q * COLS, COLS)
        for n, source in enumerate((signal, cotangent)):
            copy = pltpu.make_async_copy(source.at[:, here], values.at[q, n], into.at[q, n])
            copy.start()
            reads.append(copy)
    for q in range(quarters):
        for copy in reads[2 * q : 2 * q + 2]:
            copy.wait()
        for n, part in enumerate(zip_rows(values[q, 0], values[q, 1])):
            turned[q, :, n] = part.reshape(-1, 8, COLS)
        copy = pltpu.make_async_copy(
            turned.at[q], out.at[:, :, pl.ds(8 * q, 8), :], outof.at[q]
        )
        copy.start()
        writes.append(copy)
    for copy in writes:
        copy.wait()


def filter_kernel(
    weights, columns, rates, rows, spread, left, right, tcos, tsin,
    high_out, low_out, slope_out, filt_out, window_out, norms, spectra_out,
    high, low, slope, filt, window, spectra, raws, wins, sems,
):
    order = weights.shape[0]
    batch = FILTER_BATCH
    wide = batch * COLS

    def copy(source, target, n, here=None):
        if here is not None:
            source, target = source.at[:, here], target.at[:, here]
        return pltpu.make_async_copy(source, target, sems.at[n])

    mixer = jnp.concatenate(split(columns[...]), axis=0)
    table = jnp.concatenate([spread[...], spread[: 2 * COLS], spread[:COLS]], axis=0)
    lane = lax.broadcasted_iota(jnp.int32, (8, COLS), 1)

    def block(n, total):
        scaled = jnp.concatenate(
            [weights[...] * rows[pl.ds(n * batch + i, 1), :] for i in range(batch)], axis=0
        )
        one = scaled.astype(bf16)
        rest = scaled - one.astype(f32)
        two = rest.astype(bf16)
        three = (rest - two.astype(f32)).astype(bf16)
        turns = mm(jnp.concatenate([one, one, one, two, two, three], axis=1), table)
        for i in range(batch):
            here = pl.ds(pl.multiple_of(n * wide + i * COLS, COLS), COLS)
            s, c = sin_and_cos(turns[i * order : (i + 1) * order])
            slope[:, here] = c
            s_high, s_low = split(s)
            high[:, here] = s_high
            low[:, here] = s_low
        here = pl.ds(pl.multiple_of(n * wide, wide), wide)
        copy(high, high_out, 0, here).start()
        copy(low, low_out, 1, here).start()
        copy(slope, slope_out, 2, here).start()
        p = mm(mixer, high[:, here])
        r = mm(mixer, low[:, here])
        mixed = p[:8] + p[8:] + (r[:8] + r[8:])
        for i in range(batch):
            a = n * batch + i
            fraction = (a * COLS + lane).astype(f32) * (1.0 / LENGTH)
            win = jnp.exp(-rates[...] * fraction)
            raw = win * mixed[:, i * COLS : (i + 1) * COLS]
            raws[pl.ds(pl.multiple_of(a * 8, 8), 8), :] = raw
            wins[pl.ds(pl.multiple_of(a * 8, 8), 8), :] = win
            total = total + raw * raw
        return total

    total = lax.fori_loop(0, ROWS // batch, block, jnp.zeros((8, COLS), f32))
    norm = jnp.sqrt(jnp.sum(total, axis=1, keepdims=True) + TINY)
    norms[...] = jnp.broadcast_to(norm, norms.shape)
    for c in range(NARROW):
        filt[c] = raws[pl.ds(c, ROWS, stride=8), :] / norms[pl.ds(c, 1), :]
        window[c] = wins[pl.ds(c, ROWS, stride=8), :]
    copy(filt, filt_out, 3).start()
    copy(window, window_out, 4).start()
    for c in range(0, NARROW, 2):
        x, y = forward_pair(filt[c], filt[c + 1], left[...], right[...], tcos[...], tsin[...])
        spectra[c] = x
        spectra[c + 1] = y
    copy(spectra, spectra_out, 5).start()
    copy(high, high_out, 0).wait()
    copy(low, low_out, 1).wait()
    copy(slope, slope_out, 2).wait()
    copy(filt, filt_out, 3).wait()
    copy(window, window_out, 4).wait()
    copy(spectra, spectra_out, 5).wait()


def main_kernel(
    both, columns, norms, rows, gather, fleft, fright, ileft, iright, tcos, tsin,
    high_in, low_in, slope_in, filt_in, window_in,
    small, first, cotan,
    high, low, slope, filt, window, dmix, product, early, late,
):
    order = slope.shape[0]
    factor = 1.0 / math.sqrt(LENGTH)
    batch = TAIL_BATCH
    wide = batch * COLS
    starts = [
        pltpu.make_async_copy(source, target, early.at[n])
        for n, (source, target) in enumerate(((filt_in, filt), (window_in, window)))
    ]

    def fetch(n):
        here = pl.ds(pl.multiple_of(n * wide, wide), wide)
        return [
            pltpu.make_async_copy(source.at[:, here], target.at[:, here], late.at[m, n])
            for m, (source, target) in enumerate(((high_in, high), (low_in, low), (slope_in, slope)))
        ]

    for copy in starts:
        copy.start()
    lane = lax.broadcasted_iota(jnp.int32, (1, COLS), 1)
    scalars = jnp.zeros((1, COLS), f32)
    fraction = fraction_rows(ROWS, 0)
    dmix[...] = jnp.zeros(dmix.shape, f32)
    for c in range(NARROW):
        x = both[pl.ds(c, ROWS, stride=2 * NARROW), :]
        y = both[pl.ds(NARROW + c, ROWS, stride=2 * NARROW), :]
        skip = factor * jnp.sum(x * y, keepdims=True)
        scalars = jnp.where(lane == NARROW + c, skip, scalars)
        val, cot = forward_pair(x, y, fleft[...], fright[...], tcos[...], tsin[...])
        if c == 0:
            for copy in starts:
                copy.wait()
            for n in range(ROWS // batch):
                for copy in fetch(n):
                    copy.start()
        cotan[c] = cot
        product[c] = times_conj(val, cot)
    for c in range(0, NARROW, 2):
        pair = inverse_pair(
            product[c], product[c + 1], ileft[...], iright[...], tcos[...], tsin[...]
        )
        for n in range(2):
            i = c + n
            dfilt = pair[n] * (factor / LENGTH)
            project = jnp.sum(filt[i] * dfilt, keepdims=True)
            norm = norms[pl.ds(i, 1), :][:, :1]
            draw = (dfilt - filt[i] * project) / norm
            decay = -jnp.sum(draw * filt[i] * fraction, keepdims=True) * norm
            dmix[pl.ds(i, ROWS, stride=8), :] = draw * window[i]
            scalars = jnp.where(lane == i, decay, scalars)
    doubled = jnp.concatenate([gather[...], gather[...]], axis=0)
    lanes = lax.broadcasted_iota(jnp.int32, columns.shape, 1)
    col_high = columns[...].astype(bf16).astype(f32)
    mixer = jnp.where(lanes // 8 == 2, columns[...] - col_high, col_high).astype(bf16)[:, :32]

    def tail(n, carry):
        firsts, seconds = carry
        for copy in fetch(n):
            copy.wait()
        stack = []
        for i in range(batch):
            d = dmix[pl.ds(pl.multiple_of((n * batch + i) * 8, 8), 8), :]
            d_high = d.astype(bf16).astype(f32)
            stack.append(
                jnp.concatenate([d_high, d - d_high, d_high, jnp.zeros_like(d)], axis=0).astype(bf16)
            )
        stack = jnp.concatenate(stack, axis=1)
        here = pl.ds(pl.multiple_of(n * wide, wide), wide)
        both_halves = jnp.concatenate([high[:, here], low[:, here]], axis=0)
        seconds = seconds + lax.dot_general(
            both_halves, stack[:16], (((1,), (1,)), ((), ())), preferred_element_type=f32
        )
        q = mm(mixer, stack) * slope[:, here]
        q = jnp.concatenate([q[:, i * COLS : (i + 1) * COLS] for i in range(batch)], axis=0)
        r = mm(jnp.concatenate(split(q), axis=1), doubled)
        r = r[:, :COLS] + r[:, COLS:]
        for i in range(batch):
            firsts = firsts + r[i * order : (i + 1) * order] * rows[pl.ds(n * batch + i, 1), :]
        return firsts, seconds

    firsts, seconds = lax.fori_loop(
        0, ROWS // batch, tail,
        (jnp.zeros((order, COLS), f32), jnp.zeros((2 * order, 16), f32)),
    )
    seconds = jnp.transpose(seconds[:order] + seconds[order:], (1, 0))
    seconds = seconds[:8] + seconds[8:]
    small[:1] = jnp.concatenate([seconds[0:1], seconds[1:2]], axis=1)
    small[1:2] = jnp.concatenate([seconds[2:3], seconds[3:4]], axis=1)
    small[2:3] = scalars
    turned = jnp.transpose(firsts, (1, 0))
    half = COLS // 2
    folded = turned[:half] + turned[half:]
    first[...] = jnp.concatenate([folded[:20], folded[20:40]], axis=1)


def input_kernel(both, gains, spectra, cotan, ileft, iright, tcos, tsin, grad):
    for c in range(0, NARROW, 2):
        pair = inverse_pair(
            times_conj(spectra[c], cotan[c]), times_conj(spectra[c + 1], cotan[c + 1]),
            ileft[...], iright[...], tcos[...], tsin[...],
        )
        for n in range(2):
            i = c + n
            y = both[pl.ds(NARROW + i, ROWS, stride=2 * NARROW), :]
            grad[pl.ds(i, ROWS, stride=NARROW), :] = pair[n] * (1.0 / LENGTH) + gains[i] * y


def join_kernel(grad, small, own, one, two, three, out, tile):
    rows = grad.shape[0] // out.shape[0]
    tile[:3] = small[...]
    tile[3:] = own[...] + one[...] + two[...] + three[...]
    out[:, :rows, :] = grad[...].reshape(out.shape[0], rows, COLS)
    out[:, rows:, :] = jnp.broadcast_to(tile[...][None], (out.shape[0],) + tile.shape)


def unpack_kernel(pairs, home, grad, second, decay, skip):
    groups = grad.shape[0] // NARROW
    order = second.shape[0]
    rows = grad.shape[1] // COLS * NARROW
    block = rows + 8
    for p in range(rows // 8):
        even = pairs[:, 0, 8 * p : 8 * p + 8, :].reshape(-1, COLS)
        odd = pairs[:, 1, 8 * p : 8 * p + 8, :].reshape(-1, COLS)
        for n, part in enumerate(zip_rows(even, odd)):
            grad[:, pl.ds((2 * p + n) * COLS, COLS)] = part
    i = lax.broadcasted_iota(jnp.int32, (groups, groups * NARROW), 0)
    j = lax.broadcasted_iota(jnp.int32, (groups, groups * NARROW), 1)
    flat = [jnp.transpose(home[pl.ds(rows + n, groups, stride=block), :], (1, 0)) for n in range(3)]
    total = jnp.zeros(second.shape, f32)
    scalars = jnp.zeros((8, groups * NARROW), f32)
    line = lax.broadcasted_iota(jnp.int32, scalars.shape, 0)
    for c in range(NARROW):
        place = (j == NARROW * i + c).astype(f32)
        mine = flat[c // 2][(c % 2) * order : (c % 2 + 1) * order]
        total = total + jnp.dot(mine, place, precision=highest, preferred_element_type=f32)
        moved = jnp.dot(flat[2][:8], place, precision=highest, preferred_element_type=f32)
        scalars = scalars + jnp.where(line % NARROW == c, moved, 0.0)
    second[...] = total
    decay[...] = jnp.sum(scalars[:NARROW], axis=0, keepdims=True)
    skip[...] = jnp.sum(scalars[NARROW:], axis=0, keepdims=True)


def finish_kernel(side, own, three, two, one, out, table):
    pieces = (own[...], one[...], two[...], three[...])
    count = own.shape[0]
    order = out.shape[1]
    for n in range(len(pieces)):
        chosen = jnp.zeros(own.shape, f32)
        for i, piece in enumerate(pieces):
            chosen = jnp.where((side[0] ^ i) == n, piece, chosen)
        table[n * count : (n + 1) * count] = chosen
    total = table.shape[0]
    out[:total] = table[:, :order]
    out[total:] = table[: out.shape[0] - total, order:]


def local(signal, cotangent, first_layer, second_layer, decay_rate, skip_gain):
    groups = lax.axis_size("batch")
    place = lax.axis_index("batch")
    side = lax.axis_index("chan")
    sides = lax.axis_size("chan")
    embed, order = first_layer.shape
    t = make_tables(embed)
    vmem = pl.BlockSpec(memory_space=pltpu.VMEM)
    smem = pl.BlockSpec(memory_space=pltpu.SMEM)
    hbm = pl.BlockSpec(memory_space=pltpu.HBM)
    shape = jax.ShapeDtypeStruct
    rows = signal.shape[1] // COLS * NARROW

    def keep(x):
        return pltpu.with_memory_space_constraint(x, pltpu.HBM)

    def call(body, name, outs, specs, args, mib, flops=0, scratch=(), out_specs=None, lp=False):
        return pl.pallas_call(
            body,
            out_shape=outs,
            in_specs=specs,
            out_specs=out_specs or (vmem,) * len(outs),
            scratch_shapes=list(scratch),
            compiler_params=pltpu.CompilerParams(
                vmem_limit_bytes=mib << 20
            ),
            cost_estimate=pl.CostEstimate(flops=flops, bytes_accessed=0, transcendentals=0),
            name=name,
        )(*args)

    quarters = signal.shape[1] // COLS
    (sent,) = call(
        pack_kernel, "pack", (pltpu.HBM((groups // 2, 2, 2 * rows, COLS), f32),), [hbm] * 2,
        (keep(signal), keep(cotangent)), 8, out_specs=(hbm,),
        scratch=[
            pltpu.VMEM((quarters, 2, signal.shape[0], COLS), f32),
            pltpu.VMEM((quarters, groups // 2, 2, 8, COLS), f32),
            pltpu.SemaphoreType.DMA((quarters, 2)),
            pltpu.SemaphoreType.DMA((quarters,)),
        ],
    )
    spread = lax.all_to_all(
        sent.reshape(groups, 2 * rows, COLS), "batch", split_axis=0, concat_axis=0, tiled=True
    ).reshape(-1, COLS)

    columns = lax.dynamic_slice_in_dim(second_layer, place * NARROW, NARROW, 1)
    rates = lax.dynamic_slice_in_dim(decay_rate, place * NARROW, NARROW, 0)
    gains = lax.dynamic_slice_in_dim(skip_gain, place * NARROW, NARROW, 0)
    weights = jnp.pad(first_layer.T * (0.5 / math.pi), ((0, 0), (0, COLS // 2 - embed)))
    weights = jnp.concatenate([weights, weights], axis=1)
    eight = jnp.pad(columns, ((0, 0), (0, 8 - NARROW)))
    tiled = jnp.pad(jnp.concatenate([eight] * 3, axis=1), ((0, 0), (0, COLS - 24)))
    rates = jnp.broadcast_to(jnp.pad(rates, (0, 8 - NARROW))[:, None], (8, COLS))

    full = (order, LENGTH)
    four = (NARROW, ROWS, COLS)
    wide = (NARROW, ROWS, 2 * COLS)
    kept = ((full, bf16), (full, bf16), (full, f32), (four, f32), (four, f32))
    tall = (ROWS * 8, COLS)
    *state, norms, spectra = call(
        filter_kernel, "make_filter",
        tuple(pltpu.HBM(*k) for k in kept) + (shape((8, COLS), f32), pltpu.HBM(wide, f32)),
        [vmem] * 9,
        (
            weights, eight.T, rates, t["rows"], t["spread"],
            t["forward_left"], t["forward_right"], t["twist_cos"], t["twist_sin"],
        ),
        40, flops=20_000_000_000,
        scratch=[pltpu.VMEM(*k) for k in kept] + [
            pltpu.VMEM(wide, f32), pltpu.VMEM(tall, f32), pltpu.VMEM(tall, f32),
            pltpu.SemaphoreType.DMA((6,)),
        ],
        out_specs=(hbm,) * 5 + (vmem, hbm),
    )
    small, first, cotan = call(
        main_kernel, "correlate",
        (shape((3, COLS), f32), shape((20, COLS), f32), shape(wide, f32)),
        [vmem] * 11 + [hbm] * 5,
        (
            spread, tiled, norms, t["rows"], t["gather"],
            t["forward_left"], t["forward_right"], t["inverse_left"], t["inverse_right"],
            t["twist_cos"], t["twist_sin"], *map(keep, state),
        ),
        40, flops=10_000_000_000, lp=True,
        scratch=[pltpu.VMEM(*k) for k in kept] + [
            pltpu.VMEM(tall, f32), pltpu.VMEM(wide, f32),
            pltpu.SemaphoreType.DMA((2,)), pltpu.SemaphoreType.DMA((3, ROWS // TAIL_BATCH)),
        ],
    )

    quarter = first.shape[0] // sides
    pieces = [lax.dynamic_slice_in_dim(first, side * quarter, quarter, 0)]
    for step in reversed(range(1, sides)):
        swap = [(i, i ^ step) for i in range(sides)]
        piece = lax.dynamic_slice_in_dim(first, (side ^ step) * quarter, quarter, 0)
        pieces.append(lax.ppermute(piece, "chan", swap))
    (grad,) = call(
        input_kernel, "input_grad", (shape((groups * rows, COLS), f32),),
        [vmem, smem] + [vmem] * 6,
        (
            spread, gains, spectra, cotan, t["inverse_left"], t["inverse_right"],
            t["twist_cos"], t["twist_sin"],
        ),
        16, flops=4_000_000_000,
    )
    (back,) = call(
        join_kernel, "join", (shape((groups, rows + 8, COLS), f32),), [vmem] * 6,
        (grad, small, *pieces), 8, scratch=[pltpu.VMEM((8, COLS), f32)],
    )
    home = lax.all_to_all(back, "batch", split_axis=0, concat_axis=0, tiled=True)

    mine = home[:, rows + 3 :].sum(0)
    gathered = [mine]
    for step in reversed(range(1, sides)):
        gathered.append(lax.ppermute(mine, "chan", [(i, i ^ step) for i in range(sides)]))
    input_grad, second_grad, decay_grad, skip_grad = call(
        unpack_kernel, "unpack",
        (
            shape(signal.shape, f32), shape(second_layer.shape, f32),
            shape((1,) + decay_rate.shape, f32), shape((1,) + skip_gain.shape, f32),
        ),
        [vmem] * 2, (home.reshape(groups // 2, 2, -1, COLS), home.reshape(-1, COLS)), 8,
        flops=1_000_000_000,
    )
    (first_grad,) = call(
        finish_kernel, "finish", (shape((embed, order), f32),), [smem] + [vmem] * 4,
        (side.reshape(1), *gathered), 4,
        scratch=[pltpu.VMEM((sides * quarter, 2 * order), f32)],
    )
    return (input_grad, first_grad, second_grad, decay_grad[0], skip_grad[0])


def solution(mesh):
    placed = (P("chan", "batch"), P("chan", "batch"), P(), P(None, "chan"), P("chan"), P("chan"))
    return jax.shard_map(
        local,
        mesh=mesh,
        in_specs=placed,
        out_specs=(P("chan", "batch"), P(), P(None, "chan"), P("chan"), P("chan")),
        check_vma=False,
    )
```

```python
import math

import jax
import jax.numpy as jnp
import numpy as np
from jax import lax
from jax.experimental import pallas as pl
from jax.experimental.pallas import tpu as pltpu
from jax.sharding import PartitionSpec as P

ROWS = 256
COLS = 128
LENGTH = ROWS * COLS
NARROW = 4
FILTER_BATCH = 16
TAIL_BATCH = 128
TINY = 1e-06
f32 = jnp.float32
bf16 = jnp.bfloat16
highest = lax.Precision.HIGHEST


def halves(x):
    high = x.astype(bf16)
    low = (x - high.astype(np.float64)).astype(bf16)
    return high, low


SIN = (6.28318528, -10.33542017, 5.100155046, -1.196582571, 0.1553153206)
COS = (0.9999999532, -4.934792831, 4.058411353, -1.331876568, 0.2196896111)


def make_tables(embed):
    a = np.arange(ROWS)
    k = np.arange(ROWS)
    m = np.arange(COLS)
    bands = embed // 2
    turn = np.pi * ((a[None, :] * (4 * k + 1)[:, None]) % (4 * ROWS)) / (2 * ROWS)
    first = np.concatenate([np.cos(turn), -np.sin(turn)], axis=0)
    twist = np.pi * (4 * k + 1)[:, None] * m[None, :] / (2 * LENGTH)
    angle = 2.0 * np.pi * ((m[:, None] * m[None, :]) % COLS) / COLS
    c, s = np.cos(angle), np.sin(angle)
    second = np.concatenate(
        [np.concatenate([c, -s], axis=1), np.concatenate([s, c], axis=1)], axis=0
    )
    high, low = halves(first)
    forward_left = np.concatenate([high, low], axis=1)
    inverse_left = np.concatenate([high.T, low.T], axis=1)
    high, low = halves(second)
    forward_right = np.concatenate([high, low], axis=0)
    inverse_right = np.concatenate([high.T, low.T], axis=0)
    rows = np.zeros((ROWS, COLS))
    lanes = np.zeros((COLS, COLS))
    half = COLS // 2
    rows[:, 0] = a * COLS / LENGTH
    lanes[0] = 1.0
    rows[:, half] = 1.0
    lanes[half] = m / LENGTH
    for b in range(1, bands + 1):
        big = 2.0 * np.pi * ((b * COLS * a) % LENGTH) / LENGTH
        small = 2.0 * np.pi * b * m / LENGTH
        rows[:, b] = np.cos(big)
        rows[:, half + b] = -np.sin(big)
        rows[:, bands + b] = np.sin(big)
        rows[:, half + bands + b] = np.cos(big)
        lanes[b] = np.cos(small)
        lanes[half + b] = np.sin(small)
        lanes[bands + b] = np.cos(small)
        lanes[half + bands + b] = np.sin(small)
    high, low = halves(lanes.T)
    gather = np.concatenate([high, low], axis=1)
    high, low = halves(lanes)
    lowest = (lanes - high.astype(np.float64) - low.astype(np.float64)).astype(bf16)
    spread = np.concatenate([high, low, lowest], axis=0)
    return dict(
        forward_left=forward_left,
        inverse_left=inverse_left,
        forward_right=forward_right,
        inverse_right=inverse_right,
        twist_cos=np.cos(twist).astype(np.float32),
        twist_sin=np.sin(twist).astype(np.float32),
        rows=rows.astype(np.float32),
        spread=spread,
        gather=gather,
    )


def split(x):
    high = x.astype(bf16)
    low = (x - high.astype(f32)).astype(bf16)
    return high, low


def mm(left, right):
    return lax.dot_general(left, right, (((1,), (0,)), ((), ())), preferred_element_type=f32)


def dot_rows(table, x):
    high, low = split(x)
    left = jnp.concatenate([table, table[:, : x.shape[0]]], axis=1)
    return mm(left, jnp.concatenate([high, high, low], axis=0))


def dot_cols(x, table):
    high, low = split(x)
    count = x.shape[1]
    right = jnp.concatenate([table[:count], table], axis=0)
    return mm(jnp.concatenate([high, low, high], axis=1), right)


def forward_pair(x, y, left, right, twist_cos, twist_sin):
    u = dot_rows(left, jnp.concatenate([x, y], axis=1))
    turned = []
    for n in range(2):
        re = u[:ROWS, n * COLS : (n + 1) * COLS]
        im = u[ROWS:, n * COLS : (n + 1) * COLS]
        turned.append(
            jnp.concatenate(
                [re * twist_cos + im * twist_sin, im * twist_cos - re * twist_sin], axis=1
            )
        )
    both = dot_cols(jnp.concatenate(turned, axis=0), right)
    return both[:ROWS], both[ROWS:]


def times_conj(f, c):
    fr, fi, cr, ci = f[:, :COLS], f[:, COLS:], c[:, :COLS], c[:, COLS:]
    return jnp.concatenate([fr * cr + fi * ci, fr * ci - fi * cr], axis=1)


def inverse_pair(g, h, left, right, twist_cos, twist_sin):
    parts = []
    both = dot_cols(jnp.concatenate([g, h], axis=0), right)
    for w in (both[:ROWS], both[ROWS:]):
        re, im = w[:, :COLS], w[:, COLS:]
        parts.append(
            jnp.concatenate(
                [re * twist_cos - im * twist_sin, im * twist_cos + re * twist_sin], axis=0
            )
        )
    y = dot_rows(left, jnp.concatenate(parts, axis=1))
    return y[:, :COLS], y[:, COLS:]


def sin_and_cos(x):
    r = x - ((x + 12582912.0) - 12582912.0)
    z = r * r
    s = SIN[4]
    for n in (3, 2, 1, 0):
        s = s * z + SIN[n]
    s = s * r
    c = COS[4]
    for n in (3, 2, 1, 0):
        c = c * z + COS[n]
    return s * c, 1.0 - 0.5 * (s * s)


def fraction_rows(count, offset):
    a = lax.broadcasted_iota(jnp.int32, (count, COLS), 0) + offset
    m = lax.broadcasted_iota(jnp.int32, (count, COLS), 1)
    return (a * COLS + m).astype(f32) * (1.0 / LENGTH)


def zip_rows(x, y):
    low = lax.broadcasted_iota(jnp.int32, x.shape, 0) % 8 < 4
    count = x.shape[0]
    return (
        jnp.where(low, x, pltpu.roll(y, 4, 0)),
        jnp.where(low, pltpu.roll(x, count - 4, 0), y),
    )


def pack_kernel(signal, cotangent, out, values, turned, into, outof):
    quarters = signal.shape[1] // COLS
    reads, writes = [], []
    for q in range(quarters):
        here = pl.ds(q * COLS, COLS)
        for n, source in enumerate((signal, cotangent)):
            copy = pltpu.make_async_copy(source.at[:, here], values.at[q, n], into.at[q, n])
            copy.start()
            reads.append(copy)
    for q in range(quarters):
        for copy in reads[2 * q : 2 * q + 2]:
            copy.wait()
        for n, part in enumerate(zip_rows(values[q, 0], values[q, 1])):
            turned[q, :, n] = part.reshape(-1, 8, COLS)
        copy = pltpu.make_async_copy(
            turned.at[q], out.at[:, :, pl.ds(8 * q, 8), :], outof.at[q]
        )
        copy.start()
        writes.append(copy)
    for copy in writes:
        copy.wait()


def filter_kernel(
    weights, columns, rates, rows_in, spread_in, left_in, right_in, tcos_in, tsin_in,
    high_out, low_out, slope_out, filt_out, window_out, norms, spectra_out,
    high, low, slope, filt, window, spectra, raws, wins, sems,
    rows, spread, left, right, tcos, tsin, table_sems,
):
    tables = [
        pltpu.make_async_copy(source, target, table_sems.at[n])
        for n, (source, target) in enumerate((
            (rows_in, rows), (spread_in, spread), (left_in, left),
            (right_in, right), (tcos_in, tcos), (tsin_in, tsin),
        ))
    ]
    for one in tables:
        one.start()
    for one in tables:
        one.wait()
    order = weights.shape[0]
    batch = FILTER_BATCH
    wide = batch * COLS

    def copy(source, target, n, here=None):
        if here is not None:
            source, target = source.at[:, here], target.at[:, here]
        return pltpu.make_async_copy(source, target, sems.at[n])

    mixer = jnp.concatenate(split(columns[...]), axis=0)
    table = jnp.concatenate([spread[...], spread[: 2 * COLS], spread[:COLS]], axis=0)
    lane = lax.broadcasted_iota(jnp.int32, (8, COLS), 1)

    def block(n, total):
        scaled = jnp.concatenate(
            [weights[...] * rows[pl.ds(n * batch + i, 1), :] for i in range(batch)], axis=0
        )
        one = scaled.astype(bf16)
        rest = scaled - one.astype(f32)
        two = rest.astype(bf16)
        three = (rest - two.astype(f32)).astype(bf16)
        turns = mm(jnp.concatenate([one, one, one, two, two, three], axis=1), table)
        for i in range(batch):
            here = pl.ds(pl.multiple_of(n * wide + i * COLS, COLS), COLS)
            s, c = sin_and_cos(turns[i * order : (i + 1) * order])
            slope[:, here] = c
            s_high, s_low = split(s)
            high[:, here] = s_high
            low[:, here] = s_low
        here = pl.ds(pl.multiple_of(n * wide, wide), wide)
        copy(high, high_out, 0, here).start()
        copy(low, low_out, 1, here).start()
        copy(slope, slope_out, 2, here).start()
        p = mm(mixer, high[:, here])
        r = mm(mixer, low[:, here])
        mixed = p[:8] + p[8:] + (r[:8] + r[8:])
        for i in range(batch):
            a = n * batch + i
            fraction = (a * COLS + lane).astype(f32) * (1.0 / LENGTH)
            win = jnp.exp(-rates[...] * fraction)
            raw = win * mixed[:, i * COLS : (i + 1) * COLS]
            raws[pl.ds(pl.multiple_of(a * 8, 8), 8), :] = raw
            wins[pl.ds(pl.multiple_of(a * 8, 8), 8), :] = win
            total = total + raw * raw
        return total

    total = lax.fori_loop(0, ROWS // batch, block, jnp.zeros((8, COLS), f32))
    norm = jnp.sqrt(jnp.sum(total, axis=1, keepdims=True) + TINY)
    norms[...] = jnp.broadcast_to(norm, norms.shape)
    for c in range(NARROW):
        filt[c] = raws[pl.ds(c, ROWS, stride=8), :] / norms[pl.ds(c, 1), :]
        window[c] = wins[pl.ds(c, ROWS, stride=8), :]
    copy(filt, filt_out, 3).start()
    copy(window, window_out, 4).start()
    for c in range(0, NARROW, 2):
        x, y = forward_pair(filt[c], filt[c + 1], left[...], right[...], tcos[...], tsin[...])
        spectra[c] = x
        spectra[c + 1] = y
    copy(spectra, spectra_out, 5).start()
    copy(high, high_out, 0).wait()
    copy(low, low_out, 1).wait()
    copy(slope, slope_out, 2).wait()
    copy(filt, filt_out, 3).wait()
    copy(window, window_out, 4).wait()
    copy(spectra, spectra_out, 5).wait()


def main_kernel(
    both, columns, norms, rows, gather, fleft, fright, ileft, iright, tcos, tsin,
    high_in, low_in, slope_in, filt_in, window_in,
    small, first, cotan,
    high, low, slope, filt, window, dmix, product, early, late,
):
    order = slope.shape[0]
    factor = 1.0 / math.sqrt(LENGTH)
    batch = TAIL_BATCH
    wide = batch * COLS
    starts = [
        pltpu.make_async_copy(source, target, early.at[n])
        for n, (source, target) in enumerate(((filt_in, filt), (window_in, window)))
    ]

    def fetch(n):
        here = pl.ds(pl.multiple_of(n * wide, wide), wide)
        return [
            pltpu.make_async_copy(source.at[:, here], target.at[:, here], late.at[m, n])
            for m, (source, target) in enumerate(((high_in, high), (low_in, low), (slope_in, slope)))
        ]

    for copy in starts:
        copy.start()
    lane = lax.broadcasted_iota(jnp.int32, (1, COLS), 1)
    scalars = jnp.zeros((1, COLS), f32)
    fraction = fraction_rows(ROWS, 0)
    dmix[...] = jnp.zeros(dmix.shape, f32)
    for c in range(NARROW):
        x = both[pl.ds(c, ROWS, stride=2 * NARROW), :]
        y = both[pl.ds(NARROW + c, ROWS, stride=2 * NARROW), :]
        skip = factor * jnp.sum(x * y, keepdims=True)
        scalars = jnp.where(lane == NARROW + c, skip, scalars)
        val, cot = forward_pair(x, y, fleft[...], fright[...], tcos[...], tsin[...])
        if c == 0:
            for copy in starts:
                copy.wait()
            for n in range(ROWS // batch):
                for copy in fetch(n):
                    copy.start()
        cotan[c] = cot
        product[c] = times_conj(val, cot)
    for c in range(0, NARROW, 2):
        pair = inverse_pair(
            product[c], product[c + 1], ileft[...], iright[...], tcos[...], tsin[...]
        )
        for n in range(2):
            i = c + n
            dfilt = pair[n] * (factor / LENGTH)
            project = jnp.sum(filt[i] * dfilt, keepdims=True)
            norm = norms[pl.ds(i, 1), :][:, :1]
            draw = (dfilt - filt[i] * project) / norm
            decay = -jnp.sum(draw * filt[i] * fraction, keepdims=True) * norm
            dmix[pl.ds(i, ROWS, stride=8), :] = draw * window[i]
            scalars = jnp.where(lane == i, decay, scalars)
    doubled = jnp.concatenate([gather[...], gather[...]], axis=0)
    lanes = lax.broadcasted_iota(jnp.int32, columns.shape, 1)
    col_high = columns[...].astype(bf16).astype(f32)
    mixer = jnp.where(lanes // 8 == 2, columns[...] - col_high, col_high).astype(bf16)[:, :32]

    def tail(n, carry):
        firsts, seconds = carry
        for copy in fetch(n):
            copy.wait()
        stack = []
        for i in range(batch):
            d = dmix[pl.ds(pl.multiple_of((n * batch + i) * 8, 8), 8), :]
            d_high = d.astype(bf16).astype(f32)
            stack.append(
                jnp.concatenate([d_high, d - d_high, d_high, jnp.zeros_like(d)], axis=0).astype(bf16)
            )
        stack = jnp.concatenate(stack, axis=1)
        here = pl.ds(pl.multiple_of(n * wide, wide), wide)
        both_halves = jnp.concatenate([high[:, here], low[:, here]], axis=0)
        seconds = seconds + lax.dot_general(
            both_halves, stack[:16], (((1,), (1,)), ((), ())), preferred_element_type=f32
        )
        q = mm(mixer, stack) * slope[:, here]
        q = jnp.concatenate([q[:, i * COLS : (i + 1) * COLS] for i in range(batch)], axis=0)
        r = mm(jnp.concatenate(split(q), axis=1), doubled)
        r = r[:, :COLS] + r[:, COLS:]
        for i in range(batch):
            firsts = firsts + r[i * order : (i + 1) * order] * rows[pl.ds(n * batch + i, 1), :]
        return firsts, seconds

    firsts, seconds = lax.fori_loop(
        0, ROWS // batch, tail,
        (jnp.zeros((order, COLS), f32), jnp.zeros((2 * order, 16), f32)),
    )
    seconds = jnp.transpose(seconds[:order] + seconds[order:], (1, 0))
    seconds = seconds[:8] + seconds[8:]
    small[:1] = jnp.concatenate([seconds[0:1], seconds[1:2]], axis=1)
    small[1:2] = jnp.concatenate([seconds[2:3], seconds[3:4]], axis=1)
    small[2:3] = scalars
    turned = jnp.transpose(firsts, (1, 0))
    half = COLS // 2
    folded = turned[:half] + turned[half:]
    first[...] = jnp.concatenate([folded[:20], folded[20:40]], axis=1)


def input_kernel(both, gains, spectra, cotan, ileft, iright, tcos, tsin, grad):
    for c in range(0, NARROW, 2):
        pair = inverse_pair(
            times_conj(spectra[c], cotan[c]), times_conj(spectra[c + 1], cotan[c + 1]),
            ileft[...], iright[...], tcos[...], tsin[...],
        )
        for n in range(2):
            i = c + n
            y = both[pl.ds(NARROW + i, ROWS, stride=2 * NARROW), :]
            grad[pl.ds(i, ROWS, stride=NARROW), :] = pair[n] * (1.0 / LENGTH) + gains[i] * y


def join_kernel(grad, small, own, one, two, three, out, tile):
    rows = grad.shape[0] // out.shape[0]
    tile[:3] = small[...]
    tile[3:] = own[...] + one[...] + two[...] + three[...]
    out[:, :rows, :] = grad[...].reshape(out.shape[0], rows, COLS)
    out[:, rows:, :] = jnp.broadcast_to(tile[...][None], (out.shape[0],) + tile.shape)


def unpack_kernel(pairs, home, grad, second, decay, skip):
    groups = grad.shape[0] // NARROW
    order = second.shape[0]
    rows = grad.shape[1] // COLS * NARROW
    block = rows + 8
    for p in range(rows // 8):
        even = pairs[:, 0, 8 * p : 8 * p + 8, :].reshape(-1, COLS)
        odd = pairs[:, 1, 8 * p : 8 * p + 8, :].reshape(-1, COLS)
        for n, part in enumerate(zip_rows(even, odd)):
            grad[:, pl.ds((2 * p + n) * COLS, COLS)] = part
    i = lax.broadcasted_iota(jnp.int32, (groups, groups * NARROW), 0)
    j = lax.broadcasted_iota(jnp.int32, (groups, groups * NARROW), 1)
    flat = [jnp.transpose(home[pl.ds(rows + n, groups, stride=block), :], (1, 0)) for n in range(3)]
    total = jnp.zeros(second.shape, f32)
    scalars = jnp.zeros((8, groups * NARROW), f32)
    line = lax.broadcasted_iota(jnp.int32, scalars.shape, 0)
    for c in range(NARROW):
        place = (j == NARROW * i + c).astype(f32)
        mine = flat[c // 2][(c % 2) * order : (c % 2 + 1) * order]
        total = total + jnp.dot(mine, place, precision=highest, preferred_element_type=f32)
        moved = jnp.dot(flat[2][:8], place, precision=highest, preferred_element_type=f32)
        scalars = scalars + jnp.where(line % NARROW == c, moved, 0.0)
    second[...] = total
    decay[...] = jnp.sum(scalars[:NARROW], axis=0, keepdims=True)
    skip[...] = jnp.sum(scalars[NARROW:], axis=0, keepdims=True)


def finish_kernel(side, own, three, two, one, out, table):
    pieces = (own[...], one[...], two[...], three[...])
    count = own.shape[0]
    order = out.shape[1]
    for n in range(len(pieces)):
        chosen = jnp.zeros(own.shape, f32)
        for i, piece in enumerate(pieces):
            chosen = jnp.where((side[0] ^ i) == n, piece, chosen)
        table[n * count : (n + 1) * count] = chosen
    total = table.shape[0]
    out[:total] = table[:, :order]
    out[total:] = table[: out.shape[0] - total, order:]


def local(signal, cotangent, first_layer, second_layer, decay_rate, skip_gain):
    groups = lax.axis_size("batch")
    place = lax.axis_index("batch")
    side = lax.axis_index("chan")
    sides = lax.axis_size("chan")
    embed, order = first_layer.shape
    t = make_tables(embed)
    vmem = pl.BlockSpec(memory_space=pltpu.VMEM)
    smem = pl.BlockSpec(memory_space=pltpu.SMEM)
    hbm = pl.BlockSpec(memory_space=pltpu.HBM)
    shape = jax.ShapeDtypeStruct
    rows = signal.shape[1] // COLS * NARROW

    def keep(x):
        return pltpu.with_memory_space_constraint(x, pltpu.HBM)

    def call(body, name, outs, specs, args, mib, flops=0, scratch=(), out_specs=None, lp=False):
        return pl.pallas_call(
            body,
            out_shape=outs,
            in_specs=specs,
            out_specs=out_specs or (vmem,) * len(outs),
            scratch_shapes=list(scratch),
            compiler_params=pltpu.CompilerParams(
                vmem_limit_bytes=mib << 20
            ),
            cost_estimate=pl.CostEstimate(flops=flops, bytes_accessed=0, transcendentals=0),
            name=name,
        )(*args)

    quarters = signal.shape[1] // COLS
    (sent,) = call(
        pack_kernel, "pack", (pltpu.HBM((groups // 2, 2, 2 * rows, COLS), f32),), [hbm] * 2,
        (keep(signal), keep(cotangent)), 8, out_specs=(hbm,),
        scratch=[
            pltpu.VMEM((quarters, 2, signal.shape[0], COLS), f32),
            pltpu.VMEM((quarters, groups // 2, 2, 8, COLS), f32),
            pltpu.SemaphoreType.DMA((quarters, 2)),
            pltpu.SemaphoreType.DMA((quarters,)),
        ],
    )
    spread = lax.all_to_all(
        sent.reshape(groups, 2 * rows, COLS), "batch", split_axis=0, concat_axis=0, tiled=True
    ).reshape(-1, COLS)

    columns = lax.dynamic_slice_in_dim(second_layer, place * NARROW, NARROW, 1)
    rates = lax.dynamic_slice_in_dim(decay_rate, place * NARROW, NARROW, 0)
    gains = lax.dynamic_slice_in_dim(skip_gain, place * NARROW, NARROW, 0)
    weights = jnp.pad(first_layer.T * (0.5 / math.pi), ((0, 0), (0, COLS // 2 - embed)))
    weights = jnp.concatenate([weights, weights], axis=1)
    eight = jnp.pad(columns, ((0, 0), (0, 8 - NARROW)))
    tiled = jnp.pad(jnp.concatenate([eight] * 3, axis=1), ((0, 0), (0, COLS - 24)))
    rates = jnp.broadcast_to(jnp.pad(rates, (0, 8 - NARROW))[:, None], (8, COLS))

    full = (order, LENGTH)
    four = (NARROW, ROWS, COLS)
    wide = (NARROW, ROWS, 2 * COLS)
    kept = ((full, bf16), (full, bf16), (full, f32), (four, f32), (four, f32))
    tall = (ROWS * 8, COLS)
    names = ("rows", "spread", "forward_left", "forward_right", "twist_cos", "twist_sin")
    *state, norms, spectra = call(
        filter_kernel, "make_filter",
        tuple(pltpu.HBM(*k) for k in kept) + (shape((8, COLS), f32), pltpu.HBM(wide, f32)),
        [vmem] * 3 + [hbm] * 6,
        (
            weights, eight.T, rates, *(keep(t[name]) for name in names),
        ),
        40, flops=20_000_000_000,
        scratch=[pltpu.VMEM(*k) for k in kept] + [
            pltpu.VMEM(wide, f32), pltpu.VMEM(tall, f32), pltpu.VMEM(tall, f32),
            pltpu.SemaphoreType.DMA((6,)),
            *(pltpu.VMEM(t[name].shape, t[name].dtype) for name in names),
            pltpu.SemaphoreType.DMA((6,)),
        ],
        out_specs=(hbm,) * 5 + (vmem, hbm),
    )
    small, first, cotan = call(
        main_kernel, "correlate",
        (shape((3, COLS), f32), shape((20, COLS), f32), shape(wide, f32)),
        [vmem] * 11 + [hbm] * 5,
        (
            spread, tiled, norms, t["rows"], t["gather"],
            t["forward_left"], t["forward_right"], t["inverse_left"], t["inverse_right"],
            t["twist_cos"], t["twist_sin"], *map(keep, state),
        ),
        40, flops=10_000_000_000, lp=True,
        scratch=[pltpu.VMEM(*k) for k in kept] + [
            pltpu.VMEM(tall, f32), pltpu.VMEM(wide, f32),
            pltpu.SemaphoreType.DMA((2,)), pltpu.SemaphoreType.DMA((3, ROWS // TAIL_BATCH)),
        ],
    )

    quarter = first.shape[0] // sides
    pieces = [lax.dynamic_slice_in_dim(first, side * quarter, quarter, 0)]
    for step in reversed(range(1, sides)):
        swap = [(i, i ^ step) for i in range(sides)]
        piece = lax.dynamic_slice_in_dim(first, (side ^ step) * quarter, quarter, 0)
        pieces.append(lax.ppermute(piece, "chan", swap))
    (grad,) = call(
        input_kernel, "input_grad", (shape((groups * rows, COLS), f32),),
        [vmem, smem] + [vmem] * 6,
        (
            spread, gains, spectra, cotan, t["inverse_left"], t["inverse_right"],
            t["twist_cos"], t["twist_sin"],
        ),
        16, flops=4_000_000_000,
    )
    (back,) = call(
        join_kernel, "join", (shape((groups, rows + 8, COLS), f32),), [vmem] * 6,
        (grad, small, *pieces), 8, scratch=[pltpu.VMEM((8, COLS), f32)],
    )
    home = lax.all_to_all(back, "batch", split_axis=0, concat_axis=0, tiled=True)

    mine = home[:, rows + 3 :].sum(0)
    gathered = [mine]
    for step in reversed(range(1, sides)):
        gathered.append(lax.ppermute(mine, "chan", [(i, i ^ step) for i in range(sides)]))
    input_grad, second_grad, decay_grad, skip_grad = call(
        unpack_kernel, "unpack",
        (
            shape(signal.shape, f32), shape(second_layer.shape, f32),
            shape((1,) + decay_rate.shape, f32), shape((1,) + skip_gain.shape, f32),
        ),
        [vmem] * 2, (home.reshape(groups // 2, 2, -1, COLS), home.reshape(-1, COLS)), 8,
        flops=1_000_000_000,
    )
    (first_grad,) = call(
        finish_kernel, "finish", (shape((embed, order), f32),), [smem] + [vmem] * 4,
        (side.reshape(1), *gathered), 4,
        scratch=[pltpu.VMEM((sides * quarter, 2 * order), f32)],
    )
    return (input_grad, first_grad, second_grad, decay_grad[0], skip_grad[0])


def solution(mesh):
    placed = (P("chan", "batch"), P("chan", "batch"), P(), P(None, "chan"), P("chan"), P("chan"))
    return jax.shard_map(
        local,
        mesh=mesh,
        in_specs=placed,
        out_specs=(P("chan", "batch"), P(), P(None, "chan"), P("chan"), P("chan")),
        check_vma=False,
    )
```
